32 devices in a mesh: model: 4 (over z), data: 8 (over y, x, core).
Axes of the slice: x: 2, y: 2, z: 4, core: 2. Of those that a mesh axis runs over, the one named last changes fastest.
Arguments:
- grad_wi0: float32 [8, 1024, 2816], P('data', None, 'model')
- param_wi0: float32 [1024, 2816], P('data', 'model')
- vrow_wi0: float32 [1024], P('data')
- vcol_wi0: float32 [2816], P('model')
- grad_wi1: float32 [8, 1024, 2816], P('data', None, 'model')
- param_wi1: float32 [1024, 2816], P('data', 'model')
- vrow_wi1: float32 [1024], P('data')
- vcol_wi1: float32 [2816], P('model')
- grad_wo: float32 [8, 2816, 1024], P('data', None, 'model')
- param_wo: float32 [2816, 1024], P('data', 'model')
- vrow_wo: float32 [2816], P('data')
- vcol_wo: float32 [1024], P('model')
- grad_wq: float32 [8, 1024, 1024], P('data', None, 'model')
- param_wq: float32 [1024, 1024], P('data', 'model')
- vrow_wq: float32 [1024], P('data')
- vcol_wq: float32 [1024], P('model')
Outputs:
- output 1: float32 [1024, 2816], P('data', 'model')
- output 2: float32 [1024, 2816], P('data', 'model')
- output 3: float32 [1024], P('data')
- output 4: float32 [2816], P('model')
- output 5: float32 [1024, 2816], P('data', 'model')
- output 6: float32 [1024, 2816], P('data', 'model')
- output 7: float32 [1024], P('data')
- output 8: float32 [2816], P('model')
- output 9: float32 [2816, 1024], P('data', 'model')
- output 10: float32 [2816, 1024], P('data', 'model')
- output 11: float32 [2816], P('data')
- output 12: float32 [1024], P('model')
- output 13: float32 [1024, 1024], P('data', 'model')
- output 14: float32 [1024, 1024], P('data', 'model')
- output 15: float32 [1024], P('data')
- output 16: float32 [1024], P('model')
All inputs are finite; a program needn't handle non-finite values.
Results may differ from the reference program's by a relative error of at most 0.001.
Values sent between devices are 32-bit elements.
A program may use at most 1 GiB of HBM per device.

```python
import jax
import jax.numpy as jnp
from jax import lax

D_MODEL = 1024
D_FF = 2816
NUM_HEADS = 16
HEAD_DIM = 64
REPLICAS = 8
OPT_STEP = 3


def matrix_draw(key, rows, cols):
    keys = jax.random.split(key, 7)
    row_pos = (jnp.arange(rows, dtype=jnp.float32) + 0.5) * (2.0 / rows) - 1.0
    col_pos = (jnp.arange(cols, dtype=jnp.float32) + 0.5) * (2.0 / cols) - 1.0
    row_scale = jnp.exp(row_pos + 0.25 * jax.random.normal(keys[0], (rows,), jnp.float32))
    col_scale = jnp.exp(-col_pos + 0.25 * jax.random.normal(keys[1], (cols,), jnp.float32))
    rep_scale = jnp.exp(0.3 * jax.random.normal(keys[2], (REPLICAS,), jnp.float32)) / jnp.sqrt(jnp.float32(REPLICAS))
    noise = jax.random.normal(keys[3], (REPLICAS, rows, cols), jnp.float32)
    grad_reps = noise * rep_scale[:, None, None] * row_scale[None, :, None] * col_scale[None, None, :]
    vrow = 0.5 * jnp.exp(-row_pos + jax.random.uniform(keys[4], (rows,), jnp.float32, -0.7, 0.7))
    vcol = 0.5 * jnp.exp(col_pos + jax.random.uniform(keys[5], (cols,), jnp.float32, -0.7, 0.7))
    param = jax.random.normal(keys[6], (rows, cols), jnp.float32) * jnp.exp(0.6 * row_pos)[:, None] * jnp.exp(0.6 * col_pos)[None, :]
    return grad_reps, param, vrow, vcol


def setup_inputs(seed: int = 0) -> dict:
    base_key = jax.random.key(seed)
    q_dim = NUM_HEADS * HEAD_DIM
    layout = (('wi0', D_MODEL, D_FF), ('wi1', D_MODEL, D_FF), ('wo', D_FF, D_MODEL), ('wq', D_MODEL, q_dim))
    inputs = {}
    for index, (label, rows, cols) in enumerate(layout):
        grad_reps, param, vrow, vcol = matrix_draw(jax.random.fold_in(base_key, index), rows, cols)
        inputs['grad_' + label] = grad_reps
        inputs['param_' + label] = param
        inputs['vrow_' + label] = vrow
        inputs['vcol_' + label] = vcol
    return inputs


def matrix_update(grad_reps, param, vrow, vcol):
    decay_pow = OPT_STEP ** -0.8
    beta = 1.0 - decay_pow
    step_pow = OPT_STEP ** -0.5
    lr_rel = min(0.01, step_pow)
    grad = jnp.sum(grad_reps, axis=0)
    grad_sq = grad * grad + 1e-30
    vrow_new = beta * vrow + (1.0 - beta) * jnp.mean(grad_sq, axis=1)
    vcol_new = beta * vcol + (1.0 - beta) * jnp.mean(grad_sq, axis=0)
    row_factor = lax.rsqrt(vrow_new / jnp.mean(vrow_new))
    col_factor = lax.rsqrt(vcol_new)
    update = grad * row_factor[:, None] * col_factor[None, :]
    update = update / jnp.maximum(1.0, jnp.sqrt(jnp.mean(update * update)))
    param_scale = jnp.maximum(1e-3, jnp.sqrt(jnp.mean(param * param)))
    delta = -(lr_rel * param_scale) * update
    return param + delta, delta, vrow_new, vcol_new


def reference(grad_wi0, param_wi0, vrow_wi0, vcol_wi0, grad_wi1, param_wi1, vrow_wi1, vcol_wi1, grad_wo, param_wo, vrow_wo, vcol_wo, grad_wq, param_wq, vrow_wq, vcol_wq):
    param_new_wi0, delta_wi0, vrow_new_wi0, vcol_new_wi0 = matrix_update(grad_wi0, param_wi0, vrow_wi0, vcol_wi0)
    param_new_wi1, delta_wi1, vrow_new_wi1, vcol_new_wi1 = matrix_update(grad_wi1, param_wi1, vrow_wi1, vcol_wi1)
    param_new_wo, delta_wo, vrow_new_wo, vcol_new_wo = matrix_update(grad_wo, param_wo, vrow_wo, vcol_wo)
    param_new_wq, delta_wq, vrow_new_wq, vcol_new_wq = matrix_update(grad_wq, param_wq, vrow_wq, vcol_wq)
    return (param_new_wi0, delta_wi0, vrow_new_wi0, vcol_new_wi0, param_new_wi1, delta_wi1, vrow_new_wi1, vcol_new_wi1, param_new_wo, delta_wo, vrow_new_wo, vcol_new_wo, param_new_wq, delta_wq, vrow_new_wq, vcol_new_wq)
```

```python
import jax
import jax.numpy as jnp
from jax import lax
from jax.experimental import pallas as pl
from jax.experimental.pallas import tpu as pltpu
from jax.sharding import PartitionSpec as P

OPT_STEP = 3
BETA = 1.0 - OPT_STEP ** -0.8
LR_REL = min(0.01, OPT_STEP ** -0.5)
NM = 4
OWN, NX, NY, ND = 0, 1, 2, 3
STEP_ROWS = (32, 32, 88, 64)
MESH_ID = pl.DeviceIdType.MESH


def make_reduce_kernel(rows_b, cols, n_model, n_data):
    rh = [r // 2 for r in rows_b]
    tiles = [-(-c // 128) for c in cols]
    vtiles = [-(-r // 128) for r in rows_b]
    rows_t = [r * n_data for r in rows_b]
    cols_t = [c * n_model for c in cols]

    def kernel(*refs):
        grads = refs[0:4]
        params = refs[4:8]
        vrows = refs[8:12]
        vcols = refs[12:16]
        upd = refs[16:20]
        vrow_out = refs[20:24]
        vcol_out = refs[24:28]
        fac_out = refs[28]
        sc = list(refs[29:])
        take = lambda n: [sc.pop(0) for _ in range(n)]
        loc, rec, fx, fy, wbuf, vrbuf, vcbuf, crow = (take(4) for _ in range(8))
        rmsg, rrx, cmsg, crx, bmsg, brx, vrc, vcc, w2 = take(9)
        (ld_sem, dd_s, dd_r, x_s, x_r, y_s, y_r, in_sem,
         ra_s, ra_r, ca_s, ca_r, b_s, b_r) = take(14)
        greet = take(1)[0]

        z = lax.axis_index('model')
        d = lax.axis_index('data')
        core = lax.rem(d, 2)
        xx = lax.rem(d // 2, 2)
        yy = d // 4
        sib = d + 1 - 2 * core
        dx = d + 2 - 4 * xx
        dy = d + 4 - 8 * yy
        dd = dx + 4 - 8 * yy
        owner = {OWN: d, NX: dx, NY: dy, ND: dd}
        flip = 1 - 2 * core

        lane = lax.broadcasted_iota(jnp.int32, (8, 128), 1)
        sub = lax.broadcasted_iota(jnp.int32, (8, 128), 0)

        def remote(src, dst, ssem, rsem, data=None, model=None):
            return pltpu.make_async_remote_copy(
                src_ref=src, dst_ref=dst, send_sem=ssem, recv_sem=rsem,
                device_id=(z if model is None else model, d if data is None else data),
                device_id_type=MESH_ID)

        def signal(sem, data=None, model=None):
            pl.semaphore_signal(
                sem, inc=1,
                device_id=(z if model is None else model, d if data is None else data),
                device_id_type=MESH_ID)

        order = []
        for m in range(NM):
            order += [(m, ND, 0), (m, ND, 1), (m, NX, 0), (m, NY, 1)]
        for m in range(NM):
            order += [(m, NY, 0), (m, NX, 1)]
        for m in range(NM):
            order += [(m, OWN, 0), (m, OWN, 1)]

        def slot(m, j, h):
            return (m * 4 + j) * 2 + h

        loads = {}
        for m, j, h in order:
            start = pl.multiple_of(owner[j] * rows_b[m] + h * rh[m], 8)
            loads[m, j, h] = pltpu.make_async_copy(
                grads[m].at[0, pl.ds(start, rh[m]), :], loc[m].at[j, h], ld_sem.at[slot(m, j, h)])
            loads[m, j, h].start()
        small = []
        for m in range(NM):
            small.append(pltpu.make_async_copy(params[m], wbuf[m], in_sem.at[m]))
            small.append(pltpu.make_async_copy(vrows[m], vrbuf[m], in_sem.at[4 + m]))
            small.append(pltpu.make_async_copy(vcols[m], vcbuf[m], in_sem.at[8 + m]))
        for cp in small:
            cp.start()

        barrier = pltpu.get_barrier_semaphore()
        for peer in (sib, dx, dy):
            signal(barrier, data=peer)
        up_ok = z < n_model - 1
        down_ok = z > 0

        def signal_z(sem):
            @pl.when(up_ok)
            def _():
                signal(sem, model=z + 1)

            @pl.when(down_ok)
            def _():
                signal(sem, model=z - 1)

        n_z = jnp.where(up_ok, 1, 0) + jnp.where(down_ok, 1, 0)
        signal_z(barrier)
        pl.semaphore_wait(barrier, 3 + n_z)

        dsend = {}
        for m, j, h in order:
            start = pl.multiple_of((owner[j] + flip) * rows_b[m] + h * rh[m], 8)
            k = slot(m, j, h)
            dsend[m, j, h] = remote(
                grads[m].at[0, pl.ds(start, rh[m]), :], rec[m].at[j, h], dd_s.at[k], dd_r.at[k], data=sib)
            dsend[m, j, h].start()

        def pair_sum(m, j, h, extra=None):
            loads[m, j, h].wait()
            dsend[m, j, h].wait_recv()
            total = loc[m][j, h] + rec[m][j, h]
            if extra is not None:
                total = total + extra
            loc[m][j, h] = total

        xsend, ysend = {}, {}
        for m in range(NM):
            xsend[m, 0] = remote(loc[m].at[ND, 0], fx[m].at[0], x_s.at[3 * m], x_r.at[3 * m], data=dx)
            xsend[m, 1] = remote(loc[m].at[NX, 0], fx[m].at[1], x_s.at[3 * m + 1], x_r.at[3 * m + 1], data=dx)
            xsend[m, 2] = remote(loc[m].at[NX, 1], fx[m].at[2], x_s.at[3 * m + 2], x_r.at[3 * m + 2], data=dx)
            ysend[m, 0] = remote(loc[m].at[ND, 1], fy[m].at[0], y_s.at[3 * m], y_r.at[3 * m], data=dy)
            ysend[m, 1] = remote(loc[m].at[NY, 0], fy[m].at[1], y_s.at[3 * m + 1], y_r.at[3 * m + 1], data=dy)
            ysend[m, 2] = remote(loc[m].at[NY, 1], fy[m].at[2], y_s.at[3 * m + 2], y_r.at[3 * m + 2], data=dy)

        for m in range(NM):
            pair_sum(m, ND, 0)
            xsend[m, 0].start()
            pair_sum(m, ND, 1)
            ysend[m, 0].start()
            pair_sum(m, NX, 0)
            xsend[m, 1].start()
            pair_sum(m, NY, 1)
            ysend[m, 2].start()

        for cp in small:
            cp.wait()
        w2v = jnp.zeros((8, 128), jnp.float32)
        for m in range(NM):
            w = wbuf[m][...]
            part = jnp.sum(w * w, axis=(0, 1), keepdims=True) * (1.0 / (rows_t[m] * cols_t[m]))
            w2v = jnp.where((sub == 2) & (lane == m), part, w2v)
            cmsg[m] = jnp.zeros((8, 128), jnp.float32)
            vcc[m] = jnp.ones((8, 128), jnp.float32)
            for k in range(tiles[m]):
                w_k = min(128, cols[m] - 128 * k)
                vcc[m, k:k + 1, 0:w_k] = vcbuf[m][0:1, 128 * k:128 * k + w_k]
            acc = jnp.zeros((8, 128), jnp.float32)
            for t in range(vtiles[m]):
                n_t = min(128, rows_b[m] - 128 * t)
                row = jnp.broadcast_to(vrbuf[m][t:t + 1, :], (8, 128))
                for g in range(n_t // 8):
                    col = jnp.sum(jnp.where(lane == 8 * g + sub, row, 0.0), axis=1, keepdims=True)
                    acc = jnp.where(lane == 16 * t + g, col, acc)
            vrc[m] = acc
        w2[...] = w2v

        signal(greet.at[0], data=sib)
        pl.semaphore_wait(greet.at[0], 1)
        signal(greet.at[1], data=dx)
        pl.semaphore_wait(greet.at[1], 1)
        signal(greet.at[2], data=dy)
        pl.semaphore_wait(greet.at[2], 1)
        signal_z(greet.at[3])
        pl.semaphore_wait(greet.at[3], n_z)
        signal_z(greet.at[4])
        pl.semaphore_wait(greet.at[4], n_z)

        for m in range(NM):
            xsend[m, 0].wait_recv()
            pair_sum(m, NY, 0, fx[m][0])
            ysend[m, 1].start()
            ysend[m, 0].wait_recv()
            pair_sum(m, NX, 1, fy[m][0])
            xsend[m, 2].start()

        rsend, csend = {}, {}
        for m in range(NM):
            for k in range(1, n_model):
                i = m * (n_model - 1) + k - 1
                rsend[m, k] = remote(rmsg.at[m], rrx.at[i], ra_s.at[i], ra_r.at[i],
                                     model=lax.rem(z + k, n_model))
            for k in range(1, n_data):
                i = m * (n_data - 1) + k - 1
                csend[m, k] = remote(cmsg.at[m], crx.at[i], ca_s.at[i], ca_r.at[i],
                                     data=lax.rem(d + k, n_data))

        for m in range(NM):
            step = STEP_ROWS[m]
            cacc = jnp.zeros((8, cols[m]), jnp.float32)
            racc = jnp.zeros((8, 128), jnp.float32)
            for h in range(2):
                loads[m, OWN, h].wait()
                dsend[m, OWN, h].wait_recv()
                xsend[m, 1 + h].wait_recv()
                ysend[m, 1 + h].wait_recv()

                def body(it, carry, m=m, h=h, step=step):
                    cacc, racc = carry
                    r0 = pl.multiple_of(it * step, 8)
                    rows = pl.ds(r0, step)
                    total = (loc[m][OWN, h, rows, :] + rec[m][OWN, h, rows, :]
                             + fx[m][1 + h, rows, :] + fy[m][1 + h, rows, :])
                    upd[m][pl.ds(pl.multiple_of(h * rh[m] + r0, 8), step), :] = total
                    sq = total * total + 1e-30
                    for g in range(step // 8):
                        part = sq[8 * g:8 * g + 8, :]
                        cacc = cacc + part
                        rsum = jnp.sum(part, axis=1, keepdims=True)
                        racc = jnp.where(lane == (h * rh[m] + it * step) // 8 + g, rsum, racc)
                    return cacc, racc

                cacc, racc = lax.fori_loop(0, rh[m] // step, body, (cacc, racc))
            rmsg[m] = racc
            csum = jnp.sum(cacc, axis=0, keepdims=True)
            for k in range(tiles[m]):
                w_k = min(128, cols[m] - 128 * k)
                cmsg[m, k:k + 1, 0:w_k] = csum[:, 128 * k:128 * k + w_k]
            for k in range(1, n_model):
                rsend[m, k].start()
            for k in range(n_data - 1, 0, -1):
                csend[m, k].start()

        bv = w2[...]
        locrow = jnp.ones((8, 128), jnp.float32)
        for m in range(NM):
            rtot = rmsg[m]
            for k in range(1, n_model):
                rsend[m, k].wait_recv()
                rtot = rtot + rrx[m * (n_model - 1) + k - 1]
            ctot = cmsg[m]
            for k in range(1, n_data):
                csend[m, k].wait_recv()
                ctot = ctot + crx[m * (n_data - 1) + k - 1]
            vr = BETA * vrc[m] + (1.0 - BETA) * (rtot * (1.0 / cols_t[m]))
            vc = BETA * vcc[m] + (1.0 - BETA) * (ctot * (1.0 / rows_t[m]))
            vrc[m] = vr
            valid = lane < rows_b[m] // 8
            vr_sum = jnp.sum(jnp.where(valid, vr, 0.0), axis=(0, 1), keepdims=True)
            mloc = vr_sum * (1.0 / rows_b[m])
            rfac = lax.rsqrt(jnp.where(valid, vr / mloc, 1.0))
            cfac = lax.rsqrt(vc)
            for k in range(tiles[m]):
                w_k = min(128, cols[m] - 128 * k)
                crow[m][0:1, 128 * k:128 * k + w_k] = cfac[k:k + 1, 0:w_k]
                vcol_out[m][0:1, 128 * k:128 * k + w_k] = vc[k:k + 1, 0:w_k]
            cf = jnp.broadcast_to(crow[m][0:1, :], (8, cols[m]))
            step = STEP_ROWS[m]

            def tbody(it, tacc, m=m, step=step, cf=cf, rfac=rfac):
                for g in range(step // 8):
                    r0 = pl.multiple_of(it * step + 8 * g, 8)
                    rcol = jnp.sum(jnp.where(lane == it * (step // 8) + g, rfac, 0.0), axis=1, keepdims=True)
                    u = upd[m][pl.ds(r0, 8), :] * rcol * cf
                    upd[m][pl.ds(r0, 8), :] = u
                    tacc = tacc + u * u
                return tacc

            tacc = lax.fori_loop(0, rows_b[m] // step, tbody, jnp.zeros((8, cols[m]), jnp.float32))
            t_m = jnp.sum(tacc, axis=(0, 1), keepdims=True) * (1.0 / (rows_t[m] * cols_t[m]))
            bv = jnp.where((sub == 0) & (lane == m), t_m / mloc, bv)
            bv = jnp.where((sub == 1) & (lane == m), vr_sum * (1.0 / (rows_t[m] * n_model)), bv)
            locrow = jnp.where(lane == m, mloc, locrow)

        bmsg[...] = bv
        bsend = []
        for kz in range(n_model):
            for kd in range(n_data):
                if kz == 0 and kd == 0:
                    continue
                i = kz * n_data + kd - 1
                bsend.append(remote(bmsg, brx.at[i], b_s.at[i], b_r.at[i],
                                    data=lax.rem(d + kd, n_data), model=lax.rem(z + kz, n_model)))
        for cp in reversed(bsend):
            cp.start()

        for m in range(NM):
            vr = vrc[m]
            for t in range(vtiles[m]):
                n_t = min(128, rows_b[m] - 128 * t)
                acc = jnp.zeros((8, 128), jnp.float32)
                for g in range(n_t // 8):
                    col = jnp.sum(jnp.where(lane == 16 * t + g, vr, 0.0), axis=1, keepdims=True)
                    acc = jnp.where(lane == 8 * g + sub, col, acc)
                keep = jnp.where(lax.rem(lane, 8) == sub, acc, 0.0)
                vrow_out[m][t:t + 1, :] = jnp.sum(keep, axis=0, keepdims=True)

        for cp in bsend:
            cp.wait_recv()
        tot = bmsg[...]
        for i in range(n_model * n_data - 1):
            tot = tot + brx[i]
        mean_vr = tot[1:2, :]
        u_rms = jnp.sqrt(mean_vr * tot[0:1, :])
        w_rms = jnp.sqrt(tot[2:3, :])
        fac = -(LR_REL * jnp.maximum(1e-3, w_rms)) * (jnp.sqrt(mean_vr) * lax.rsqrt(locrow[0:1, :]))
        fac_out[...] = jnp.broadcast_to(fac / jnp.maximum(1.0, u_rms), (8, 128))

        for key in dsend:
            dsend[key].wait_send()
        for group in (xsend, ysend, rsend, csend):
            for key in group:
                group[key].wait_send()
        for cp in bsend:
            cp.wait_send()

    f32 = jnp.float32
    n_row_msgs = NM * (n_model - 1)
    n_col_msgs = NM * (n_data - 1)
    n_b = n_model * n_data - 1
    dma = pltpu.SemaphoreType.DMA
    scratch = []
    scratch += [pltpu.VMEM((4, 2, rh[m], cols[m]), f32) for m in range(NM)]
    scratch += [pltpu.VMEM((4, 2, rh[m], cols[m]), f32) for m in range(NM)]
    scratch += [pltpu.VMEM((3, rh[m], cols[m]), f32) for m in range(NM)]
    scratch += [pltpu.VMEM((3, rh[m], cols[m]), f32) for m in range(NM)]
    scratch += [pltpu.VMEM((rows_b[m], cols[m]), f32) for m in range(NM)]
    scratch += [pltpu.VMEM((vtiles[m], 128), f32) for m in range(NM)]
    scratch += [pltpu.VMEM((1, cols[m]), f32) for m in range(NM)]
    scratch += [pltpu.VMEM((1, cols[m]), f32) for m in range(NM)]
    scratch += [
        pltpu.VMEM((NM, 8, 128), f32), pltpu.VMEM((n_row_msgs, 8, 128), f32),
        pltpu.VMEM((NM, 8, 128), f32), pltpu.VMEM((n_col_msgs, 8, 128), f32),
        pltpu.VMEM((8, 128), f32), pltpu.VMEM((n_b, 8, 128), f32),
        pltpu.VMEM((NM, 8, 128), f32), pltpu.VMEM((NM, 8, 128), f32), pltpu.VMEM((8, 128), f32),
    ]
    scratch += [dma((32,)), dma((32,)), dma((32,)), dma((12,)), dma((12,)), dma((12,)), dma((12,)), dma((12,)),
                dma((n_row_msgs,)), dma((n_row_msgs,)), dma((n_col_msgs,)), dma((n_col_msgs,)),
                dma((n_b,)), dma((n_b,))]
    scratch += [pltpu.SemaphoreType.REGULAR((5,))]
    out_shape = ([jax.ShapeDtypeStruct((rows_b[m], cols[m]), f32) for m in range(NM)]
                 + [jax.ShapeDtypeStruct((vtiles[m], 128), f32) for m in range(NM)]
                 + [jax.ShapeDtypeStruct((1, cols[m]), f32) for m in range(NM)]
                 + [jax.ShapeDtypeStruct((8, 128), f32)])
    vmem = pl.BlockSpec(memory_space=pltpu.VMEM)
    anyspace = pl.BlockSpec(memory_space=pl.ANY)
    return pl.pallas_call(
        kernel, out_shape=out_shape, in_specs=[anyspace] * 16, out_specs=[vmem] * len(out_shape),
        scratch_shapes=scratch,
        compiler_params=pltpu.CompilerParams(collective_id=0, has_side_effects=True,
                                             vmem_limit_bytes=48 * 1024 * 1024))


def make_apply_kernel(rows_b, cols):
    def kernel(*refs):
        upd, params, vrow_in, vcol_in = refs[0:4], refs[4:8], refs[8:12], refs[12:16]
        fac_ref = refs[16]
        new, delta, vrow_out, vcol_out = refs[17:21], refs[21:25], refs[25:29], refs[29:33]
        for m in range(NM):
            fac = fac_ref[0:1, m:m + 1]
            step = fac * upd[m][...]
            delta[m][...] = step
            new[m][...] = params[m][...] + step
            vrow_out[m][...] = vrow_in[m][...]
            vcol_out[m][...] = vcol_in[m][...]

    f32 = jnp.float32
    vmem = pl.BlockSpec(memory_space=pltpu.VMEM)
    vtiles = [-(-r // 128) for r in rows_b]
    mats = [jax.ShapeDtypeStruct((rows_b[m], cols[m]), f32) for m in range(NM)]
    out_shape = (mats + mats + [jax.ShapeDtypeStruct((vtiles[m], 128), f32) for m in range(NM)]
                 + [jax.ShapeDtypeStruct((1, cols[m]), f32) for m in range(NM)])
    return pl.pallas_call(kernel, out_shape=out_shape, in_specs=[vmem] * 17, out_specs=[vmem] * 16)


def solution(mesh):
    n_data = mesh.shape['data']
    n_model = mesh.shape['model']
    mat_spec = P('data', 'model')
    in_specs = (P('data', None, 'model'), mat_spec, P('data'), P('model')) * NM
    out_specs = (mat_spec, mat_spec, P('data'), P('model')) * NM

    def per_device(*arrays):
        grads, params = arrays[0::4], arrays[1::4]
        rows_b = [p.shape[0] for p in params]
        cols = [p.shape[1] for p in params]
        vrows = [jnp.pad(v, (0, -v.shape[0] % 128)).reshape(-1, 128) for v in arrays[2::4]]
        vcols = [v.reshape(1, -1) for v in arrays[3::4]]
        outs = make_reduce_kernel(rows_b, cols, n_model, n_data)(*grads, *params, *vrows, *vcols)
        upd, vr, vc, fac = outs[0:4], outs[4:8], outs[8:12], outs[12]
        res = make_apply_kernel(rows_b, cols)(*upd, *params, *vr, *vc, fac)
        flat = []
        for m in range(NM):
            flat += [res[m], res[4 + m], res[8 + m].reshape(-1)[:rows_b[m]], res[12 + m].reshape(-1)]
        return tuple(flat)

    return jax.shard_map(per_device, mesh=mesh, in_specs=in_specs, out_specs=out_specs, check_vma=False)
```

```python
import jax
import jax.numpy as jnp
from jax import lax
from jax.experimental import pallas as pl
from jax.experimental.pallas import tpu as pltpu
from jax.sharding import PartitionSpec as P

OPT_STEP = 3
BETA = 1.0 - OPT_STEP ** -0.8
LR_REL = min(0.01, OPT_STEP ** -0.5)
NM = 4
OWN, NX, NY, ND = 0, 1, 2, 3
STEP_ROWS = (88, 88, 88, 64)
MESH_ID = pl.DeviceIdType.MESH


def layout_of(rows_b, cols, n_model, n_data):
    mats = []
    for r, c in zip(rows_b, cols):
        flip = c % 128 != 0
        n0, n1 = (c, r) if flip else (r, c)
        mats.append(dict(flip=flip, n0=n0, n1=n1, half=n0 // 2, groups=n0 // 8, tiles=-(-n0 // 128), lanes=n1 // 128,
                         rows_b=r, rows_t=r * n_data, cols_t=c * n_model,
                         size=float(r * n_data * c * n_model)))
    return mats


def make_reduce_kernel(rows_b, cols, n_model, n_data):
    mats = layout_of(rows_b, cols, n_model, n_data)

    def kernel(*refs):
        grads = refs[0:4]
        params = refs[4:8]
        vrows = refs[8:12]
        vcols = refs[12:16]
        upd = refs[16:20]
        wbuf = refs[20:24]
        stats = refs[24]
        sc = list(refs[25:])
        take = lambda n: [sc.pop(0) for _ in range(n)]
        loc, rec, fx, fy, vrbuf, vcbuf = (take(4) for _ in range(6))
        rmsg, rrx, cmsg, crx, bmsg, brx, vrc, vcc, stage = take(9)
        (ld_sem, dd_s, dd_r, x_s, x_r, y_s, y_r, in_sem,
         ra_s, ra_r, ca_s, ca_r, b_s, b_r) = take(14)
        greet = take(1)[0]

        z = lax.axis_index('model')
        d = lax.axis_index('data')
        core = lax.rem(d, 2)
        xx = lax.rem(d // 2, 2)
        yy = d // 4
        sib = d + 1 - 2 * core
        dx = d + 2 - 4 * xx
        dy = d + 4 - 8 * yy
        dd = dx + 4 - 8 * yy
        owner = {OWN: d, NX: dx, NY: dy, ND: dd}
        sib_step = 1 - 2 * core

        lane = lax.broadcasted_iota(jnp.int32, (8, 128), 1)
        sub = lax.broadcasted_iota(jnp.int32, (8, 128), 0)

        def remote(src, dst, ssem, rsem, data=None, model=None):
            return pltpu.make_async_remote_copy(
                src_ref=src, dst_ref=dst, send_sem=ssem, recv_sem=rsem,
                device_id=(z if model is None else model, d if data is None else data),
                device_id_type=MESH_ID)

        def signal(sem, data=None, model=None):
            pl.semaphore_signal(
                sem, inc=1,
                device_id=(z if model is None else model, d if data is None else data),
                device_id_type=MESH_ID)

        order = []
        for m in range(NM):
            order += [(m, ND, 0), (m, ND, 1), (m, NX, 0), (m, NY, 1)]
        for m in range(NM):
            order += [(m, NY, 0), (m, NX, 1)]
        for m in range(NM):
            order += [(m, OWN, 0), (m, OWN, 1)]

        def slot(m, j, h):
            return (m * 4 + j) * 2 + h

        def block(m, who, h):
            q = mats[m]
            if q['flip']:
                cut = pl.ds(pl.multiple_of(who * q['n1'], 128), q['n1'])
                return grads[m].at[0, pl.ds(h * q['half'], q['half']), cut]
            return grads[m].at[0, pl.ds(pl.multiple_of(who * q['n0'] + h * q['half'], 8), q['half']), :]

        loads = {}
        for m, j, h in order:
            loads[m, j, h] = pltpu.make_async_copy(block(m, owner[j], h), loc[m].at[j, h], ld_sem.at[slot(m, j, h)])
            loads[m, j, h].start()
        small = []
        for m in range(NM):
            small.append(pltpu.make_async_copy(params[m], wbuf[m], in_sem.at[m]))
            small.append(pltpu.make_async_copy(vrows[m], vrbuf[m], in_sem.at[4 + m]))
            small.append(pltpu.make_async_copy(vcols[m], vcbuf[m], in_sem.at[8 + m]))
        for cp in small:
            cp.start()

        barrier = pltpu.get_barrier_semaphore()
        for peer in (sib, dx, dy):
            signal(barrier, data=peer)
        up_ok = z < n_model - 1
        down_ok = z > 0

        def signal_z(sem):
            @pl.when(up_ok)
            def _():
                signal(sem, model=z + 1)

            @pl.when(down_ok)
            def _():
                signal(sem, model=z - 1)

        n_z = jnp.where(up_ok, 1, 0) + jnp.where(down_ok, 1, 0)
        signal_z(barrier)
        pl.semaphore_wait(barrier, 3 + n_z)

        dsend = {}
        for m, j, h in order:
            k = slot(m, j, h)
            dsend[m, j, h] = remote(block(m, owner[j] + sib_step, h), rec[m].at[j, h], dd_s.at[k], dd_r.at[k], data=sib)
            dsend[m, j, h].start()

        def pair_sum(m, j, h, extra=None):
            loads[m, j, h].wait()
            dsend[m, j, h].wait_recv()
            total = loc[m][j, h] + rec[m][j, h]
            if extra is not None:
                total = total + extra
            loc[m][j, h] = total

        xsend, ysend = {}, {}
        for m in range(NM):
            for i, (j, h) in enumerate(((ND, 0), (NX, 0), (NX, 1))):
                xsend[m, i] = remote(loc[m].at[j, h], fx[m].at[i], x_s.at[3 * m + i], x_r.at[3 * m + i], data=dx)
            for i, (j, h) in enumerate(((ND, 1), (NY, 0), (NY, 1))):
                ysend[m, i] = remote(loc[m].at[j, h], fy[m].at[i], y_s.at[3 * m + i], y_r.at[3 * m + i], data=dy)

        for m in range(NM):
            pair_sum(m, ND, 0)
            xsend[m, 0].start()
            pair_sum(m, ND, 1)
            ysend[m, 0].start()
            pair_sum(m, NX, 0)
            xsend[m, 1].start()
            pair_sum(m, NY, 1)
            ysend[m, 2].start()

        for cp in small:
            cp.wait()

        def rows_of(buf, n, i):
            stage[i] = jnp.zeros((8, 128), jnp.float32)
            for t in range(-(-n // 128)):
                n_t = min(128, n - 128 * t)
                stage[i, t:t + 1, 0:n_t] = buf[pl.ds(128 * t, n_t)].reshape(1, n_t)

        def to_compact(i, n):
            acc = jnp.zeros((8, 128), jnp.float32)
            for t in range(-(-n // 128)):
                row = jnp.broadcast_to(stage[i, t:t + 1, :], (8, 128))
                for g in range(min(128, n - 128 * t) // 8):
                    col = jnp.sum(jnp.where(lane == 8 * g + sub, row, 0.0), axis=1, keepdims=True)
                    acc = jnp.where(lane == 16 * t + g, col, acc)
            return acc

        bv = jnp.zeros((8, 128), jnp.float32)
        for m in range(NM):
            q = mats[m]
            w = wbuf[m][...]
            part = jnp.sum(w * w, axis=(0, 1), keepdims=True) * (1.0 / q['size'])
            bv = jnp.where((sub == 2) & (lane == m), part, bv)
            rows_of(vrbuf[m], q['rows_b'], 2 * m)
            rows_of(vcbuf[m], cols[m], 2 * m + 1)
            if q['flip']:
                vrc[m] = stage[2 * m]
                vcc[m] = to_compact(2 * m + 1, q['n0'])
            else:
                vrc[m] = to_compact(2 * m, q['n0'])
                vcc[m] = stage[2 * m + 1]
            rmsg[m] = jnp.zeros((8, 128), jnp.float32)
            cmsg[m] = jnp.zeros((8, 128), jnp.float32)
        bmsg[...] = bv

        signal(greet.at[0], data=sib)
        pl.semaphore_wait(greet.at[0], 1)
        signal(greet.at[1], data=dx)
        pl.semaphore_wait(greet.at[1], 1)
        signal(greet.at[2], data=dy)
        pl.semaphore_wait(greet.at[2], 1)
        signal_z(greet.at[3])
        pl.semaphore_wait(greet.at[3], n_z)
        signal_z(greet.at[4])
        pl.semaphore_wait(greet.at[4], n_z)

        for m in range(NM):
            xsend[m, 0].wait_recv()
            pair_sum(m, NY, 0, fx[m][0])
            ysend[m, 1].start()
            ysend[m, 0].wait_recv()
            pair_sum(m, NX, 1, fy[m][0])
            xsend[m, 2].start()

        rsend, csend = {}, {}
        for m in range(NM):
            for k in range(1, n_model):
                i = m * (n_model - 1) + k - 1
                rsend[m, k] = remote(rmsg.at[m], rrx.at[i], ra_s.at[i], ra_r.at[i],
                                     model=lax.rem(z + k, n_model))
            for k in range(1, n_data):
                i = m * (n_data - 1) + k - 1
                csend[m, k] = remote(cmsg.at[m], crx.at[i], ca_s.at[i], ca_r.at[i],
                                     data=lax.rem(d + k, n_data))

        for m in range(NM):
            q = mats[m]
            step = STEP_ROWS[m]
            acc1 = jnp.zeros((8, q['n1']), jnp.float32)
            acc0 = jnp.zeros((8, 128), jnp.float32)
            for h in range(2):
                loads[m, OWN, h].wait()
                dsend[m, OWN, h].wait_recv()
                xsend[m, 1 + h].wait_recv()
                ysend[m, 1 + h].wait_recv()

                def body(it, carry, m=m, h=h, step=step, half=q['half']):
                    acc1, acc0 = carry
                    r0 = pl.multiple_of(it * step, 8)
                    rows = pl.ds(r0, step)
                    total = (loc[m][OWN, h, rows, :] + rec[m][OWN, h, rows, :]
                             + fx[m][1 + h, rows, :] + fy[m][1 + h, rows, :])
                    upd[m][pl.ds(pl.multiple_of(h * half + r0, 8), step), :] = total
                    sq = total * total + 1e-30
                    for g in range(step // 8):
                        part = sq[8 * g:8 * g + 8, :]
                        acc1 = acc1 + part
                        rsum = jnp.sum(part, axis=1, keepdims=True)
                        acc0 = jnp.where(lane == (h * half + it * step) // 8 + g, rsum, acc0)
                    return acc1, acc0

                acc1, acc0 = lax.fori_loop(0, q['half'] // step, body, (acc1, acc0))
            sum1 = jnp.sum(acc1, axis=0, keepdims=True)
            msg0, msg1 = (cmsg, rmsg) if q['flip'] else (rmsg, cmsg)
            msg0[m] = acc0
            for k in range(q['lanes']):
                msg1[m, k:k + 1, :] = sum1[:, 128 * k:128 * k + 128]
            for k in range(1, n_model):
                rsend[m, k].start()
            for k in range(n_data - 1, 0, -1):
                csend[m, k].start()

        bv = bmsg[...]
        locrow = jnp.ones((8, 128), jnp.float32)
        for m in range(NM):
            q = mats[m]
            rtot = rmsg[m]
            for k in range(1, n_model):
                rsend[m, k].wait_recv()
                rtot = rtot + rrx[m * (n_model - 1) + k - 1]
            ctot = cmsg[m]
            for k in range(1, n_data):
                csend[m, k].wait_recv()
                ctot = ctot + crx[m * (n_data - 1) + k - 1]
            vr = BETA * vrc[m] + (1.0 - BETA) * (rtot * (1.0 / q['cols_t']))
            vc = BETA * vcc[m] + (1.0 - BETA) * (ctot * (1.0 / q['rows_t']))
            ok0 = lane < q['groups']
            ok1 = sub < q['lanes']
            okr, okc = (ok1, ok0) if q['flip'] else (ok0, ok1)
            vr_sum = jnp.sum(jnp.where(okr, vr, 0.0), axis=(0, 1), keepdims=True)
            mloc = vr_sum * (1.0 / q['rows_b'])
            rfac = lax.rsqrt(jnp.where(okr, vr / mloc, 1.0))
            cfac = lax.rsqrt(jnp.where(okc, vc, 1.0))
            fac0, fac1 = (cfac, rfac) if q['flip'] else (rfac, cfac)
            if q['flip']:
                vcc[m] = vc
                stats[1 + 2 * m] = vr
            else:
                vcc[m] = vr
                stats[1 + 2 * m] = vc
            f1 = jnp.concatenate([jnp.broadcast_to(fac1[k:k + 1, :], (8, 128)) for k in range(q['lanes'])], axis=1)
            step = STEP_ROWS[m]

            def tbody(it, tacc, m=m, step=step, f1=f1, fac0=fac0):
                for g in range(step // 8):
                    r0 = pl.multiple_of(it * step + 8 * g, 8)
                    f0 = jnp.sum(jnp.where(lane == it * (step // 8) + g, fac0, 0.0), axis=1, keepdims=True)
                    u = upd[m][pl.ds(r0, 8), :] * f0 * f1
                    upd[m][pl.ds(r0, 8), :] = u
                    tacc = tacc + u * u
                return tacc

            tacc = lax.fori_loop(0, q['n0'] // step, tbody, jnp.zeros((8, q['n1']), jnp.float32))
            t_m = jnp.sum(tacc, axis=(0, 1), keepdims=True) * (1.0 / q['size'])
            bv = jnp.where((sub == 0) & (lane == m), t_m / mloc, bv)
            bv = jnp.where((sub == 1) & (lane == m), vr_sum * (1.0 / (q['rows_t'] * n_model)), bv)
            locrow = jnp.where(lane == m, mloc, locrow)

        bmsg[...] = bv
        bsend = []
        for kz in range(n_model):
            for kd in range(n_data):
                if kz == 0 and kd == 0:
                    continue
                i = kz * n_data + kd - 1
                bsend.append(remote(bmsg, brx.at[i], b_s.at[i], b_r.at[i],
                                    data=lax.rem(d + kd, n_data), model=lax.rem(z + kz, n_model)))
        for cp in reversed(bsend):
            cp.start()

        for m in range(NM):
            q = mats[m]
            v = vcc[m]
            out = jnp.zeros((8, 128), jnp.float32)
            for t in range(q['tiles']):
                acc = jnp.zeros((8, 128), jnp.float32)
                for g in range(min(128, q['n0'] - 128 * t) // 8):
                    col = jnp.sum(jnp.where(lane == 16 * t + g, v, 0.0), axis=1, keepdims=True)
                    acc = jnp.where(lane == 8 * g + sub, col, acc)
                out = jnp.where(sub == t, jnp.sum(acc, axis=0, keepdims=True), out)
            stats[2 + 2 * m] = out

        for cp in bsend:
            cp.wait_recv()
        tot = bmsg[...]
        for i in range(n_model * n_data - 1):
            tot = tot + brx[i]
        mean_vr = tot[1:2, :]
        u_rms = jnp.sqrt(mean_vr * tot[0:1, :])
        w_rms = jnp.sqrt(tot[2:3, :])
        fac = -(LR_REL * jnp.maximum(1e-3, w_rms)) * (jnp.sqrt(mean_vr) * lax.rsqrt(locrow[0:1, :]))
        stats[0] = jnp.broadcast_to(fac / jnp.maximum(1.0, u_rms), (8, 128))

        for key in dsend:
            dsend[key].wait_send()
        for group in (xsend, ysend, rsend, csend):
            for key in group:
                group[key].wait_send()
        for cp in bsend:
            cp.wait_send()

    f32 = jnp.float32
    n_row_msgs = NM * (n_model - 1)
    n_col_msgs = NM * (n_data - 1)
    n_b = n_model * n_data - 1
    dma = pltpu.SemaphoreType.DMA
    vm = pltpu.VMEM
    scratch = []
    scratch += [vm((4, 2, q['half'], q['n1']), f32) for q in mats]
    scratch += [vm((4, 2, q['half'], q['n1']), f32) for q in mats]
    scratch += [vm((3, q['half'], q['n1']), f32) for q in mats]
    scratch += [vm((3, q['half'], q['n1']), f32) for q in mats]
    scratch += [vm((r,), f32) for r in rows_b]
    scratch += [vm((c,), f32) for c in cols]
    tile = lambda *lead: vm((*lead, 8, 128), f32)
    scratch += [tile(NM), tile(n_row_msgs), tile(NM), tile(n_col_msgs), tile(), tile(n_b),
                tile(NM), tile(NM), tile(2 * NM)]
    scratch += [dma((32,)), dma((32,)), dma((32,)), dma((12,)), dma((12,)), dma((12,)), dma((12,)), dma((12,)),
                dma((n_row_msgs,)), dma((n_row_msgs,)), dma((n_col_msgs,)), dma((n_col_msgs,)),
                dma((n_b,)), dma((n_b,))]
    scratch += [pltpu.SemaphoreType.REGULAR((5,))]
    blocks = [jax.ShapeDtypeStruct((q['n0'], q['n1']), f32) for q in mats]
    out_shape = blocks + blocks + [jax.ShapeDtypeStruct((1 + 2 * NM, 8, 128), f32)]
    vmem = pl.BlockSpec(memory_space=pltpu.VMEM)
    hbm = pl.BlockSpec(memory_space=pltpu.HBM)
    return pl.pallas_call(
        kernel, out_shape=out_shape, in_specs=[hbm] * 16, out_specs=[vmem] * len(out_shape),
        scratch_shapes=scratch,
        compiler_params=pltpu.CompilerParams(collective_id=0, has_side_effects=True,
                                             vmem_limit_bytes=28 * 1024 * 1024))


def make_apply_kernel(rows_b, cols, n_model, n_data):
    mats = layout_of(rows_b, cols, n_model, n_data)

    def kernel(*refs):
        upd, params, stats = refs[0:4], refs[4:8], refs[8]
        new, delta, vrow_out, vcol_out = refs[9:13], refs[13:17], refs[17:21], refs[21:25]
        bufs = refs[25:33]
        sem = refs[33]
        copies = []
        for m in range(NM):
            fac = stats[0, 0:1, m:m + 1]
            step = fac * upd[m][...]
            bufs[4 + m][...] = step
            bufs[m][...] = params[m][...] + step
            for i, out in ((m, new[m]), (4 + m, delta[m])):
                copies.append(pltpu.make_async_copy(bufs[i], out, sem.at[i]))
                copies[-1].start()
        for m in range(NM):
            q = mats[m]
            out1, out0 = (vrow_out[m], vcol_out[m]) if q['flip'] else (vcol_out[m], vrow_out[m])
            for k in range(q['lanes']):
                out1[pl.ds(128 * k, 128)] = stats[1 + 2 * m, k:k + 1, :].reshape(128)
            for t in range(q['tiles']):
                n_t = min(128, q['n0'] - 128 * t)
                out0[pl.ds(128 * t, n_t)] = stats[2 + 2 * m, t:t + 1, 0:n_t].reshape(n_t)
        for cp in copies:
            cp.wait()

    f32 = jnp.float32
    vmem = pl.BlockSpec(memory_space=pltpu.VMEM)
    hbm = pl.BlockSpec(memory_space=pltpu.HBM)
    blocks = [jax.ShapeDtypeStruct((q['n0'], q['n1']), f32) for q in mats]
    out_shape = (blocks + blocks + [jax.ShapeDtypeStruct((r,), f32) for r in rows_b]
                 + [jax.ShapeDtypeStruct((c,), f32) for c in cols])
    return pl.pallas_call(
        kernel, out_shape=out_shape, in_specs=[vmem] * 9, out_specs=[hbm] * 8 + [vmem] * 8,
        scratch_shapes=[pltpu.VMEM((q['n0'], q['n1']), f32) for q in mats] * 2 + [pltpu.SemaphoreType.DMA((8,))],
        compiler_params=pltpu.CompilerParams(vmem_limit_bytes=6 * 1024 * 1024))


def solution(mesh):
    n_data = mesh.shape['data']
    n_model = mesh.shape['model']
    mat_spec = P('data', 'model')
    in_specs = (P('data', None, 'model'), mat_spec, P('data'), P('model')) * NM
    out_specs = (mat_spec, mat_spec, P('data'), P('model')) * NM

    def per_device(*arrays):
        grads, params = arrays[0::4], arrays[1::4]
        rows_b = [p.shape[0] for p in params]
        cols = [p.shape[1] for p in params]
        mats = layout_of(rows_b, cols, n_model, n_data)
        view = lambda i, a: jnp.swapaxes(a, -1, -2) if mats[i]['flip'] else a
        grads = [view(i, g) for i, g in enumerate(grads)]
        params = [view(i, p) for i, p in enumerate(params)]
        pin = lambda a: pltpu.with_memory_space_constraint(a, pltpu.HBM)
        outs = make_reduce_kernel(rows_b, cols, n_model, n_data)(
            *map(pin, grads), *map(pin, params), *map(pin, arrays[2::4]), *map(pin, arrays[3::4]))
        res = make_apply_kernel(rows_b, cols, n_model, n_data)(*outs)
        flat = []
        for m in range(NM):
            flat += [view(m, res[m]), view(m, res[4 + m]), res[8 + m], res[12 + m]]
        return tuple(flat)

    return jax.shard_map(per_device, mesh=mesh, in_specs=in_specs, out_specs=out_specs, check_vma=False)
```

```python
import jax
import jax.numpy as jnp
from jax import lax
from jax.experimental import pallas as pl
from jax.experimental.pallas import tpu as pltpu
from jax.sharding import PartitionSpec as P

OPT_STEP = 3
BETA = 1.0 - OPT_STEP ** -0.8
LR_REL = min(0.01, OPT_STEP ** -0.5)
NM = 4
OWN, NX, NY, ND = 0, 1, 2, 3
FIRST_ROWS = 88
MESH_ID = pl.DeviceIdType.MESH


def layout_of(rows_b, cols, n_model, n_data):
    mats = []
    for r, c in zip(rows_b, cols):
        flip = c % 128 != 0
        n0, n1 = (c, r) if flip else (r, c)
        mats.append(dict(flip=flip, n0=n0, n1=n1, half=n0 // 2, groups=n0 // 8, tiles=-(-n0 // 128), lanes=n1 // 128,
                         rows_b=r, rows_t=r * n_data, cols_t=c * n_model,
                         size=float(r * n_data * c * n_model)))
    return mats


def make_reduce_kernel(rows_b, cols, n_model, n_data):
    mats = layout_of(rows_b, cols, n_model, n_data)
    halves = [q['half'] for q in mats]
    first = []
    for lo, hi in ((0, FIRST_ROWS), (FIRST_ROWS, halves[0])):
        first += [(0, ND, lo, hi - lo), (0, ND, halves[0] + lo, hi - lo)]
    whole = {(m, j): (m, j, 0, mats[m]['n0']) for m in range(NM) for j in (OWN, NX, NY, ND) if (m, j) != (0, ND)}
    fetches = first + list(whole.values())
    index = {f: i for i, f in enumerate(fetches)}
    ld_slot = {f: i for i, f in enumerate(first)}
    for m in range(NM):
        for i, j in enumerate((ND, NX, NY)):
            if (m, j) in whole:
                ld_slot[whole[m, j]] = {0: 3 + i, 1: 6 + i, 2: (0, 4, 5)[i], 3: 6 + i}[m]
        ld_slot[whole[m, OWN]] = 9 + m

    def kernel(*refs):
        grads = refs[0:4]
        params = refs[4:8]
        vrows = refs[8:12]
        vcols = refs[12:16]
        upd = refs[16:20]
        wbuf = refs[20:24]
        stats = refs[24]
        sc = list(refs[25:])
        take = lambda n: [sc.pop(0) for _ in range(n)]
        loc, rec, fxy, vrbuf, vcbuf = (take(4) for _ in range(5))
        stg, rmsg, rrx, cmsg, crx, csib, brx, vrc, vcc, stage = take(10)
        ld_sem, dd_s, dd_r, l_s, l_r, in_sem, a_s, ra_r, ca_r, cs_r, b_s, b_r, greet = take(13)

        z = lax.axis_index('model')
        d = lax.axis_index('data')
        core = lax.rem(d, 2)
        xx = lax.rem(d // 2, 2)
        yy = d // 4
        sib_step = 1 - 2 * core
        sib = d + sib_step
        dx = d + 2 - 4 * xx
        dy = d + 4 - 8 * yy
        dd = dx + 4 - 8 * yy
        owner = {OWN: d, NX: dx, NY: dy, ND: dd}

        def remote(src, dst, ssem, rsem, data=None, model=None):
            return pltpu.make_async_remote_copy(
                src_ref=src, dst_ref=dst, send_sem=ssem, recv_sem=rsem,
                device_id=(z if model is None else model, d if data is None else data),
                device_id_type=MESH_ID)

        def signal(sem, data=None, model=None):
            pl.semaphore_signal(
                sem, inc=1,
                device_id=(z if model is None else model, d if data is None else data),
                device_id_type=MESH_ID)

        def wait_bytes(ref, sem):
            pltpu.make_async_copy(ref, ref, sem).wait()

        barrier = pltpu.get_barrier_semaphore()
        for peer in (sib, dx, dy):
            signal(barrier, data=peer)
        up_ok = z < n_model - 1
        down_ok = z > 0

        def signal_z(sem):
            @pl.when(up_ok)
            def _():
                signal(sem, model=z + 1)

            @pl.when(down_ok)
            def _():
                signal(sem, model=z - 1)

        n_z = jnp.where(up_ok, 1, 0) + jnp.where(down_ok, 1, 0)
        signal_z(barrier)

        def block(who, f):
            m, j, r0, n = f
            q = mats[m]
            if q['flip']:
                cut = pl.ds(pl.multiple_of(who * q['n1'], 128), q['n1'])
                return grads[m].at[0, pl.ds(r0, n), cut]
            return grads[m].at[0, pl.ds(pl.multiple_of(who * q['n0'] + r0, 8), n), :]

        loads, dsend, stage_in = {}, {}, {}
        for f in fetches:
            m, j, r0, n = f
            part = (m, pl.ds(r0, n))
            loads[f] = pltpu.make_async_copy(block(owner[j], f), loc[m].at[j, pl.ds(r0, n), :], ld_sem.at[ld_slot[f]])
            source = block(owner[j] + sib_step, f)
            if f in first:
                held = stg.at[pl.ds(r0, n), :]
                stage_in[f] = pltpu.make_async_copy(source, held, ld_sem.at[9 + first.index(f)])
                source = held
            dsend[f] = remote(source, rec[m].at[j, pl.ds(r0, n), :], dd_s.at[m], dd_r.at[index[f]], data=sib)

        def fetch(pieces):
            for f in pieces:
                dsend[f].start()
                loads[f].start()

        def fetch_done(f):
            loads[f].wait()
            dsend[f].wait_recv()

        def link_send(m, j, r0, n):
            h, off = (0, r0) if r0 < halves[m] else (1, r0 - halves[m])
            along_x = (j == ND and h == 0) or j == NX
            slot = (0 if along_x else 3) + (0 if j == ND else 1 + h)
            return remote(loc[m].at[j, pl.ds(r0, n), :], fxy[m].at[slot, pl.ds(off, n), :],
                          l_s.at[m], l_r.at[6 * m + slot], data=dx if along_x else dy)

        def arrived(m, slot):
            wait_bytes(fxy[m].at[slot], l_r.at[6 * m + slot])

        def pair_sum(m, j, r0, n, relay=None):
            total = loc[m][j, r0:r0 + n, :] + rec[m][j, r0:r0 + n, :]
            if relay is not None:
                total = total + fxy[m][relay]
            loc[m][j, r0:r0 + n, :] = total
            link_send(m, j, r0, n).start()

        def send_raw(m):
            n = halves[m]
            fetch_done(whole[m, ND])
            pair_sum(m, ND, 0, n)
            pair_sum(m, ND, n, n)
            send_near(m)

        def send_near(m):
            n = halves[m]
            fetch_done(whole[m, NX])
            pair_sum(m, NX, 0, n)
            fetch_done(whole[m, NY])
            pair_sum(m, NY, n, n)

        def send_acc(m):
            n = halves[m]
            arrived(m, 0)
            pair_sum(m, NY, 0, n, 0)
            arrived(m, 3)
            pair_sum(m, NX, n, n, 3)

        for f in first:
            stage_in[f].start()
        for f in first:
            loads[f].start()
        pl.semaphore_wait(barrier, 3 + n_z)
        for f in first:
            stage_in[f].wait()
            dsend[f].start()
        fetch([whole[0, NX], whole[0, NY]])
        for f in first[0:2]:
            fetch_done(f)
            pair_sum(*f)
        fetch([whole[1, ND], whole[1, NX], whole[1, NY]])
        for f in first[2:4]:
            fetch_done(f)
            pair_sum(*f)
        send_near(0)
        fetch([whole[2, ND], whole[2, NX], whole[2, NY]])
        send_raw(1)
        fetch([whole[3, ND], whole[3, NX], whole[3, NY]])
        fetch([whole[m, OWN] for m in range(NM)])
        small = []
        for m in range(NM):
            small.append(pltpu.make_async_copy(params[m], wbuf[m], in_sem.at[m]))
            small.append(pltpu.make_async_copy(vrows[m], vrbuf[m], in_sem.at[4 + m]))
            small.append(pltpu.make_async_copy(vcols[m], vcbuf[m], in_sem.at[8 + m]))
        for cp in small:
            cp.start()

        lane = lax.broadcasted_iota(jnp.int32, (8, 128), 1)
        sub = lax.broadcasted_iota(jnp.int32, (8, 128), 0)
        lane1 = lax.broadcasted_iota(jnp.int32, (1, 128), 1)

        def group_mask(g):
            shape = (g, 8, 128)
            return lax.broadcasted_iota(jnp.int32, shape, 2) == lax.broadcasted_iota(jnp.int32, shape, 0)

        def compact(values):
            return jnp.sum(jnp.where(group_mask(values.shape[0]), values, 0.0), axis=0)

        def expand(vec, g):
            return jnp.sum(jnp.where(group_mask(g), vec[None], 0.0), axis=2, keepdims=True)

        def rows_of(buf, n, i):
            stage[i] = jnp.zeros((8, 128), jnp.float32)
            for t in range(-(-n // 128)):
                n_t = min(128, n - 128 * t)
                stage[i, t:t + 1, 0:n_t] = buf[pl.ds(128 * t, n_t)].reshape(1, n_t)

        def to_compact(i, n):
            out = jnp.zeros((8, 128), jnp.float32)
            for t in range(-(-n // 128)):
                row = jnp.broadcast_to(stage[i, t:t + 1, :], (8, 128))
                for g in range(min(128, n - 128 * t) // 8):
                    col = jnp.sum(jnp.where(lane == 8 * g + sub, row, 0.0), axis=1, keepdims=True)
                    out = jnp.where(lane == 16 * t + g, col, out)
            return out

        for cp in small:
            cp.wait()
        bv = jnp.zeros((1, 128), jnp.float32)
        for m in range(NM):
            q = mats[m]
            w = wbuf[m][...]
            part = jnp.sum(w * w, axis=(0, 1), keepdims=True) * (1.0 / q['size'])
            bv = jnp.where(lane1 == 2 * NM + m, part, bv)
            rows_of(vrbuf[m], q['rows_b'], 2 * m)
            rows_of(vcbuf[m], cols[m], 2 * m + 1)
            if q['flip']:
                vrc[m] = stage[2 * m]
                vcc[m] = to_compact(2 * m + 1, q['n0'])
            else:
                vrc[m] = to_compact(2 * m, q['n0'])
                vcc[m] = stage[2 * m + 1]

        for i in range(2):
            signal_z(greet.at[i])
            pl.semaphore_wait(greet.at[i], n_z)

        n_rc = [(q['lanes'], 8) if q['flip'] else (8, q['lanes']) for q in mats]

        def send_rows(m):
            n_r = n_rc[m][0]
            for k in (3, 1, 2):
                remote(rmsg.at[m, pl.ds(0, n_r)], rrx.at[3 * m + k - 1, pl.ds(0, n_r)], a_s.at[0], ra_r.at[m],
                       model=lax.rem(z + k, n_model)).start()

        def send_cols(m):
            n_c = n_rc[m][1]
            if n_c == 8:
                remote(cmsg.at[m], csib.at[m], a_s.at[0], cs_r.at[m], data=sib).start()
                return
            for k in range(n_data - 1, 0, -1):
                remote(cmsg.at[m, pl.ds(0, n_c)], crx.at[7 * m + k - 1, pl.ds(0, n_c)], a_s.at[0], ca_r.at[m],
                       data=lax.rem(d + k, n_data)).start()

        def share_pair(m):
            wait_bytes(csib.at[m], cs_r.at[m])
            csib[m] = csib[m] + cmsg[m]
            for k, peer in enumerate((dd, dx, dy)):
                remote(csib.at[m], crx.at[7 * m + k], a_s.at[0], ca_r.at[m], data=peer).start()

        a_rows = sum(3 * r + (32 if c == 8 else 7 * c) for r, c in n_rc)

        def finish_sum(m):
            q = mats[m]
            half, n1 = q['half'], q['n1']
            acc1 = jnp.zeros((8, n1), jnp.float32)
            rsums = []
            fetch_done(whole[m, OWN])
            for h in range(2):
                arrived(m, 1 + h)
                arrived(m, 4 + h)
                rows = slice(h * half, (h + 1) * half)
                total = loc[m][OWN, rows, :] + rec[m][OWN, rows, :] + fxy[m][1 + h] + fxy[m][4 + h]
                upd[m][rows, :] = total
                sq = (total * total + 1e-30).reshape(half // 8, 8, n1)
                acc1 = acc1 + jnp.sum(sq, axis=0)
                rsums.append(jnp.sum(sq, axis=2, keepdims=True))
            sum1 = jnp.sum(acc1, axis=0, keepdims=True)
            msg0, msg1 = (cmsg, rmsg) if q['flip'] else (rmsg, cmsg)
            msg0[m] = compact(jnp.concatenate(rsums, axis=0))
            for k in range(q['lanes']):
                msg1[m, k:k + 1, :] = sum1[:, 128 * k:128 * k + 128]
            send_rows(m)
            send_cols(m)

        def apply_factors(m, bv, locrow):
            q = mats[m]
            n_r, n_c = n_rc[m]
            rtot = rmsg[m, 0:n_r, :]
            wait_bytes(rrx.at[pl.ds(3 * m, 3), pl.ds(0, n_r)], ra_r.at[m])
            for k in range(3):
                rtot = rtot + rrx[3 * m + k, 0:n_r, :]
            n_in = 3 if n_c == 8 else 7
            ctot = csib[m] if n_c == 8 else cmsg[m, 0:n_c, :]
            wait_bytes(crx.at[pl.ds(7 * m, n_in), pl.ds(0, n_c)], ca_r.at[m])
            for k in range(n_in):
                ctot = ctot + crx[7 * m + k, 0:n_c, :]
            vr = BETA * vrc[m, 0:n_r, :] + (1.0 - BETA) * (rtot * (1.0 / q['cols_t']))
            vc = BETA * vcc[m, 0:n_c, :] + (1.0 - BETA) * (ctot * (1.0 / q['rows_t']))
            ok = lane < q['groups']
            if q['flip']:
                vr_sum = jnp.sum(vr, axis=(0, 1), keepdims=True)
            else:
                vr_sum = jnp.sum(jnp.where(ok, vr, 0.0), axis=(0, 1), keepdims=True)
            mloc = vr_sum * (1.0 / q['rows_b'])
            if q['flip']:
                fac0 = lax.rsqrt(jnp.where(ok, vc, 1.0))
                fac1 = lax.rsqrt(vr / mloc)
                vcc[m] = vc
                stats[1 + 2 * m, 0:n_r, :] = vr
            else:
                fac0 = lax.rsqrt(jnp.where(ok, vr / mloc, 1.0))
                fac1 = lax.rsqrt(vc)
                vcc[m] = vr
                stats[1 + 2 * m, 0:n_c, :] = vc
            f1 = jnp.concatenate([jnp.broadcast_to(fac1[k:k + 1, :], (8, 128)) for k in range(q['lanes'])], axis=1)
            g_n = q['groups']
            f0 = expand(fac0, g_n)
            u = upd[m][...].reshape(g_n, 8, q['n1']) * f0 * f1[None]
            upd[m][...] = u.reshape(q['n0'], q['n1'])
            t_m = jnp.sum(jnp.sum(u * u, axis=0), axis=(0, 1), keepdims=True) * (1.0 / q['size'])
            bv = jnp.where(lane1 == m, t_m / mloc, bv)
            bv = jnp.where(lane1 == NM + m, vr_sum * (1.0 / (q['rows_t'] * n_model)), bv)
            locrow = jnp.where(lane1 == m, mloc, locrow)
            return bv, locrow

        locrow = jnp.ones((1, 128), jnp.float32)
        send_acc(0)
        send_raw(2)
        send_acc(1)
        finish_sum(0)
        send_raw(3)
        share_pair(0)
        send_acc(2)
        finish_sum(1)
        share_pair(1)
        send_acc(3)
        bv, locrow = apply_factors(0, bv, locrow)
        finish_sum(2)
        bv, locrow = apply_factors(1, bv, locrow)
        finish_sum(3)
        bv, locrow = apply_factors(2, bv, locrow)
        bv, locrow = apply_factors(3, bv, locrow)

        brx[0:1, :] = bv
        for kz in (3, 1, 2, 0):
            for kd in range(n_data - 1, -1, -1):
                if kz == 0 and kd == 0:
                    continue
                i = kz * n_data + kd
                remote(brx.at[pl.ds(0, 1), :], brx.at[pl.ds(i, 1), :], b_s.at[0], b_r.at[0],
                       data=lax.rem(d + kd, n_data), model=lax.rem(z + kz, n_model)).start()

        for m in range(NM):
            q = mats[m]
            wide = expand(vcc[m], q['groups'])
            for t in range(q['tiles']):
                n_t = min(128, q['n0'] - 128 * t)
                g_n = n_t // 8
                shape = (g_n, 8, 128)
                pick = (lax.broadcasted_iota(jnp.int32, shape, 2)
                        == 8 * lax.broadcasted_iota(jnp.int32, shape, 0) + lax.broadcasted_iota(jnp.int32, shape, 1))
                rows = jnp.sum(jnp.where(pick, wide[16 * t:16 * t + g_n], 0.0), axis=0)
                stats[2 + 2 * m, t:t + 1, :] = jnp.sum(rows, axis=0, keepdims=True)

        for m in range(NM):
            wait_bytes(rec[m], dd_s.at[m])
            wait_bytes(fxy[m], l_s.at[m])
        wait_bytes(loc[0].at[0, pl.ds(0, a_rows), :], a_s.at[0])
        wait_bytes(brx.at[pl.ds(1, n_model * n_data - 1), :], b_r.at[0])
        tot = jnp.broadcast_to(jnp.sum(brx[...], axis=0, keepdims=True), (8, 128))
        mean_vr = pltpu.roll(tot, 128 - NM, 1)
        u_rms = jnp.sqrt(mean_vr * tot)
        w_rms = jnp.sqrt(pltpu.roll(tot, 128 - 2 * NM, 1))
        fac = -(LR_REL * jnp.maximum(1e-3, w_rms)) * (jnp.sqrt(mean_vr) * lax.rsqrt(locrow))
        stats[0] = fac / jnp.maximum(1.0, u_rms)
        wait_bytes(brx.at[pl.ds(1, n_model * n_data - 1), :], b_s.at[0])

    f32 = jnp.float32
    dma = pltpu.SemaphoreType.DMA
    vm = pltpu.VMEM
    scratch = []
    scratch += [vm((4, q['n0'], q['n1']), f32) for q in mats]
    scratch += [vm((4, q['n0'], q['n1']), f32) for q in mats]
    scratch += [vm((6, q['half'], q['n1']), f32) for q in mats]
    scratch += [vm((r,), f32) for r in rows_b]
    scratch += [vm((c,), f32) for c in cols]
    scratch += [vm((mats[0]['n0'], mats[0]['n1']), f32)]
    tile = lambda *lead: vm((*lead, 8, 128), f32)
    scratch += [tile(NM), tile(3 * NM), tile(NM), tile(7 * NM), tile(NM), vm((n_model * n_data, 128), f32),
                tile(NM), tile(NM), tile(2 * NM)]
    scratch += [dma((13,)), dma((NM,)), dma((len(fetches),)), dma((NM,)), dma((6 * NM,)), dma((3 * NM,)),
                dma((1,)), dma((NM,)), dma((NM,)), dma((2,)), dma((1,)), dma((1,)), pltpu.SemaphoreType.REGULAR((2,))]
    blocks = [jax.ShapeDtypeStruct((q['n0'], q['n1']), f32) for q in mats]
    out_shape = blocks + blocks + [jax.ShapeDtypeStruct((1 + 2 * NM, 8, 128), f32)]
    vmem = pl.BlockSpec(memory_space=pltpu.VMEM)
    hbm = pl.BlockSpec(memory_space=pltpu.HBM)
    return pl.pallas_call(
        kernel, out_shape=out_shape, in_specs=[hbm] * 16, out_specs=[vmem] * len(out_shape),
        scratch_shapes=scratch,
        compiler_params=pltpu.CompilerParams(collective_id=0, has_side_effects=True,
                                             vmem_limit_bytes=28 * 1024 * 1024))


def make_apply_kernel(rows_b, cols, n_model, n_data):
    mats = layout_of(rows_b, cols, n_model, n_data)

    def kernel(*refs):
        upd, params, stats = refs[0:4], refs[4:8], refs[8]
        new, delta, vrow_out, vcol_out = refs[9:13], refs[13:17], refs[17:21], refs[21:25]
        bufs, vrbuf, vcbuf = refs[25:33], refs[33:37], refs[37:41]
        sem = refs[41]
        copies = []

        def put(src, dst, i):
            copies.append(pltpu.make_async_copy(src, dst, sem.at[i]))
            copies[-1].start()

        for m in range(NM):
            fac = stats[0, 0:1, m:m + 1]
            step = fac * upd[m][...]
            bufs[4 + m][...] = step
            put(bufs[4 + m], delta[m], 4 + m)
            bufs[m][...] = params[m][...] + step
            put(bufs[m], new[m], m)
        for m in range(NM):
            q = mats[m]
            out1, out0 = (vrbuf[m], vcbuf[m]) if q['flip'] else (vcbuf[m], vrbuf[m])
            for k in range(q['lanes']):
                out1[pl.ds(128 * k, 128)] = stats[1 + 2 * m, k:k + 1, :].reshape(128)
            for t in range(q['tiles']):
                n_t = min(128, q['n0'] - 128 * t)
                out0[pl.ds(128 * t, n_t)] = stats[2 + 2 * m, t:t + 1, 0:n_t].reshape(n_t)
            put(vrbuf[m], vrow_out[m], 8 + m)
            put(vcbuf[m], vcol_out[m], 12 + m)
        for cp in copies:
            cp.wait()

    f32 = jnp.float32
    vmem = pl.BlockSpec(memory_space=pltpu.VMEM)
    hbm = pl.BlockSpec(memory_space=pltpu.HBM)
    blocks = [jax.ShapeDtypeStruct((q['n0'], q['n1']), f32) for q in mats]
    out_shape = (blocks + blocks + [jax.ShapeDtypeStruct((r,), f32) for r in rows_b]
                 + [jax.ShapeDtypeStruct((c,), f32) for c in cols])
    scratch = [pltpu.VMEM((q['n0'], q['n1']), f32) for q in mats] * 2
    scratch += [pltpu.VMEM((n,), f32) for n in (*rows_b, *cols)] + [pltpu.SemaphoreType.DMA((16,))]
    return pl.pallas_call(
        kernel, out_shape=out_shape, in_specs=[vmem] * 9, out_specs=[hbm] * 16, scratch_shapes=scratch,
        compiler_params=pltpu.CompilerParams(vmem_limit_bytes=6 * 1024 * 1024))


def solution(mesh):
    n_data = mesh.shape['data']
    n_model = mesh.shape['model']
    mat_spec = P('data', 'model')
    in_specs = (P('data', None, 'model'), mat_spec, P('data'), P('model')) * NM
    out_specs = (mat_spec, mat_spec, P('data'), P('model')) * NM

    def per_device(*arrays):
        grads, params = arrays[0::4], arrays[1::4]
        rows_b = [p.shape[0] for p in params]
        cols = [p.shape[1] for p in params]
        mats = layout_of(rows_b, cols, n_model, n_data)
        view = lambda i, a: jnp.swapaxes(a, -1, -2) if mats[i]['flip'] else a
        grads = [view(i, g) for i, g in enumerate(grads)]
        params = [view(i, p) for i, p in enumerate(params)]
        pin = lambda a: pltpu.with_memory_space_constraint(a, pltpu.HBM)
        outs = make_reduce_kernel(rows_b, cols, n_model, n_data)(
            *map(pin, grads), *map(pin, params), *map(pin, arrays[2::4]), *map(pin, arrays[3::4]))
        res = make_apply_kernel(rows_b, cols, n_model, n_data)(*outs)
        flat = []
        for m in range(NM):
            flat += [view(m, res[m]), view(m, res[4 + m]), res[8 + m], res[12 + m]]
        return tuple(flat)

    return jax.shard_map(per_device, mesh=mesh, in_specs=in_specs, out_specs=out_specs, check_vma=False)
```

```python
import jax
import jax.numpy as jnp
from jax import lax
from jax.experimental import pallas as pl
from jax.experimental.pallas import tpu as pltpu
from jax.sharding import PartitionSpec as P

OPT_STEP = 3
BETA = 1.0 - OPT_STEP ** -0.8
LR_REL = min(0.01, OPT_STEP ** -0.5)
NM = 4
OWN, NX, NY, ND = 0, 1, 2, 3
FIRST_ROWS = 88
MESH_ID = pl.DeviceIdType.MESH


def layout_of(rows_b, cols, n_model, n_data):
    mats = []
    for r, c in zip(rows_b, cols):
        flip = c % 128 != 0
        n0, n1 = (c, r) if flip else (r, c)
        mats.append(dict(flip=flip, n0=n0, n1=n1, half=n0 // 2, groups=n0 // 8, tiles=-(-n0 // 128), lanes=n1 // 128,
                         rows_b=r, rows_t=r * n_data, cols_t=c * n_model,
                         size=float(r * n_data * c * n_model)))
    return mats


def make_reduce_kernel(rows_b, cols, n_model, n_data):
    mats = layout_of(rows_b, cols, n_model, n_data)
    halves = [q['half'] for q in mats]
    first = []
    for lo, hi in ((0, FIRST_ROWS), (FIRST_ROWS, halves[0])):
        first += [(0, ND, lo, hi - lo), (0, ND, halves[0] + lo, hi - lo)]
    group = {m: [(m, j, 0, mats[m]['n0']) for j in ((NX, NY, OWN) if m == 0 else (ND, NX, NY, OWN))] for m in range(NM)}

    def kernel(*refs):
        grads = refs[0:4]
        params = refs[4:8]
        vrows = refs[8:12]
        vcols = refs[12:16]
        upd = refs[16:20]
        wbuf = refs[20:24]
        stats = refs[24]
        sc = list(refs[25:])
        take = lambda n: [sc.pop(0) for _ in range(n)]
        loc, rec, fxy, vrbuf, vcbuf = (take(4) for _ in range(5))
        stg, rmsg, rrx, cmsg, crx, csib, brx, vrc, vcc, stage = take(10)
        ld_sem, dd_s, dd_r, l_s, l_r, a_s, a_r, cs_r, b_s, b_r, greet = take(11)

        z = lax.axis_index('model')
        d = lax.axis_index('data')
        core = lax.rem(d, 2)
        xx = lax.rem(d // 2, 2)
        yy = d // 4
        sib_step = 1 - 2 * core
        sib = d + sib_step
        dx = d + 2 - 4 * xx
        dy = d + 4 - 8 * yy
        dd = dx + 4 - 8 * yy
        owner = {OWN: d, NX: dx, NY: dy, ND: dd}

        def remote(src, dst, ssem, rsem, data=None, model=None):
            return pltpu.make_async_remote_copy(
                src_ref=src, dst_ref=dst, send_sem=ssem, recv_sem=rsem,
                device_id=(z if model is None else model, d if data is None else data),
                device_id_type=MESH_ID)

        def signal(sem, data=None, model=None):
            pl.semaphore_signal(
                sem, inc=1,
                device_id=(z if model is None else model, d if data is None else data),
                device_id_type=MESH_ID)

        def wait_bytes(ref, sem):
            pltpu.make_async_copy(ref, ref, sem).wait()

        barrier = pltpu.get_barrier_semaphore()
        for peer in (sib, dx, dy):
            signal(barrier, data=peer)
        up_ok = z < n_model - 1
        down_ok = z > 0

        def signal_z(sem):
            @pl.when(up_ok)
            def _():
                signal(sem, model=z + 1)

            @pl.when(down_ok)
            def _():
                signal(sem, model=z - 1)

        n_z = jnp.where(up_ok, 1, 0) + jnp.where(down_ok, 1, 0)
        signal_z(barrier)

        def block(who, f):
            m, j, r0, n = f
            q = mats[m]
            if q['flip']:
                cut = pl.ds(pl.multiple_of(who * q['n1'], 128), q['n1'])
                return grads[m].at[0, pl.ds(r0, n), cut]
            return grads[m].at[0, pl.ds(pl.multiple_of(who * q['n0'] + r0, 8), n), :]

        loads, dsend, stage_in = {}, {}, {}
        for f in first + group[0] + group[1] + group[2] + group[3]:
            m, j, r0, n = f
            slot = first.index(f) if f in first else 4 + m
            loads[f] = pltpu.make_async_copy(block(owner[j], f), loc[m].at[j, pl.ds(r0, n), :], ld_sem.at[slot])
            source = block(owner[j] + sib_step, f)
            if f in first:
                held = stg.at[pl.ds(r0, n), :]
                stage_in[f] = pltpu.make_async_copy(source, held, ld_sem.at[4 + slot])
                source = held
            dsend[f] = remote(source, rec[m].at[j, pl.ds(r0, n), :], dd_s.at[m], dd_r.at[slot], data=sib)

        def fetch(pieces):
            for f in pieces:
                dsend[f].start()
                loads[f].start()

        def fetch_done(m):
            some = pl.ds(0, 3) if m == 0 else pl.ds(0, 4)
            wait_bytes(loc[m].at[some], ld_sem.at[4 + m])
            wait_bytes(rec[m].at[some], dd_r.at[4 + m])

        def link_send(m, j, r0, n):
            h, off = (0, r0) if r0 < halves[m] else (1, r0 - halves[m])
            along_x = (j == ND and h == 0) or j == NX
            slot = (0 if along_x else 1) if j == ND else (2 if along_x else 4) + h
            return remote(loc[m].at[j, pl.ds(r0, n), :], fxy[m].at[slot, pl.ds(off, n), :],
                          l_s.at[m], l_r.at[2 * m + (0 if j == ND else 1)], data=dx if along_x else dy)

        def relays_in(m):
            wait_bytes(fxy[m].at[pl.ds(0, 2)], l_r.at[2 * m])

        def finals_in(m):
            wait_bytes(fxy[m].at[pl.ds(2, 4)], l_r.at[2 * m + 1])

        def pair_sum(m, j, r0, n, relay=None):
            total = loc[m][j, r0:r0 + n, :] + rec[m][j, r0:r0 + n, :]
            if relay is not None:
                total = total + fxy[m][relay]
            loc[m][j, r0:r0 + n, :] = total
            link_send(m, j, r0, n).start()

        def send_raw(m):
            n = halves[m]
            fetch_done(m)
            if m > 0:
                pair_sum(m, ND, 0, n)
                pair_sum(m, ND, n, n)
            pair_sum(m, NX, 0, n)
            pair_sum(m, NY, n, n)

        def send_acc(m):
            n = halves[m]
            relays_in(m)
            pair_sum(m, NY, 0, n, 0)
            pair_sum(m, NX, n, n, 1)

        for f in first:
            stage_in[f].start()
        for f in first:
            loads[f].start()
        pl.semaphore_wait(barrier, 3 + n_z)
        for f in first:
            stage_in[f].wait()
            dsend[f].start()
        fetch(group[0])
        for i, f in enumerate(first):
            loads[f].wait()
            dsend[f].wait_recv()
            pair_sum(*f)
            if i == 1:
                fetch(group[1])
        send_raw(0)
        fetch(group[2])
        send_raw(1)
        fetch(group[3])
        small = [pltpu.make_async_copy(vrows[m], vrbuf[m], ld_sem.at[m]) for m in range(NM)]
        small += [pltpu.make_async_copy(vcols[m], vcbuf[m], ld_sem.at[4 + m]) for m in range(2)]
        late = [pltpu.make_async_copy(params[m], wbuf[m], ld_sem.at[m]) for m in range(NM)]
        late += [pltpu.make_async_copy(vcols[m], vcbuf[m], ld_sem.at[2 + m]) for m in range(2, NM)]
        for turn in (small, late):
            for cp in turn:
                cp.start()
            for cp in turn:
                cp.wait()

        lane = lax.broadcasted_iota(jnp.int32, (8, 128), 1)
        sub = lax.broadcasted_iota(jnp.int32, (8, 128), 0)
        lane1 = lax.broadcasted_iota(jnp.int32, (1, 128), 1)

        def group_mask(g):
            shape = (g, 8, 128)
            return lax.broadcasted_iota(jnp.int32, shape, 2) == lax.broadcasted_iota(jnp.int32, shape, 0)

        def compact(values):
            return jnp.sum(jnp.where(group_mask(values.shape[0]), values, 0.0), axis=0)

        def expand(vec, g):
            return jnp.sum(jnp.where(group_mask(g), vec[None], 0.0), axis=2, keepdims=True)

        def rows_of(buf, n, i):
            stage[i] = jnp.zeros((8, 128), jnp.float32)
            for t in range(-(-n // 128)):
                n_t = min(128, n - 128 * t)
                stage[i, t:t + 1, 0:n_t] = buf[pl.ds(128 * t, n_t)].reshape(1, n_t)

        def to_compact(i, n):
            out = jnp.zeros((8, 128), jnp.float32)
            for t in range(-(-n // 128)):
                row = jnp.broadcast_to(stage[i, t:t + 1, :], (8, 128))
                for g in range(min(128, n - 128 * t) // 8):
                    col = jnp.sum(jnp.where(lane == 8 * g + sub, row, 0.0), axis=1, keepdims=True)
                    out = jnp.where(lane == 16 * t + g, col, out)
            return out

        bv = jnp.zeros((1, 128), jnp.float32)
        for m in range(NM):
            q = mats[m]
            w = wbuf[m][...]
            part = jnp.sum(w * w, axis=(0, 1), keepdims=True) * (1.0 / q['size'])
            bv = jnp.where(lane1 == 2 * NM + m, part, bv)
            rows_of(vrbuf[m], q['rows_b'], 2 * m)
            rows_of(vcbuf[m], cols[m], 2 * m + 1)
            if q['flip']:
                vrc[m] = stage[2 * m]
                vcc[m] = to_compact(2 * m + 1, q['n0'])
            else:
                vrc[m] = to_compact(2 * m, q['n0'])
                vcc[m] = stage[2 * m + 1]

        for i in range(2):
            signal_z(greet.at[i])
            pl.semaphore_wait(greet.at[i], n_z)

        n_rc = [(q['lanes'], 8) if q['flip'] else (8, q['lanes']) for q in mats]

        def send_rows(m):
            n_r = n_rc[m][0]
            for k in (3, 1, 2):
                remote(rmsg.at[m, pl.ds(0, n_r)], rrx.at[3 * m + k - 1, pl.ds(0, n_r)], a_s.at[0], a_r.at[m],
                       model=lax.rem(z + k, n_model)).start()

        def send_cols(m):
            n_c = n_rc[m][1]
            if n_c == 8:
                remote(cmsg.at[m], csib.at[m], a_s.at[0], cs_r.at[m], data=sib).start()
                return
            for k in range(n_data - 1, 0, -1):
                remote(cmsg.at[m, pl.ds(0, n_c)], crx.at[7 * m + k - 1, pl.ds(0, n_c)], a_s.at[0], a_r.at[m],
                       data=lax.rem(d + k, n_data)).start()

        def share_pair(m):
            wait_bytes(csib.at[m], cs_r.at[m])
            csib[m] = csib[m] + cmsg[m]
            for k, peer in enumerate((dd, dx, dy)):
                remote(csib.at[m], crx.at[7 * m + k], a_s.at[0], a_r.at[m], data=peer).start()

        a_rows = sum(3 * r + (32 if c == 8 else 7 * c) for r, c in n_rc)

        def finish_sum(m):
            q = mats[m]
            half, n1 = q['half'], q['n1']
            acc1 = jnp.zeros((8, n1), jnp.float32)
            rsums = []
            finals_in(m)
            for h in range(2):
                rows = slice(h * half, (h + 1) * half)
                total = loc[m][OWN, rows, :] + rec[m][OWN, rows, :] + fxy[m][2 + h] + fxy[m][4 + h]
                upd[m][rows, :] = total
                sq = (total * total + 1e-30).reshape(half // 8, 8, n1)
                acc1 = acc1 + jnp.sum(sq, axis=0)
                rsums.append(jnp.sum(sq, axis=2, keepdims=True))
            sum1 = jnp.sum(acc1, axis=0, keepdims=True)
            msg0, msg1 = (cmsg, rmsg) if q['flip'] else (rmsg, cmsg)
            msg0[m] = compact(jnp.concatenate(rsums, axis=0))
            for k in range(q['lanes']):
                msg1[m, k:k + 1, :] = sum1[:, 128 * k:128 * k + 128]
            send_rows(m)
            send_cols(m)

        def apply_factors(m, bv, locrow):
            q = mats[m]
            n_r, n_c = n_rc[m]
            rtot = rmsg[m, 0:n_r, :]
            n_in = 3 if n_c == 8 else 7
            wait_bytes(loc[0].at[0, pl.ds(0, 3 * n_r + n_in * n_c), :], a_r.at[m])
            for k in range(3):
                rtot = rtot + rrx[3 * m + k, 0:n_r, :]
            ctot = csib[m] if n_c == 8 else cmsg[m, 0:n_c, :]
            for k in range(n_in):
                ctot = ctot + crx[7 * m + k, 0:n_c, :]
            vr = BETA * vrc[m, 0:n_r, :] + (1.0 - BETA) * (rtot * (1.0 / q['cols_t']))
            vc = BETA * vcc[m, 0:n_c, :] + (1.0 - BETA) * (ctot * (1.0 / q['rows_t']))
            ok = lane < q['groups']
            if q['flip']:
                vr_sum = jnp.sum(vr, axis=(0, 1), keepdims=True)
            else:
                vr_sum = jnp.sum(jnp.where(ok, vr, 0.0), axis=(0, 1), keepdims=True)
            mloc = vr_sum * (1.0 / q['rows_b'])
            if q['flip']:
                fac0 = lax.rsqrt(jnp.where(ok, vc, 1.0))
                fac1 = lax.rsqrt(vr / mloc)
                vcc[m] = vc
                stats[1 + 2 * m, 0:n_r, :] = vr
            else:
                fac0 = lax.rsqrt(jnp.where(ok, vr / mloc, 1.0))
                fac1 = lax.rsqrt(vc)
                vcc[m] = vr
                stats[1 + 2 * m, 0:n_c, :] = vc
            f1 = jnp.concatenate([jnp.broadcast_to(fac1[k:k + 1, :], (8, 128)) for k in range(q['lanes'])], axis=1)
            g_n = q['groups']
            f0 = expand(fac0, g_n)
            u = upd[m][...].reshape(g_n, 8, q['n1']) * f0 * f1[None]
            upd[m][...] = u.reshape(q['n0'], q['n1'])
            t_m = jnp.sum(jnp.sum(u * u, axis=0), axis=(0, 1), keepdims=True) * (1.0 / q['size'])
            bv = jnp.where(lane1 == m, t_m / mloc, bv)
            bv = jnp.where(lane1 == NM + m, vr_sum * (1.0 / (q['rows_t'] * n_model)), bv)
            locrow = jnp.where(lane1 == m, mloc, locrow)
            return bv, locrow

        locrow = jnp.ones((1, 128), jnp.float32)
        send_acc(0)
        send_raw(2)
        send_acc(1)
        finish_sum(0)
        send_raw(3)
        share_pair(0)
        send_acc(2)
        finish_sum(1)
        share_pair(1)
        send_acc(3)
        bv, locrow = apply_factors(0, bv, locrow)
        finish_sum(2)
        bv, locrow = apply_factors(1, bv, locrow)
        finish_sum(3)
        bv, locrow = apply_factors(2, bv, locrow)
        bv, locrow = apply_factors(3, bv, locrow)

        brx[0:1, :] = bv
        for kz in (3, 1, 2, 0):
            for kd in range(n_data - 1, -1, -1):
                if kz == 0 and kd == 0:
                    continue
                i = kz * n_data + kd
                remote(brx.at[pl.ds(0, 1), :], brx.at[pl.ds(i, 1), :], b_s.at[0], b_r.at[0],
                       data=lax.rem(d + kd, n_data), model=lax.rem(z + kz, n_model)).start()

        for m in range(NM):
            q = mats[m]
            wide = expand(vcc[m], q['groups'])
            for t in range(q['tiles']):
                n_t = min(128, q['n0'] - 128 * t)
                g_n = n_t // 8
                shape = (g_n, 8, 128)
                pick = (lax.broadcasted_iota(jnp.int32, shape, 2)
                        == 8 * lax.broadcasted_iota(jnp.int32, shape, 0) + lax.broadcasted_iota(jnp.int32, shape, 1))
                rows = jnp.sum(jnp.where(pick, wide[16 * t:16 * t + g_n], 0.0), axis=0)
                stats[2 + 2 * m, t:t + 1, :] = jnp.sum(rows, axis=0, keepdims=True)

        for m in range(NM):
            wait_bytes(rec[m], dd_s.at[m])
            wait_bytes(fxy[m], l_s.at[m])
        wait_bytes(loc[0].at[0, pl.ds(0, a_rows), :], a_s.at[0])
        wait_bytes(brx.at[pl.ds(1, n_model * n_data - 1), :], b_r.at[0])
        tot = jnp.broadcast_to(jnp.sum(brx[...], axis=0, keepdims=True), (8, 128))
        mean_vr = pltpu.roll(tot, 128 - NM, 1)
        u_rms = jnp.sqrt(mean_vr * tot)
        w_rms = jnp.sqrt(pltpu.roll(tot, 128 - 2 * NM, 1))
        fac = -(LR_REL * jnp.maximum(1e-3, w_rms)) * (jnp.sqrt(mean_vr) * lax.rsqrt(locrow))
        stats[0] = fac / jnp.maximum(1.0, u_rms)
        wait_bytes(brx.at[pl.ds(1, n_model * n_data - 1), :], b_s.at[0])

    f32 = jnp.float32
    dma = pltpu.SemaphoreType.DMA
    vm = pltpu.VMEM
    scratch = []
    scratch += [vm((4, q['n0'], q['n1']), f32) for q in mats]
    scratch += [vm((4, q['n0'], q['n1']), f32) for q in mats]
    scratch += [vm((6, q['half'], q['n1']), f32) for q in mats]
    scratch += [vm((r,), f32) for r in rows_b]
    scratch += [vm((c,), f32) for c in cols]
    scratch += [vm((mats[0]['n0'], mats[0]['n1']), f32)]
    tile = lambda *lead: vm((*lead, 8, 128), f32)
    scratch += [tile(NM), tile(3 * NM), tile(NM), tile(7 * NM), tile(NM), vm((n_model * n_data, 128), f32),
                tile(NM), tile(NM), tile(2 * NM)]
    scratch += [dma((8,)), dma((NM,)), dma((8,)), dma((NM,)), dma((2 * NM,)), dma((1,)), dma((NM,)), dma((2,)),
                dma((1,)), dma((1,)), pltpu.SemaphoreType.REGULAR((2,))]
    blocks = [jax.ShapeDtypeStruct((q['n0'], q['n1']), f32) for q in mats]
    out_shape = blocks + blocks + [jax.ShapeDtypeStruct((1 + 2 * NM, 8, 128), f32)]
    vmem = pl.BlockSpec(memory_space=pltpu.VMEM)
    hbm = pl.BlockSpec(memory_space=pltpu.HBM)
    return pl.pallas_call(
        kernel, out_shape=out_shape, in_specs=[hbm] * 16, out_specs=[vmem] * len(out_shape),
        scratch_shapes=scratch,
        compiler_params=pltpu.CompilerParams(collective_id=0, has_side_effects=True,
                                             vmem_limit_bytes=28 * 1024 * 1024))


def make_apply_kernel(rows_b, cols, n_model, n_data):
    mats = layout_of(rows_b, cols, n_model, n_data)

    def kernel(*refs):
        upd, params, stats = refs[0:4], refs[4:8], refs[8]
        new, delta, vrow_out, vcol_out = refs[9:13], refs[13:17], refs[17:21], refs[21:25]
        bufs, vrbuf, vcbuf = refs[25:29], refs[29:33], refs[33:37]
        sem = refs[37]
        for m in range(NM):
            fac = stats[0, 0:1, m:m + 1]
            step = fac * upd[m][...]
            bufs[m][0] = step
            pltpu.make_async_copy(bufs[m].at[0], delta[m], sem.at[m]).start()
            bufs[m][1] = params[m][...] + step
            pltpu.make_async_copy(bufs[m].at[1], new[m], sem.at[m]).start()
        copies = []
        for m in range(NM):
            q = mats[m]
            out1, out0 = (vrbuf[m], vcbuf[m]) if q['flip'] else (vcbuf[m], vrbuf[m])
            for k in range(q['lanes']):
                out1[pl.ds(128 * k, 128)] = stats[1 + 2 * m, k:k + 1, :].reshape(128)
            for t in range(q['tiles']):
                n_t = min(128, q['n0'] - 128 * t)
                out0[pl.ds(128 * t, n_t)] = stats[2 + 2 * m, t:t + 1, 0:n_t].reshape(n_t)
            for i, (buf, out) in enumerate(((vrbuf[m], vrow_out[m]), (vcbuf[m], vcol_out[m]))):
                copies.append(pltpu.make_async_copy(buf, out, sem.at[NM + 2 * m + i]))
                copies[-1].start()
        for m in range(NM):
            pltpu.make_async_copy(bufs[m], bufs[m], sem.at[m]).wait()
        for cp in copies:
            cp.wait()

    f32 = jnp.float32
    vmem = pl.BlockSpec(memory_space=pltpu.VMEM)
    hbm = pl.BlockSpec(memory_space=pltpu.HBM)
    blocks = [jax.ShapeDtypeStruct((q['n0'], q['n1']), f32) for q in mats]
    out_shape = (blocks + blocks + [jax.ShapeDtypeStruct((r,), f32) for r in rows_b]
                 + [jax.ShapeDtypeStruct((c,), f32) for c in cols])
    scratch = [pltpu.VMEM((2, q['n0'], q['n1']), f32) for q in mats]
    scratch += [pltpu.VMEM((n,), f32) for n in (*rows_b, *cols)] + [pltpu.SemaphoreType.DMA((3 * NM,))]
    return pl.pallas_call(
        kernel, out_shape=out_shape, in_specs=[vmem] * 9, out_specs=[hbm] * 16, scratch_shapes=scratch,
        compiler_params=pltpu.CompilerParams(vmem_limit_bytes=6 * 1024 * 1024))


def solution(mesh):
    n_data = mesh.shape['data']
    n_model = mesh.shape['model']
    mat_spec = P('data', 'model')
    in_specs = (P('data', None, 'model'), mat_spec, P('data'), P('model')) * NM
    out_specs = (mat_spec, mat_spec, P('data'), P('model')) * NM

    def per_device(*arrays):
        grads, params = arrays[0::4], arrays[1::4]
        rows_b = [p.shape[0] for p in params]
        cols = [p.shape[1] for p in params]
        mats = layout_of(rows_b, cols, n_model, n_data)
        view = lambda i, a: jnp.swapaxes(a, -1, -2) if mats[i]['flip'] else a
        grads = [view(i, g) for i, g in enumerate(grads)]
        params = [view(i, p) for i, p in enumerate(params)]
        pin = lambda a: pltpu.with_memory_space_constraint(a, pltpu.HBM)
        outs = make_reduce_kernel(rows_b, cols, n_model, n_data)(
            *map(pin, grads), *map(pin, params), *map(pin, arrays[2::4]), *map(pin, arrays[3::4]))
        res = make_apply_kernel(rows_b, cols, n_model, n_data)(*outs)
        flat = []
        for m in range(NM):
            flat += [view(m, res[m]), view(m, res[4 + m]), res[8 + m], res[12 + m]]
        return tuple(flat)

    return jax.shard_map(per_device, mesh=mesh, in_specs=in_specs, out_specs=out_specs, check_vma=False)
```

```python
import jax
import jax.numpy as jnp
from jax import lax
from jax.experimental import pallas as pl
from jax.experimental.pallas import tpu as pltpu
from jax.sharding import PartitionSpec as P

OPT_STEP = 3
BETA = 1.0 - OPT_STEP ** -0.8
LR_REL = min(0.01, OPT_STEP ** -0.5)
NM = 4
OWN, NX, NY, ND = 0, 1, 2, 3
FIRST_ROWS = 88
PARTS = 4
LANES = 128
TILE = (8, LANES)
MIB = 1024 * 1024
MESH_ID = pl.DeviceIdType.MESH


def layout_of(rows_b, cols, n_model, n_data):
    mats = []
    for r, c in zip(rows_b, cols):
        flip = c % LANES != 0
        n0, n1 = (c, r) if flip else (r, c)
        mats.append(dict(flip=flip, n0=n0, n1=n1, half=n0 // 2, groups=n0 // 8, tiles=-(-n0 // LANES), lanes=n1 // LANES,
                         rows_b=r, rows_t=r * n_data, cols_t=c * n_model,
                         size=float(r * n_data * c * n_model)))
    return mats


def make_reduce_kernel(rows_b, cols, n_model, n_data):
    mats = layout_of(rows_b, cols, n_model, n_data)
    halves = [q['half'] for q in mats]
    n_rc = [(q['lanes'], 8) if q['flip'] else (8, q['lanes']) for q in mats]
    sent_rows = sum(7 * q['n0'] * q['lanes'] for q in mats) + n_model * n_data - 1
    sent_rows += sum(3 * r + (24 if c == 8 else 7 * c) for r, c in n_rc)
    first = []
    for lo, hi in ((0, FIRST_ROWS), (FIRST_ROWS, halves[0])):
        first += [(0, ND, lo, hi - lo), (0, ND, halves[0] + lo, hi - lo)]
    group = {m: [(m, j, 0, mats[m]['n0']) for j in ((NX, NY, OWN) if m == 0 else (ND, NX, NY, OWN))] for m in range(NM)}

    def kernel(*refs):
        grads = refs[0:4]
        params = refs[4:8]
        vrows = refs[8:12]
        vcols = refs[12:16]
        upd = refs[16:20]
        wbuf = refs[20:24]
        stats = refs[24]
        sc = list(refs[25:])
        take = lambda n: [sc.pop(0) for _ in range(n)]
        loc, rec, fxy, vrbuf, vcbuf = (take(4) for _ in range(5))
        stg, rmsg, rrx, cmsg, crx, csib, chalf, brx, vrc, vcc, stage, sent = take(12)
        ld_sem, dd_r, l_r, ra_r, ca_r, cs_r, cm_r, b_r, s_sem, greet = take(10)

        z = lax.axis_index('model')
        d = lax.axis_index('data')
        core = lax.rem(d, 2)
        xx = lax.rem(d // 2, 2)
        yy = d // 4
        sib_step = 1 - 2 * core
        sib = d + sib_step
        dx = d + 2 - 4 * xx
        dy = d + 4 - 8 * yy
        dd = dx + 4 - 8 * yy
        owner = {OWN: d, NX: dx, NY: dy, ND: dd}

        def flip_d(k):
            return d + (k % 2) * sib_step + (k // 2 % 2) * (2 - 4 * xx) + (k // 4) * (4 - 8 * yy)

        def flip_z(k):
            return z + (k % 2) * (1 - 2 * lax.rem(z, 2)) + (k // 2) * (2 - 4 * (z // 2))

        def remote(src, dst, ssem, rsem, data=None, model=None):
            return pltpu.make_async_remote_copy(
                src_ref=src, dst_ref=dst, send_sem=ssem, recv_sem=rsem,
                device_id=(z if model is None else model, d if data is None else data),
                device_id_type=MESH_ID)

        def signal(sem, data=None, model=None):
            pl.semaphore_signal(
                sem, inc=1,
                device_id=(z if model is None else model, d if data is None else data),
                device_id_type=MESH_ID)

        def wait_bytes(ref, sem):
            pltpu.make_async_copy(ref, ref, sem).wait()

        barrier = pltpu.get_barrier_semaphore()
        first_core, second_core = core == 0, core == 1
        up_ok = z < n_model - 1
        down_ok = z > 0
        n_z = jnp.where(up_ok, 1, 0) + jnp.where(down_ok, 1, 0)

        def signal_z(sem, data=None, also=None):
            @pl.when(up_ok if also is None else up_ok & also)
            def _():
                signal(sem, data=data, model=z + 1)

            @pl.when(down_ok if also is None else down_ok & also)
            def _():
                signal(sem, data=data, model=z - 1)

        @pl.when(second_core)
        def _():
            signal(barrier, data=sib)

        def block(who, f):
            m, j, r0, n = f
            q = mats[m]
            if q['flip']:
                cut = pl.ds(pl.multiple_of(who * q['n1'], LANES), q['n1'])
                return grads[m].at[0, pl.ds(r0, n), cut]
            return grads[m].at[0, pl.ds(pl.multiple_of(who * q['n0'] + r0, 8), n), :]

        loads, dsend, stage_in = {}, {}, {}
        for f in first + group[0] + group[1] + group[2] + group[3]:
            m, j, r0, n = f
            slot = first.index(f) if f in first else 4 + m
            loads[f] = pltpu.make_async_copy(block(owner[j], f), loc[m].at[j, pl.ds(r0, n), :], ld_sem.at[slot])
            source = block(owner[j] + sib_step, f)
            if f in first:
                held = stg.at[pl.ds(r0, n), :]
                stage_in[f] = pltpu.make_async_copy(source, held, ld_sem.at[4 + slot])
                source = held
            dsend[f] = remote(source, rec[m].at[j, pl.ds(r0, n), :], s_sem.at[0], dd_r.at[slot], data=sib)

        def fetch(pieces):
            for f in pieces:
                dsend[f].start()
                loads[f].start()

        def fetch_done(m):
            some = pl.ds(0, 3) if m == 0 else pl.ds(0, 4)
            wait_bytes(loc[m].at[some], ld_sem.at[4 + m])
            wait_bytes(rec[m].at[some], dd_r.at[4 + m])

        def link_send(m, j, r0, n):
            h, off = (0, r0) if r0 < halves[m] else (1, r0 - halves[m])
            along_x = (j == ND and h == 0) or j == NX
            slot = (0 if along_x else 1) if j == ND else (2 if along_x else 4) + h
            return remote(loc[m].at[j, pl.ds(r0, n), :], fxy[m].at[slot, pl.ds(off, n), :],
                          s_sem.at[0], l_r.at[2 * m + (0 if j == ND else 1)], data=dx if along_x else dy)

        def relays_in(m):
            wait_bytes(fxy[m].at[pl.ds(0, 2)], l_r.at[2 * m])

        def finals_in(m):
            wait_bytes(fxy[m].at[pl.ds(2, 4)], l_r.at[2 * m + 1])

        def pair_sum(m, j, r0, n, relay=None):
            total = loc[m][j, r0:r0 + n, :] + rec[m][j, r0:r0 + n, :]
            if relay is not None:
                total = total + fxy[m][relay]
            loc[m][j, r0:r0 + n, :] = total
            link_send(m, j, r0, n).start()

        def send_raw(m):
            n = halves[m]
            fetch_done(m)
            if m > 0:
                pair_sum(m, ND, 0, n)
                pair_sum(m, ND, n, n)
            pair_sum(m, NX, 0, n)
            pair_sum(m, NY, n, n)

        def send_acc(m):
            n = halves[m]
            relays_in(m)
            pair_sum(m, NY, 0, n, 0)
            pair_sum(m, NX, n, n, 1)

        for f in first:
            stage_in[f].start()
            loads[f].start()

        @pl.when(first_core)
        def _():
            pl.semaphore_wait(barrier, 1)
            signal(barrier, data=dx + 1)
            signal(barrier, data=dy + 1)
            signal(greet.at[2], data=sib)

        signal_z(barrier, data=sib, also=first_core)

        @pl.when(second_core)
        def _():
            pl.semaphore_wait(greet.at[2], 1)

        for f in first:
            stage_in[f].wait()
            dsend[f].start()

        @pl.when(second_core)
        def _():
            pl.semaphore_wait(barrier, 2 + n_z)
            signal(greet.at[3], data=sib)

        @pl.when(first_core)
        def _():
            pl.semaphore_wait(greet.at[3], 1)

        for i, f in enumerate(first):
            loads[f].wait()
            dsend[f].wait_recv()
            pair_sum(*f)
            if i == 1:
                fetch(group[0])
        fetch(group[1])
        send_raw(0)
        fetch(group[2])
        send_raw(1)
        fetch(group[3])
        small = [pltpu.make_async_copy(vrows[m], vrbuf[m], ld_sem.at[m]) for m in range(NM)]
        small += [pltpu.make_async_copy(vcols[m], vcbuf[m], ld_sem.at[4 + m]) for m in range(2)]
        late = [pltpu.make_async_copy(params[m], wbuf[m], ld_sem.at[m]) for m in range(NM)]
        late += [pltpu.make_async_copy(vcols[m], vcbuf[m], ld_sem.at[2 + m]) for m in range(2, NM)]
        for turn in (small, late):
            for cp in turn:
                cp.start()
            for cp in turn:
                cp.wait()

        lane = lax.broadcasted_iota(jnp.int32, TILE, 1)
        sub = lax.broadcasted_iota(jnp.int32, TILE, 0)
        lane1 = lax.broadcasted_iota(jnp.int32, (1, LANES), 1)

        def group_mask(g):
            shape = (g, 8, LANES)
            return lax.broadcasted_iota(jnp.int32, shape, 2) == lax.broadcasted_iota(jnp.int32, shape, 0)

        def compact(values):
            return jnp.sum(jnp.where(group_mask(values.shape[0]), values, 0.0), axis=0)

        def expand(vec, g):
            return jnp.sum(jnp.where(group_mask(g), vec[None], 0.0), axis=2, keepdims=True)

        def rows_of(buf, n, i):
            stage[i] = jnp.zeros(TILE, jnp.float32)
            for t in range(-(-n // LANES)):
                n_t = min(LANES, n - LANES * t)
                stage[i, t:t + 1, 0:n_t] = buf[pl.ds(LANES * t, n_t)].reshape(1, n_t)

        def to_compact(i, n):
            out = jnp.zeros(TILE, jnp.float32)
            for t in range(-(-n // LANES)):
                row = jnp.broadcast_to(stage[i, t:t + 1, :], TILE)
                for g in range(min(LANES, n - LANES * t) // 8):
                    col = jnp.sum(jnp.where(lane == 8 * g + sub, row, 0.0), axis=1, keepdims=True)
                    out = jnp.where(lane == 16 * t + g, col, out)
            return out

        bv = jnp.zeros((1, LANES), jnp.float32)
        for m in range(NM):
            q = mats[m]
            w = wbuf[m][...]
            part = jnp.sum(w * w, axis=(0, 1), keepdims=True) * (1.0 / q['size'])
            bv = jnp.where(lane1 == 2 * NM + m, part, bv)
            rows_of(vrbuf[m], q['rows_b'], 2 * m)
            rows_of(vcbuf[m], cols[m], 2 * m + 1)
            if q['flip']:
                vrc[m] = stage[2 * m]
                vcc[m] = to_compact(2 * m + 1, q['n0'])
            else:
                vrc[m] = to_compact(2 * m, q['n0'])
                vcc[m] = stage[2 * m + 1]

        for i in range(2):
            signal_z(greet.at[i])
            pl.semaphore_wait(greet.at[i], n_z)

        def send_rows(m):
            n_r = n_rc[m][0]
            for k in (3, 2, 1):
                remote(rmsg.at[m, pl.ds(0, n_r)], rrx.at[3 * m + k - 1, pl.ds(0, n_r)], s_sem.at[0], ra_r.at[m],
                       model=flip_z(k)).start()

        def send_cols(m, ks):
            n_c = n_rc[m][1]
            for k in ks:
                remote(cmsg.at[m, pl.ds(0, n_c)], crx.at[7 * m + k - 1, pl.ds(0, n_c)], s_sem.at[0], ca_r.at[m],
                       data=flip_d(k)).start()

        def share_pair(m):
            wait_bytes(csib.at[m], cs_r.at[m])
            mine = jnp.where(core == 0, csib[m, 0:4, :] + cmsg[m, 0:4, :], csib[m, 4:8, :] + cmsg[m, 4:8, :])
            chalf[m, 0] = mine
            for k, peer in enumerate((dd, dx, dy)):
                remote(chalf.at[m, 0], chalf.at[m, 1 + k], s_sem.at[0], ca_r.at[m], data=peer).start()

        def merge_pair(m):
            wait_bytes(chalf.at[m, pl.ds(1, 3)], ca_r.at[m])
            chalf[m, 4] = chalf[m, 0] + chalf[m, 1] + chalf[m, 2] + chalf[m, 3]
            remote(chalf.at[m, 4], chalf.at[m, 5], s_sem.at[0], cm_r.at[m], data=sib).start()

        def merged(m):
            wait_bytes(chalf.at[m, 5], cm_r.at[m])
            mine, other = chalf[m, 4], chalf[m, 5]
            return jnp.concatenate([jnp.where(core == 0, mine, other), jnp.where(core == 0, other, mine)], axis=0)


        def finish_sum(m):
            q = mats[m]
            half, n1 = q['half'], q['n1']
            acc1 = jnp.zeros((8, n1), jnp.float32)
            rsums = []
            finals_in(m)
            for h in range(2):
                rows = slice(h * half, (h + 1) * half)
                total = loc[m][OWN, rows, :] + rec[m][OWN, rows, :] + fxy[m][2 + h] + fxy[m][4 + h]
                upd[m][rows, :] = total
                sq = (total * total + 1e-30).reshape(half // 8, 8, n1)
                acc1 = acc1 + jnp.sum(sq, axis=0)
                rsums.append(jnp.sum(sq, axis=2, keepdims=True))
            sum1 = jnp.sum(acc1, axis=0, keepdims=True)
            msg0, msg1 = (cmsg, rmsg) if q['flip'] else (rmsg, cmsg)
            for k in range(q['lanes']):
                msg1[m, k:k + 1, :] = sum1[:, LANES * k:LANES * k + LANES]
            if not q['flip']:
                send_cols(m, (6, 7, 2, 4, 3, 5, 1))
            msg0[m] = compact(jnp.concatenate(rsums, axis=0))
            send_rows(m)
            if q['flip']:
                remote(cmsg.at[m], csib.at[m], s_sem.at[0], cs_r.at[m], data=sib).start()

        def apply_factors(m, bv, locrow):
            q = mats[m]
            n_r, n_c = n_rc[m]
            g_n, n1 = q['groups'], q['n1']
            ok = lane < g_n

            def along0(fac):
                return expand(fac, g_n)

            def along1(fac):
                wide = [jnp.broadcast_to(fac[k:k + 1, :], TILE) for k in range(q['lanes'])]
                return jnp.concatenate(wide, axis=1)[None]

            rtot = rmsg[m, 0:n_r, :]
            wait_bytes(loc[0].at[0, pl.ds(0, 3 * n_r), :], ra_r.at[m])
            for k in range(3):
                rtot = rtot + rrx[3 * m + k, 0:n_r, :]
            vr = BETA * vrc[m, 0:n_r, :] + (1.0 - BETA) * (rtot * (1.0 / q['cols_t']))
            vr_sum = jnp.sum(vr if q['flip'] else jnp.where(ok, vr, 0.0), axis=(0, 1), keepdims=True)
            mloc = vr_sum * (1.0 / q['rows_b'])
            inv_mloc = 1.0 / mloc
            rfac = lax.rsqrt(vr / mloc) if q['flip'] else lax.rsqrt(jnp.where(ok, vr / mloc, 1.0))
            part = upd[m][...].reshape(g_n, 8, n1) * (along1 if q['flip'] else along0)(rfac)
            if n_c == 8:
                ctot = merged(m)
            else:
                ctot = cmsg[m, 0:n_c, :]
                wait_bytes(loc[0].at[0, pl.ds(0, 7 * n_c), :], ca_r.at[m])
                for k in range(7):
                    ctot = ctot + crx[7 * m + k, 0:n_c, :]
            vc = BETA * vcc[m, 0:n_c, :] + (1.0 - BETA) * (ctot * (1.0 / q['rows_t']))
            cfac = lax.rsqrt(jnp.where(ok, vc, 1.0)) if q['flip'] else lax.rsqrt(vc)
            u = part * (along0 if q['flip'] else along1)(cfac)
            t_m = jnp.sum(jnp.sum(u * u, axis=0), axis=(0, 1), keepdims=True)
            upd[m][...] = u.reshape(q['n0'], n1)
            vcc[m] = vc if q['flip'] else vr
            stats[1 + 2 * m, 0:q['lanes'], :] = vr if q['flip'] else vc
            bv = jnp.where(lane1 == NM + m, vr_sum * (1.0 / (q['rows_t'] * n_model)), bv)
            bv = jnp.where(lane1 == m, (t_m * (1.0 / q['size'])) * inv_mloc, bv)
            locrow = jnp.where(lane1 == m, mloc, locrow)
            return bv, locrow

        locrow = jnp.ones((1, LANES), jnp.float32)
        send_acc(0)
        send_raw(2)
        send_acc(1)
        finish_sum(0)
        send_raw(3)
        share_pair(0)
        send_acc(2)
        finish_sum(1)
        share_pair(1)
        send_acc(3)
        merge_pair(0)
        bv, locrow = apply_factors(0, bv, locrow)
        finish_sum(2)
        merge_pair(1)
        finish_sum(3)
        bv, locrow = apply_factors(1, bv, locrow)
        bv, locrow = apply_factors(2, bv, locrow)
        bv, locrow = apply_factors(3, bv, locrow)

        brx[0:1, :] = bv
        for kz in (3, 2, 1, 0):
            for kd in range(n_data - 1, -1, -1):
                if kz == 0 and kd == 0:
                    continue
                i = kz * n_data + kd
                remote(brx.at[pl.ds(0, 1), :], brx.at[pl.ds(i, 1), :], s_sem.at[0], b_r.at[0],
                       data=flip_d(kd), model=flip_z(kz)).start()

        for m in range(NM):
            q = mats[m]
            wide = expand(vcc[m], q['groups'])
            for t in range(q['tiles']):
                n_t = min(LANES, q['n0'] - LANES * t)
                g_n = n_t // 8
                shape = (g_n, 8, LANES)
                pick = (lax.broadcasted_iota(jnp.int32, shape, 2)
                        == 8 * lax.broadcasted_iota(jnp.int32, shape, 0) + lax.broadcasted_iota(jnp.int32, shape, 1))
                rows = jnp.sum(jnp.where(pick, wide[16 * t:16 * t + g_n], 0.0), axis=0)
                stats[2 + 2 * m, t:t + 1, :] = jnp.sum(rows, axis=0, keepdims=True)

        wait_bytes(brx.at[pl.ds(1, n_model * n_data - 1), :], b_r.at[0])
        tot = jnp.broadcast_to(jnp.sum(brx[...], axis=0, keepdims=True), TILE)
        mean_vr = pltpu.roll(tot, LANES - NM, 1)
        u_rms = jnp.sqrt(mean_vr * tot)
        w_rms = jnp.sqrt(pltpu.roll(tot, LANES - 2 * NM, 1))
        fac = -(LR_REL * jnp.maximum(1e-3, w_rms)) * (jnp.sqrt(mean_vr) * lax.rsqrt(locrow))
        stats[0] = fac / jnp.maximum(1.0, u_rms)
        wait_bytes(sent, s_sem.at[0])

    f32 = jnp.float32
    dma = pltpu.SemaphoreType.DMA
    vm = pltpu.VMEM
    scratch = []
    scratch += [vm((4, q['n0'], q['n1']), f32) for q in mats]
    scratch += [vm((4, q['n0'], q['n1']), f32) for q in mats]
    scratch += [vm((6, q['half'], q['n1']), f32) for q in mats]
    scratch += [vm((r,), f32) for r in rows_b]
    scratch += [vm((c,), f32) for c in cols]
    scratch += [vm((mats[0]['n0'], mats[0]['n1']), f32)]
    tile = lambda *lead: vm((*lead, 8, LANES), f32)
    scratch += [tile(NM), tile(3 * NM), tile(NM), tile(7 * NM), tile(2), vm((2, 6, 4, LANES), f32), vm((n_model * n_data, LANES), f32),
                tile(NM), tile(NM), tile(2 * NM), vm((sent_rows, LANES), f32)]
    scratch += [dma((8,)), dma((8,)), dma((2 * NM,)), dma((NM,)), dma((NM,)), dma((2,)), dma((2,)), dma((1,)), dma((1,)),
                pltpu.SemaphoreType.REGULAR((4,))]
    blocks = [jax.ShapeDtypeStruct((q['n0'], q['n1']), f32) for q in mats]
    out_shape = blocks + blocks + [jax.ShapeDtypeStruct((1 + 2 * NM, 8, LANES), f32)]
    vmem = pl.BlockSpec(memory_space=pltpu.VMEM)
    hbm = pl.BlockSpec(memory_space=pltpu.HBM)
    return pl.pallas_call(
        kernel, out_shape=out_shape, in_specs=[hbm] * 16, out_specs=[vmem] * len(out_shape),
        scratch_shapes=scratch,
        compiler_params=pltpu.CompilerParams(collective_id=0, has_side_effects=True,
                                             vmem_limit_bytes=36 * MIB))


def make_apply_kernel(rows_b, cols, n_model, n_data):
    mats = layout_of(rows_b, cols, n_model, n_data)

    def kernel(*refs):
        upd, params, stats = refs[0:4], refs[4:8], refs[8]
        new, delta, vrow_out, vcol_out = refs[9:13], refs[13:17], refs[17:21], refs[21:25]
        bufs, vrbuf, vcbuf = refs[25:29], refs[29:33], refs[33:37]
        sem = refs[37]
        for m in range(NM):
            fac = stats[0, 0:1, m:m + 1]
            n = mats[m]['n0'] // PARTS
            for i in range(PARTS):
                rows = slice(i * n, i * n + n)
                step = fac * upd[m][rows, :]
                bufs[m][0, rows, :] = step
                pltpu.make_async_copy(bufs[m].at[0, rows], delta[m].at[rows], sem.at[m]).start()
                bufs[m][1, rows, :] = params[m][rows, :] + step
                pltpu.make_async_copy(bufs[m].at[1, rows], new[m].at[rows], sem.at[m]).start()
        copies = []
        for m in range(NM):
            q = mats[m]
            out1, out0 = (vrbuf[m], vcbuf[m]) if q['flip'] else (vcbuf[m], vrbuf[m])
            for k in range(q['lanes']):
                out1[pl.ds(LANES * k, LANES)] = stats[1 + 2 * m, k:k + 1, :].reshape(LANES)
            for t in range(q['tiles']):
                n_t = min(LANES, q['n0'] - LANES * t)
                out0[pl.ds(LANES * t, n_t)] = stats[2 + 2 * m, t:t + 1, 0:n_t].reshape(n_t)
            for i, (buf, out) in enumerate(((vrbuf[m], vrow_out[m]), (vcbuf[m], vcol_out[m]))):
                copies.append(pltpu.make_async_copy(buf, out, sem.at[NM + 2 * m + i]))
                copies[-1].start()
        for m in range(NM):
            pltpu.make_async_copy(bufs[m], bufs[m], sem.at[m]).wait()
        for cp in copies:
            cp.wait()

    f32 = jnp.float32
    vmem = pl.BlockSpec(memory_space=pltpu.VMEM)
    hbm = pl.BlockSpec(memory_space=pltpu.HBM)
    blocks = [jax.ShapeDtypeStruct((q['n0'], q['n1']), f32) for q in mats]
    out_shape = (blocks + blocks + [jax.ShapeDtypeStruct((r,), f32) for r in rows_b]
                 + [jax.ShapeDtypeStruct((c,), f32) for c in cols])
    scratch = [pltpu.VMEM((2, q['n0'], q['n1']), f32) for q in mats]
    scratch += [pltpu.VMEM((n,), f32) for n in (*rows_b, *cols)] + [pltpu.SemaphoreType.DMA((3 * NM,))]
    return pl.pallas_call(
        kernel, out_shape=out_shape, in_specs=[vmem] * 9, out_specs=[hbm] * 16, scratch_shapes=scratch,
        compiler_params=pltpu.CompilerParams(vmem_limit_bytes=6 * MIB))


def solution(mesh):
    n_data = mesh.shape['data']
    n_model = mesh.shape['model']
    mat_spec = P('data', 'model')
    in_specs = (P('data', None, 'model'), mat_spec, P('data'), P('model')) * NM
    out_specs = (mat_spec, mat_spec, P('data'), P('model')) * NM

    def per_device(*arrays):
        grads, params = arrays[0::4], arrays[1::4]
        rows_b = [p.shape[0] for p in params]
        cols = [p.shape[1] for p in params]
        mats = layout_of(rows_b, cols, n_model, n_data)
        view = lambda i, a: jnp.swapaxes(a, -1, -2) if mats[i]['flip'] else a
        grads = [view(i, g) for i, g in enumerate(grads)]
        params = [view(i, p) for i, p in enumerate(params)]
        pin = lambda a: pltpu.with_memory_space_constraint(a, pltpu.HBM)
        outs = make_reduce_kernel(rows_b, cols, n_model, n_data)(
            *map(pin, grads), *map(pin, params), *map(pin, arrays[2::4]), *map(pin, arrays[3::4]))
        res = make_apply_kernel(rows_b, cols, n_model, n_data)(*outs)
        flat = []
        for m in range(NM):
            flat += [view(m, res[m]), view(m, res[4 + m]), res[8 + m], res[12 + m]]
        return tuple(flat)

    return jax.shard_map(per_device, mesh=mesh, in_specs=in_specs, out_specs=out_specs, check_vma=False)
```

```python
import jax
import jax.numpy as jnp
from jax import lax
from jax.experimental import pallas as pl
from jax.experimental.pallas import tpu as pltpu
from jax.sharding import PartitionSpec as P

OPT_STEP = 3
BETA = 1.0 - OPT_STEP ** -0.8
LR_REL = min(0.01, OPT_STEP ** -0.5)
NM = 4
OWN, NX, NY, ND = 0, 1, 2, 3
FIRST_ROWS = 88
PARTS = 4
LEAD_NS = 200
LANES = 128
TILE = (8, LANES)
MIB = 1024 * 1024
MESH_ID = pl.DeviceIdType.MESH


def layout_of(rows_b, cols, n_model, n_data):
    mats = []
    for r, c in zip(rows_b, cols):
        flip = c % LANES != 0
        n0, n1 = (c, r) if flip else (r, c)
        mats.append(dict(flip=flip, n0=n0, n1=n1, half=n0 // 2, groups=n0 // 8, tiles=-(-n0 // LANES), lanes=n1 // LANES,
                         rows_b=r, rows_t=r * n_data, cols_t=c * n_model,
                         size=float(r * n_data * c * n_model)))
    return mats


def make_reduce_kernel(rows_b, cols, n_model, n_data):
    mats = layout_of(rows_b, cols, n_model, n_data)
    halves = [q['half'] for q in mats]
    n_rc = [(q['lanes'], 8) if q['flip'] else (8, q['lanes']) for q in mats]
    sent_rows = sum(7 * q['n0'] * q['lanes'] for q in mats) + n_model * n_data - 1
    sent_rows += sum(3 * r + (24 if c == 8 else 7 * c) for r, c in n_rc)
    first = []
    for lo, hi in ((0, FIRST_ROWS), (FIRST_ROWS, halves[0])):
        first += [(0, ND, lo, hi - lo), (0, ND, halves[0] + lo, hi - lo)]
    group = {m: [(m, j, 0, mats[m]['n0']) for j in ((NX, NY, OWN) if m == 0 else (ND, NX, NY, OWN))] for m in range(NM)}

    def kernel(*refs):
        grads = refs[0:4]
        params = refs[4:8]
        vrows = refs[8:12]
        vcols = refs[12:16]
        upd = refs[16:20]
        wbuf = refs[20:24]
        stats = refs[24]
        sc = list(refs[25:])
        take = lambda n: [sc.pop(0) for _ in range(n)]
        loc, rec, fxy, vrbuf, vcbuf = (take(4) for _ in range(5))
        stg, rmsg, rrx, cmsg, crx, csib, chalf, brx, vrc, vcc, stage, sent = take(12)
        ld_sem, dd_r, l_r, half_r, s_sem, greet = take(6)
        row_in = lambda m: ld_sem.at[m]
        col_in = lambda m: half_r.at[m] if n_rc[m][1] == 8 else ld_sem.at[NM + m]
        pair_in = lambda m: dd_r.at[m]
        merge_in = lambda m: dd_r.at[2 + m]
        totals_in = dd_r.at[NM]

        z = lax.axis_index('model')
        d = lax.axis_index('data')
        core = lax.rem(d, 2)
        xx = lax.rem(d // 2, 2)
        yy = d // 4
        sib_step = 1 - 2 * core
        sib = d + sib_step
        dx = d + 2 - 4 * xx
        dy = d + 4 - 8 * yy
        dd = dx + 4 - 8 * yy
        owner = {OWN: d, NX: dx, NY: dy, ND: dd}

        def flip_d(k):
            return d + (k % 2) * sib_step + (k // 2 % 2) * (2 - 4 * xx) + (k // 4) * (4 - 8 * yy)

        def flip_z(k):
            return z + (k % 2) * (1 - 2 * lax.rem(z, 2)) + (k // 2) * (2 - 4 * (z // 2))

        def remote(src, dst, ssem, rsem, data=None, model=None):
            return pltpu.make_async_remote_copy(
                src_ref=src, dst_ref=dst, send_sem=ssem, recv_sem=rsem,
                device_id=(z if model is None else model, d if data is None else data),
                device_id_type=MESH_ID)

        def signal(sem, data=None, model=None):
            pl.semaphore_signal(
                sem, inc=1,
                device_id=(z if model is None else model, d if data is None else data),
                device_id_type=MESH_ID)

        def wait_bytes(ref, sem):
            pltpu.make_async_copy(ref, ref, sem).wait()

        barrier = pltpu.get_barrier_semaphore()
        first_core, second_core = core == 0, core == 1
        up_ok = z < n_model - 1
        down_ok = z > 0
        n_z = jnp.where(up_ok, 1, 0) + jnp.where(down_ok, 1, 0)

        def signal_z(sem, data=None, also=None):
            @pl.when(up_ok if also is None else up_ok & also)
            def _():
                signal(sem, data=data, model=z + 1)

            @pl.when(down_ok if also is None else down_ok & also)
            def _():
                signal(sem, data=data, model=z - 1)

        @pl.when(second_core)
        def _():
            signal(barrier, data=sib)

        def block(who, f):
            m, j, r0, n = f
            q = mats[m]
            if q['flip']:
                cut = pl.ds(pl.multiple_of(who * q['n1'], LANES), q['n1'])
                return grads[m].at[0, pl.ds(r0, n), cut]
            return grads[m].at[0, pl.ds(pl.multiple_of(who * q['n0'] + r0, 8), n), :]

        loads, dsend, stage_in = {}, {}, {}
        for f in first + group[0] + group[1] + group[2] + group[3]:
            m, j, r0, n = f
            slot = first.index(f) if f in first else 4 + m
            loads[f] = pltpu.make_async_copy(block(owner[j], f), loc[m].at[j, pl.ds(r0, n), :], ld_sem.at[slot])
            source = block(owner[j] + sib_step, f)
            if f in first:
                held = stg.at[pl.ds(r0, n), :]
                stage_in[f] = pltpu.make_async_copy(source, held, ld_sem.at[4 + slot])
                source = held
            dsend[f] = remote(source, rec[m].at[j, pl.ds(r0, n), :], s_sem.at[0], dd_r.at[slot], data=sib)

        def fetch(pieces):
            for f in pieces:
                dsend[f].start()
                loads[f].start()

        def fetch_done(m):
            some = pl.ds(0, 3) if m == 0 else pl.ds(0, 4)
            wait_bytes(loc[m].at[some], ld_sem.at[4 + m])
            wait_bytes(rec[m].at[some], dd_r.at[4 + m])

        def link_send(m, j, r0, n):
            h, off = (0, r0) if r0 < halves[m] else (1, r0 - halves[m])
            along_x = (j == ND and h == 0) or j == NX
            slot = (0 if along_x else 1) if j == ND else (2 if along_x else 4) + h
            return remote(loc[m].at[j, pl.ds(r0, n), :], fxy[m].at[slot, pl.ds(off, n), :],
                          s_sem.at[0], l_r.at[2 * m + (0 if j == ND else 1)], data=dx if along_x else dy)

        def relays_in(m):
            wait_bytes(fxy[m].at[pl.ds(0, 2)], l_r.at[2 * m])

        def finals_in(m):
            wait_bytes(fxy[m].at[pl.ds(2, 4)], l_r.at[2 * m + 1])

        def pair_sum(m, j, r0, n, relay=None):
            total = loc[m][j, r0:r0 + n, :] + rec[m][j, r0:r0 + n, :]
            if relay is not None:
                total = total + fxy[m][relay]
            loc[m][j, r0:r0 + n, :] = total
            link_send(m, j, r0, n).start()

        def send_raw(m):
            n = halves[m]
            fetch_done(m)
            if m > 0:
                pair_sum(m, ND, 0, n)
                pair_sum(m, ND, n, n)
            pair_sum(m, NX, 0, n)
            pair_sum(m, NY, n, n)

        def send_acc(m):
            n = halves[m]
            relays_in(m)
            pair_sum(m, NY, 0, n, 0)
            pair_sum(m, NX, n, n, 1)

        for f in first:
            stage_in[f].start()
            loads[f].start()

        @pl.when(first_core)
        def _():
            pl.semaphore_wait(barrier, 1)
            signal(barrier, data=dx + 1)
            signal(barrier, data=dy + 1)
            signal(greet.at[3], data=sib)

        signal_z(barrier, data=sib, also=first_core)

        @pl.when(second_core)
        def _():
            pl.semaphore_wait(greet.at[3], 1)

        for f in first:
            stage_in[f].wait()
            dsend[f].start()

        @pl.when(second_core)
        def _():
            pl.semaphore_wait(barrier, 2 + n_z)
            signal(greet.at[4], data=sib)

        @pl.when(first_core)
        def _():
            pl.semaphore_wait(greet.at[4], 1)

        def first_done(pieces):
            for f in pieces:
                loads[f].wait()
                dsend[f].wait_recv()

        @pl.when(second_core)
        def _():
            first_done(first[2:])
            pl.delay(LEAD_NS)

        first_done(first[:2])
        for f in first[:2]:
            pair_sum(*f)
        fetch(group[0])
        pl.when(first_core)(lambda: first_done(first[2:]))
        for f in first[2:]:
            pair_sum(*f)
        fetch(group[1])
        send_raw(0)
        fetch(group[2])
        send_raw(1)
        fetch(group[3])
        small = [pltpu.make_async_copy(vrows[m], vrbuf[m], ld_sem.at[m]) for m in range(NM)]
        small += [pltpu.make_async_copy(vcols[m], vcbuf[m], ld_sem.at[4 + m]) for m in range(2)]
        late = [pltpu.make_async_copy(params[m], wbuf[m], ld_sem.at[m]) for m in range(NM)]
        late += [pltpu.make_async_copy(vcols[m], vcbuf[m], ld_sem.at[2 + m]) for m in range(2, NM)]
        for turn in (small, late):
            for cp in turn:
                cp.start()
            for cp in turn:
                cp.wait()

        lane = lax.broadcasted_iota(jnp.int32, TILE, 1)
        sub = lax.broadcasted_iota(jnp.int32, TILE, 0)
        lane1 = lax.broadcasted_iota(jnp.int32, (1, LANES), 1)

        def group_mask(g):
            shape = (g, 8, LANES)
            return lax.broadcasted_iota(jnp.int32, shape, 2) == lax.broadcasted_iota(jnp.int32, shape, 0)

        def compact(values):
            return jnp.sum(jnp.where(group_mask(values.shape[0]), values, 0.0), axis=0)

        def expand(vec, g):
            return jnp.sum(jnp.where(group_mask(g), vec[None], 0.0), axis=2, keepdims=True)

        def rows_of(buf, n, i):
            stage[i] = jnp.zeros(TILE, jnp.float32)
            for t in range(-(-n // LANES)):
                n_t = min(LANES, n - LANES * t)
                stage[i, t:t + 1, 0:n_t] = buf[pl.ds(LANES * t, n_t)].reshape(1, n_t)

        def to_compact(i, n):
            out = jnp.zeros(TILE, jnp.float32)
            for t in range(-(-n // LANES)):
                row = jnp.broadcast_to(stage[i, t:t + 1, :], TILE)
                for g in range(min(LANES, n - LANES * t) // 8):
                    col = jnp.sum(jnp.where(lane == 8 * g + sub, row, 0.0), axis=1, keepdims=True)
                    out = jnp.where(lane == 16 * t + g, col, out)
            return out

        bv = jnp.zeros((1, LANES), jnp.float32)
        for m in range(NM):
            q = mats[m]
            w = wbuf[m][...]
            part = jnp.sum(w * w, axis=(0, 1), keepdims=True) * (1.0 / q['size'])
            bv = jnp.where(lane1 == 2 * NM + m, part, bv)
            rows_of(vrbuf[m], q['rows_b'], 2 * m)
            rows_of(vcbuf[m], cols[m], 2 * m + 1)
            if q['flip']:
                vrc[m] = stage[2 * m]
                vcc[m] = to_compact(2 * m + 1, q['n0'])
            else:
                vrc[m] = to_compact(2 * m, q['n0'])
                vcc[m] = stage[2 * m + 1]

        for i in range(3):
            signal_z(greet.at[i])
            pl.semaphore_wait(greet.at[i], n_z)

        def send_rows(m):
            n_r = n_rc[m][0]
            for k in (3, 2, 1):
                remote(rmsg.at[m, pl.ds(0, n_r)], rrx.at[3 * m + k - 1, pl.ds(0, n_r)], s_sem.at[0], row_in(m),
                       model=flip_z(k)).start()

        def send_cols(m, ks):
            n_c = n_rc[m][1]
            for k in ks:
                remote(cmsg.at[m, pl.ds(0, n_c)], crx.at[7 * m + k - 1, pl.ds(0, n_c)], s_sem.at[0], col_in(m),
                       data=flip_d(k)).start()

        def share_pair(m):
            wait_bytes(csib.at[m], pair_in(m))
            mine = jnp.where(core == 0, csib[m, 0:4, :] + cmsg[m, 0:4, :], csib[m, 4:8, :] + cmsg[m, 4:8, :])
            chalf[m, 0] = mine
            for k, peer in enumerate((dd, dx, dy)):
                remote(chalf.at[m, 0], chalf.at[m, 1 + k], s_sem.at[0], col_in(m), data=peer).start()

        def merge_pair(m):
            wait_bytes(chalf.at[m, pl.ds(1, 3)], col_in(m))
            chalf[m, 4] = chalf[m, 0] + chalf[m, 1] + chalf[m, 2] + chalf[m, 3]
            remote(chalf.at[m, 4], chalf.at[m, 5], s_sem.at[0], merge_in(m), data=sib).start()

        def merged(m):
            wait_bytes(chalf.at[m, 5], merge_in(m))
            mine, other = chalf[m, 4], chalf[m, 5]
            return jnp.concatenate([jnp.where(core == 0, mine, other), jnp.where(core == 0, other, mine)], axis=0)


        def finish_sum(m):
            q = mats[m]
            half, n1 = q['half'], q['n1']
            acc1 = jnp.zeros((8, n1), jnp.float32)
            rsums = []
            finals_in(m)
            for h in range(2):
                rows = slice(h * half, (h + 1) * half)
                total = loc[m][OWN, rows, :] + rec[m][OWN, rows, :] + fxy[m][2 + h] + fxy[m][4 + h]
                upd[m][rows, :] = total
                sq = (total * total + 1e-30).reshape(half // 8, 8, n1)
                acc1 = acc1 + jnp.sum(sq, axis=0)
                rsums.append(jnp.sum(sq, axis=2, keepdims=True))
            sum1 = jnp.sum(acc1, axis=0, keepdims=True)
            msg0, msg1 = (cmsg, rmsg) if q['flip'] else (rmsg, cmsg)
            for k in range(q['lanes']):
                msg1[m, k:k + 1, :] = sum1[:, LANES * k:LANES * k + LANES]
            if not q['flip']:
                send_cols(m, (6, 7, 2, 4, 3, 5, 1))
            msg0[m] = compact(jnp.concatenate(rsums, axis=0))
            send_rows(m)
            if q['flip']:
                remote(cmsg.at[m], csib.at[m], s_sem.at[0], pair_in(m), data=sib).start()

        def apply_factors(m, bv, locrow):
            q = mats[m]
            n_r, n_c = n_rc[m]
            g_n, n1 = q['groups'], q['n1']
            ok = lane < g_n

            def along0(fac):
                return expand(fac, g_n)

            def along1(fac):
                wide = [jnp.broadcast_to(fac[k:k + 1, :], TILE) for k in range(q['lanes'])]
                return jnp.concatenate(wide, axis=1)[None]

            rtot = rmsg[m, 0:n_r, :]
            wait_bytes(loc[0].at[0, pl.ds(0, 3 * n_r), :], row_in(m))
            for k in range(3):
                rtot = rtot + rrx[3 * m + k, 0:n_r, :]
            vr = BETA * vrc[m, 0:n_r, :] + (1.0 - BETA) * (rtot * (1.0 / q['cols_t']))
            vr_sum = jnp.sum(vr if q['flip'] else jnp.where(ok, vr, 0.0), axis=(0, 1), keepdims=True)
            mloc = vr_sum * (1.0 / q['rows_b'])
            inv_mloc = 1.0 / mloc
            rfac = lax.rsqrt(vr / mloc) if q['flip'] else lax.rsqrt(jnp.where(ok, vr / mloc, 1.0))
            part = upd[m][...].reshape(g_n, 8, n1) * (along1 if q['flip'] else along0)(rfac)
            if n_c == 8:
                ctot = merged(m)
            else:
                ctot = cmsg[m, 0:n_c, :]
                wait_bytes(loc[0].at[0, pl.ds(0, 7 * n_c), :], col_in(m))
                for k in range(7):
                    ctot = ctot + crx[7 * m + k, 0:n_c, :]
            vc = BETA * vcc[m, 0:n_c, :] + (1.0 - BETA) * (ctot * (1.0 / q['rows_t']))
            cfac = lax.rsqrt(jnp.where(ok, vc, 1.0)) if q['flip'] else lax.rsqrt(vc)
            u = part * (along0 if q['flip'] else along1)(cfac)
            t_m = jnp.sum(jnp.sum(u * u, axis=0), axis=(0, 1), keepdims=True)
            upd[m][...] = u.reshape(q['n0'], n1)
            vcc[m] = vc if q['flip'] else vr
            stats[1 + 2 * m, 0:q['lanes'], :] = vr if q['flip'] else vc
            bv = jnp.where(lane1 == NM + m, vr_sum * (1.0 / (q['rows_t'] * n_model)), bv)
            bv = jnp.where(lane1 == m, (t_m * (1.0 / q['size'])) * inv_mloc, bv)
            locrow = jnp.where(lane1 == m, mloc, locrow)
            return bv, locrow

        locrow = jnp.ones((1, LANES), jnp.float32)
        send_acc(0)
        send_raw(2)
        send_acc(1)
        finish_sum(0)
        send_raw(3)
        share_pair(0)
        send_acc(2)
        finish_sum(1)
        share_pair(1)
        send_acc(3)
        merge_pair(0)
        bv, locrow = apply_factors(0, bv, locrow)
        finish_sum(2)
        merge_pair(1)
        finish_sum(3)
        bv, locrow = apply_factors(1, bv, locrow)
        bv, locrow = apply_factors(2, bv, locrow)
        bv, locrow = apply_factors(3, bv, locrow)

        brx[0:1, :] = bv
        for kz in (3, 2, 1, 0):
            for kd in range(n_data - 1, -1, -1):
                if kz == 0 and kd == 0:
                    continue
                i = kz * n_data + kd
                remote(brx.at[pl.ds(0, 1), :], brx.at[pl.ds(i, 1), :], s_sem.at[0], totals_in,
                       data=flip_d(kd), model=flip_z(kz)).start()

        for m in range(NM):
            q = mats[m]
            wide = expand(vcc[m], q['groups'])
            for t in range(q['tiles']):
                n_t = min(LANES, q['n0'] - LANES * t)
                g_n = n_t // 8
                shape = (g_n, 8, LANES)
                pick = (lax.broadcasted_iota(jnp.int32, shape, 2)
                        == 8 * lax.broadcasted_iota(jnp.int32, shape, 0) + lax.broadcasted_iota(jnp.int32, shape, 1))
                rows = jnp.sum(jnp.where(pick, wide[16 * t:16 * t + g_n], 0.0), axis=0)
                stats[2 + 2 * m, t:t + 1, :] = jnp.sum(rows, axis=0, keepdims=True)

        wait_bytes(brx.at[pl.ds(1, n_model * n_data - 1), :], totals_in)
        tot = jnp.broadcast_to(jnp.sum(brx[...], axis=0, keepdims=True), TILE)
        mean_vr = pltpu.roll(tot, LANES - NM, 1)
        u_rms = jnp.sqrt(mean_vr * tot)
        w_rms = jnp.sqrt(pltpu.roll(tot, LANES - 2 * NM, 1))
        fac = -(LR_REL * jnp.maximum(1e-3, w_rms)) * (jnp.sqrt(mean_vr) * lax.rsqrt(locrow))
        stats[0] = fac / jnp.maximum(1.0, u_rms)
        wait_bytes(sent, s_sem.at[0])

    f32 = jnp.float32
    dma = pltpu.SemaphoreType.DMA
    vm = pltpu.VMEM
    scratch = []
    scratch += [vm((4, q['n0'], q['n1']), f32) for q in mats]
    scratch += [vm((4, q['n0'], q['n1']), f32) for q in mats]
    scratch += [vm((6, q['half'], q['n1']), f32) for q in mats]
    scratch += [vm((r,), f32) for r in rows_b]
    scratch += [vm((c,), f32) for c in cols]
    scratch += [vm((mats[0]['n0'], mats[0]['n1']), f32)]
    tile = lambda *lead: vm((*lead, 8, LANES), f32)
    scratch += [tile(NM), tile(3 * NM), tile(NM), tile(7 * NM), tile(2), vm((2, 6, 4, LANES), f32), vm((n_model * n_data, LANES), f32),
                tile(NM), tile(NM), tile(2 * NM), vm((sent_rows, LANES), f32)]
    scratch += [dma((8,)), dma((8,)), dma((2 * NM,)), dma((2,)), dma((1,)), pltpu.SemaphoreType.REGULAR((5,))]
    blocks = [jax.ShapeDtypeStruct((q['n0'], q['n1']), f32) for q in mats]
    out_shape = blocks + blocks + [jax.ShapeDtypeStruct((1 + 2 * NM, 8, LANES), f32)]
    vmem = pl.BlockSpec(memory_space=pltpu.VMEM)
    hbm = pl.BlockSpec(memory_space=pltpu.HBM)
    return pl.pallas_call(
        kernel, out_shape=out_shape, in_specs=[hbm] * 16, out_specs=[vmem] * len(out_shape),
        scratch_shapes=scratch,
        compiler_params=pltpu.CompilerParams(collective_id=0, has_side_effects=True,
                                             vmem_limit_bytes=36 * MIB))


def make_apply_kernel(rows_b, cols, n_model, n_data):
    mats = layout_of(rows_b, cols, n_model, n_data)

    def kernel(*refs):
        upd, params, stats = refs[0:4], refs[4:8], refs[8]
        new, delta, vrow_out, vcol_out = refs[9:13], refs[13:17], refs[17:21], refs[21:25]
        bufs, vrbuf, vcbuf = refs[25:29], refs[29:33], refs[33:37]
        sem = refs[37]
        for m in range(NM):
            fac = stats[0, 0:1, m:m + 1]
            n = mats[m]['n0'] // PARTS
            for i in range(PARTS):
                rows = slice(i * n, i * n + n)
                step = fac * upd[m][rows, :]
                bufs[m][0, rows, :] = step
                pltpu.make_async_copy(bufs[m].at[0, rows], delta[m].at[rows], sem.at[m]).start()
                bufs[m][1, rows, :] = params[m][rows, :] + step
                pltpu.make_async_copy(bufs[m].at[1, rows], new[m].at[rows], sem.at[m]).start()
        copies = []
        for m in range(NM):
            q = mats[m]
            out1, out0 = (vrbuf[m], vcbuf[m]) if q['flip'] else (vcbuf[m], vrbuf[m])
            for k in range(q['lanes']):
                out1[pl.ds(LANES * k, LANES)] = stats[1 + 2 * m, k:k + 1, :].reshape(LANES)
            for t in range(q['tiles']):
                n_t = min(LANES, q['n0'] - LANES * t)
                out0[pl.ds(LANES * t, n_t)] = stats[2 + 2 * m, t:t + 1, 0:n_t].reshape(n_t)
            for i, (buf, out) in enumerate(((vrbuf[m], vrow_out[m]), (vcbuf[m], vcol_out[m]))):
                copies.append(pltpu.make_async_copy(buf, out, sem.at[NM + 2 * m + i]))
                copies[-1].start()
        for m in range(NM):
            pltpu.make_async_copy(bufs[m], bufs[m], sem.at[m]).wait()
        for cp in copies:
            cp.wait()

    f32 = jnp.float32
    vmem = pl.BlockSpec(memory_space=pltpu.VMEM)
    hbm = pl.BlockSpec(memory_space=pltpu.HBM)
    blocks = [jax.ShapeDtypeStruct((q['n0'], q['n1']), f32) for q in mats]
    out_shape = (blocks + blocks + [jax.ShapeDtypeStruct((r,), f32) for r in rows_b]
                 + [jax.ShapeDtypeStruct((c,), f32) for c in cols])
    scratch = [pltpu.VMEM((2, q['n0'], q['n1']), f32) for q in mats]
    scratch += [pltpu.VMEM((n,), f32) for n in (*rows_b, *cols)] + [pltpu.SemaphoreType.DMA((3 * NM,))]
    return pl.pallas_call(
        kernel, out_shape=out_shape, in_specs=[vmem] * 9, out_specs=[hbm] * 16, scratch_shapes=scratch,
        compiler_params=pltpu.CompilerParams(vmem_limit_bytes=6 * MIB))


def solution(mesh):
    n_data = mesh.shape['data']
    n_model = mesh.shape['model']
    mat_spec = P('data', 'model')
    in_specs = (P('data', None, 'model'), mat_spec, P('data'), P('model')) * NM
    out_specs = (mat_spec, mat_spec, P('data'), P('model')) * NM

    def per_device(*arrays):
        grads, params = arrays[0::4], arrays[1::4]
        rows_b = [p.shape[0] for p in params]
        cols = [p.shape[1] for p in params]
        mats = layout_of(rows_b, cols, n_model, n_data)
        view = lambda i, a: jnp.swapaxes(a, -1, -2) if mats[i]['flip'] else a
        grads = [view(i, g) for i, g in enumerate(grads)]
        params = [view(i, p) for i, p in enumerate(params)]
        pin = lambda a: pltpu.with_memory_space_constraint(a, pltpu.HBM)
        outs = make_reduce_kernel(rows_b, cols, n_model, n_data)(
            *map(pin, grads), *map(pin, params), *map(pin, arrays[2::4]), *map(pin, arrays[3::4]))
        res = make_apply_kernel(rows_b, cols, n_model, n_data)(*outs)
        flat = []
        for m in range(NM):
            flat += [view(m, res[m]), view(m, res[4 + m]), res[8 + m], res[12 + m]]
        return tuple(flat)

    return jax.shard_map(per_device, mesh=mesh, in_specs=in_specs, out_specs=out_specs, check_vma=False)
```

```python
import jax
import jax.numpy as jnp
from jax import lax
from jax.experimental import pallas as pl
from jax.experimental.pallas import tpu as pltpu
from jax.sharding import PartitionSpec as P

OPT_STEP = 3
BETA = 1.0 - OPT_STEP ** -0.8
LR_REL = min(0.01, OPT_STEP ** -0.5)
NM = 4
OWN, NX, NY, ND = 0, 1, 2, 3
FIRST_ROWS = 88
PARTS = 4
LEAD_NS = 200
LANES = 128
TILE = (8, LANES)
MIB = 1024 * 1024
MESH_ID = pl.DeviceIdType.MESH


def layout_of(rows_b, cols, n_model, n_data):
    mats = []
    for r, c in zip(rows_b, cols):
        flip = c % LANES != 0
        n0, n1 = (c, r) if flip else (r, c)
        mats.append(dict(flip=flip, n0=n0, n1=n1, half=n0 // 2, groups=n0 // 8, tiles=-(-n0 // LANES), lanes=n1 // LANES,
                         rows_b=r, rows_t=r * n_data, cols_t=c * n_model,
                         size=float(r * n_data * c * n_model)))
    return mats


def make_reduce_kernel(rows_b, cols, n_model, n_data):
    mats = layout_of(rows_b, cols, n_model, n_data)
    halves = [q['half'] for q in mats]
    n_rc = [(q['lanes'], 8) if q['flip'] else (8, q['lanes']) for q in mats]
    sent_rows = sum(7 * q['n0'] * q['lanes'] for q in mats) + n_model * n_data - 1
    sent_rows += sum(3 * r + (24 if c == 8 else 7 * c) for r, c in n_rc)
    first = []
    for lo, hi in ((0, FIRST_ROWS), (FIRST_ROWS, halves[0])):
        first += [(0, ND, lo, hi - lo), (0, ND, halves[0] + lo, hi - lo)]
    group = {m: [(m, j, 0, mats[m]['n0']) for j in ((NX, NY, OWN) if m == 0 else (ND, NX, NY, OWN))] for m in range(NM)}

    def kernel(*refs):
        grads = refs[0:4]
        params = refs[4:8]
        vrows = refs[8:12]
        vcols = refs[12:16]
        upd = refs[16:20]
        wbuf = refs[20:24]
        stats = refs[24]
        sc = list(refs[25:])
        take = lambda n: [sc.pop(0) for _ in range(n)]
        loc, rec, fxy, vrbuf, vcbuf = (take(4) for _ in range(5))
        stg, rmsg, rrx, cmsg, crx, csib, chalf, brx, vrc, vcc, stage, sent = take(12)
        ld_sem, dd_r, l_r, half_r, s_sem, greet = take(6)
        row_in = lambda m: ld_sem.at[m]
        col_in = lambda m: half_r.at[m] if n_rc[m][1] == 8 else ld_sem.at[NM + m]
        pair_in = lambda m: dd_r.at[m]
        merge_in = lambda m: dd_r.at[2 + m]
        totals_in = dd_r.at[NM]

        z = lax.axis_index('model')
        d = lax.axis_index('data')
        core = lax.rem(d, 2)
        xx = lax.rem(d // 2, 2)
        yy = d // 4
        sib_step = 1 - 2 * core
        sib = d + sib_step
        dx = d + 2 - 4 * xx
        dy = d + 4 - 8 * yy
        dd = dx + 4 - 8 * yy
        owner = {OWN: d, NX: dx, NY: dy, ND: dd}

        def flip_d(k):
            return d + (k % 2) * sib_step + (k // 2 % 2) * (2 - 4 * xx) + (k // 4) * (4 - 8 * yy)

        def flip_z(k):
            return z + (k % 2) * (1 - 2 * lax.rem(z, 2)) + (k // 2) * (2 - 4 * (z // 2))

        def remote(src, dst, ssem, rsem, data=None, model=None):
            return pltpu.make_async_remote_copy(
                src_ref=src, dst_ref=dst, send_sem=ssem, recv_sem=rsem,
                device_id=(z if model is None else model, d if data is None else data),
                device_id_type=MESH_ID)

        def signal(sem, data=None, model=None):
            pl.semaphore_signal(
                sem, inc=1,
                device_id=(z if model is None else model, d if data is None else data),
                device_id_type=MESH_ID)

        def wait_bytes(ref, sem):
            pltpu.make_async_copy(ref, ref, sem).wait()

        barrier = pltpu.get_barrier_semaphore()
        first_core, second_core = core == 0, core == 1
        up_ok = z < n_model - 1
        down_ok = z > 0
        n_z = jnp.where(up_ok, 1, 0) + jnp.where(down_ok, 1, 0)

        def signal_z(sem, data=None, also=None):
            @pl.when(up_ok if also is None else up_ok & also)
            def _():
                signal(sem, data=data, model=z + 1)

            @pl.when(down_ok if also is None else down_ok & also)
            def _():
                signal(sem, data=data, model=z - 1)

        @pl.when(second_core)
        def _():
            signal(barrier, data=sib)

        def block(who, f):
            m, j, r0, n = f
            q = mats[m]
            if q['flip']:
                cut = pl.ds(pl.multiple_of(who * q['n1'], LANES), q['n1'])
                return grads[m].at[0, pl.ds(r0, n), cut]
            return grads[m].at[0, pl.ds(pl.multiple_of(who * q['n0'] + r0, 8), n), :]

        loads, dsend, stage_in = {}, {}, {}
        for f in first + group[0] + group[1] + group[2] + group[3]:
            m, j, r0, n = f
            slot = first.index(f) if f in first else 4 + m
            loads[f] = pltpu.make_async_copy(block(owner[j], f), loc[m].at[j, pl.ds(r0, n), :], ld_sem.at[slot])
            source = block(owner[j] + sib_step, f)
            if f in first:
                held = stg.at[pl.ds(r0, n), :]
                stage_in[f] = pltpu.make_async_copy(source, held, ld_sem.at[4 + slot])
                source = held
            dsend[f] = remote(source, rec[m].at[j, pl.ds(r0, n), :], s_sem.at[0], dd_r.at[slot], data=sib)

        def fetch(pieces):
            for f in pieces:
                dsend[f].start()
                loads[f].start()

        def fetch_done(m):
            some = pl.ds(0, 3) if m == 0 else pl.ds(0, 4)
            wait_bytes(loc[m].at[some], ld_sem.at[4 + m])
            wait_bytes(rec[m].at[some], dd_r.at[4 + m])

        def link_send(m, j, r0, n):
            h, off = (0, r0) if r0 < halves[m] else (1, r0 - halves[m])
            along_x = (j == ND and h == 0) or j == NX
            slot = (0 if along_x else 1) if j == ND else (2 if along_x else 4) + h
            return remote(loc[m].at[j, pl.ds(r0, n), :], fxy[m].at[slot, pl.ds(off, n), :],
                          s_sem.at[0], l_r.at[2 * m + (0 if j == ND else 1)], data=dx if along_x else dy)

        def relays_in(m):
            wait_bytes(fxy[m].at[pl.ds(0, 2)], l_r.at[2 * m])

        def finals_in(m):
            wait_bytes(fxy[m].at[pl.ds(2, 4)], l_r.at[2 * m + 1])

        def pair_sum(m, j, r0, n, relay=None):
            total = loc[m][j, r0:r0 + n, :] + rec[m][j, r0:r0 + n, :]
            if relay is not None:
                total = total + fxy[m][relay]
            loc[m][j, r0:r0 + n, :] = total
            link_send(m, j, r0, n).start()

        def send_raw(m):
            n = halves[m]
            fetch_done(m)
            if m > 0:
                pair_sum(m, ND, 0, n)
                pair_sum(m, ND, n, n)
            pair_sum(m, NX, 0, n)
            pair_sum(m, NY, n, n)

        def send_acc(m):
            n = halves[m]
            relays_in(m)
            pair_sum(m, NY, 0, n, 0)
            pair_sum(m, NX, n, n, 1)

        for f in first:
            stage_in[f].start()
            loads[f].start()

        @pl.when(first_core)
        def _():
            pl.semaphore_wait(barrier, 1)
            signal(barrier, data=dx + 1)
            signal(barrier, data=dy + 1)
            signal(greet.at[3], data=sib)

        signal_z(barrier, data=sib, also=first_core)

        @pl.when(second_core)
        def _():
            pl.semaphore_wait(greet.at[3], 1)

        for f in first:
            stage_in[f].wait()
            dsend[f].start()

        @pl.when(second_core)
        def _():
            pl.semaphore_wait(barrier, 2 + n_z)
            signal(greet.at[4], data=sib)

        @pl.when(first_core)
        def _():
            pl.semaphore_wait(greet.at[4], 1)

        def first_done(pieces):
            for f in pieces:
                loads[f].wait()
                dsend[f].wait_recv()

        @pl.when(second_core)
        def _():
            first_done(first[2:])
            pl.delay(LEAD_NS)

        first_done(first[:2])
        for f in first[:2]:
            pair_sum(*f)
        fetch(group[0])
        pl.when(first_core)(lambda: first_done(first[2:]))
        for f in first[2:]:
            pair_sum(*f)
        fetch(group[1])
        send_raw(0)
        fetch(group[2])
        send_raw(1)
        fetch(group[3])
        small = [pltpu.make_async_copy(vrows[m], vrbuf[m], ld_sem.at[m]) for m in range(NM)]
        small += [pltpu.make_async_copy(vcols[m], vcbuf[m], ld_sem.at[4 + m]) for m in range(2)]
        late = [pltpu.make_async_copy(params[m], wbuf[m], ld_sem.at[m]) for m in range(NM)]
        late += [pltpu.make_async_copy(vcols[m], vcbuf[m], ld_sem.at[2 + m]) for m in range(2, NM)]
        for turn in (small, late):
            for cp in turn:
                cp.start()
            for cp in turn:
                cp.wait()

        lane = lax.broadcasted_iota(jnp.int32, TILE, 1)
        sub = lax.broadcasted_iota(jnp.int32, TILE, 0)
        lane1 = lax.broadcasted_iota(jnp.int32, (1, LANES), 1)

        def group_mask(g):
            shape = (g, 8, LANES)
            return lax.broadcasted_iota(jnp.int32, shape, 2) == lax.broadcasted_iota(jnp.int32, shape, 0)

        def compact(values):
            return jnp.sum(jnp.where(group_mask(values.shape[0]), values, 0.0), axis=0)

        def expand(vec, g):
            return jnp.sum(jnp.where(group_mask(g), vec[None], 0.0), axis=2, keepdims=True)

        def rows_of(buf, n, i):
            stage[i] = jnp.zeros(TILE, jnp.float32)
            for t in range(-(-n // LANES)):
                n_t = min(LANES, n - LANES * t)
                stage[i, t:t + 1, 0:n_t] = buf[pl.ds(LANES * t, n_t)].reshape(1, n_t)

        def to_compact(i, n):
            out = jnp.zeros(TILE, jnp.float32)
            for t in range(-(-n // LANES)):
                row = jnp.broadcast_to(stage[i, t:t + 1, :], TILE)
                for g in range(min(LANES, n - LANES * t) // 8):
                    col = jnp.sum(jnp.where(lane == 8 * g + sub, row, 0.0), axis=1, keepdims=True)
                    out = jnp.where(lane == 16 * t + g, col, out)
            return out

        bv = jnp.zeros((1, LANES), jnp.float32)
        for m in range(NM):
            q = mats[m]
            w = wbuf[m][...]
            part = jnp.sum(w * w, axis=(0, 1), keepdims=True) * (1.0 / q['size'])
            bv = jnp.where(lane1 == 2 * NM + m, part, bv)
            rows_of(vrbuf[m], q['rows_b'], 2 * m)
            rows_of(vcbuf[m], cols[m], 2 * m + 1)
            if q['flip']:
                vrc[m] = stage[2 * m]
                vcc[m] = to_compact(2 * m + 1, q['n0'])
            else:
                vrc[m] = to_compact(2 * m, q['n0'])
                vcc[m] = stage[2 * m + 1]

        for i in range(3):
            signal_z(greet.at[i])
            pl.semaphore_wait(greet.at[i], n_z)

        def send_rows(m):
            n_r = n_rc[m][0]
            for k in (3, 2, 1):
                remote(rmsg.at[m, pl.ds(0, n_r)], rrx.at[3 * m + k - 1, pl.ds(0, n_r)], s_sem.at[0], row_in(m),
                       model=flip_z(k)).start()

        def send_cols(m, ks):
            n_c = n_rc[m][1]
            for k in ks:
                remote(cmsg.at[m, pl.ds(0, n_c)], crx.at[7 * m + k - 1, pl.ds(0, n_c)], s_sem.at[0], col_in(m),
                       data=flip_d(k)).start()

        def share_pair(m):
            wait_bytes(csib.at[m], pair_in(m))
            mine = jnp.where(core == 0, csib[m, 0:4, :] + cmsg[m, 0:4, :], csib[m, 4:8, :] + cmsg[m, 4:8, :])
            chalf[m, 0] = mine
            for k, peer in enumerate((dd, dx, dy)):
                remote(chalf.at[m, 0], chalf.at[m, 1 + k], s_sem.at[0], col_in(m), data=peer).start()

        def merge_pair(m):
            wait_bytes(chalf.at[m, pl.ds(1, 3)], col_in(m))
            chalf[m, 4] = chalf[m, 0] + chalf[m, 1] + chalf[m, 2] + chalf[m, 3]
            remote(chalf.at[m, 4], chalf.at[m, 5], s_sem.at[0], merge_in(m), data=sib).start()

        def merged(m):
            wait_bytes(chalf.at[m, 5], merge_in(m))
            mine, other = chalf[m, 4], chalf[m, 5]
            return jnp.concatenate([jnp.where(core == 0, mine, other), jnp.where(core == 0, other, mine)], axis=0)


        def finish_sum(m):
            q = mats[m]
            half, n1 = q['half'], q['n1']
            acc1 = jnp.zeros((8, n1), jnp.float32)
            rsums = []
            finals_in(m)
            for h in range(2):
                rows = slice(h * half, (h + 1) * half)
                total = loc[m][OWN, rows, :] + rec[m][OWN, rows, :] + fxy[m][2 + h] + fxy[m][4 + h]
                upd[m][rows, :] = total
                sq = (total * total + 1e-30).reshape(half // 8, 8, n1)
                acc1 = acc1 + jnp.sum(sq, axis=0)
                rsums.append(jnp.sum(sq, axis=2, keepdims=True))
            sum1 = jnp.sum(acc1, axis=0, keepdims=True)
            msg0, msg1 = (cmsg, rmsg) if q['flip'] else (rmsg, cmsg)
            for k in range(q['lanes']):
                msg1[m, k:k + 1, :] = sum1[:, LANES * k:LANES * k + LANES]
            if not q['flip']:
                send_cols(m, (6, 7, 2, 4, 3, 5, 1))
            msg0[m] = compact(jnp.concatenate(rsums, axis=0))
            send_rows(m)
            if q['flip']:
                remote(cmsg.at[m], csib.at[m], s_sem.at[0], pair_in(m), data=sib).start()

        def apply_factors(m, bv, locrow):
            q = mats[m]
            n_r, n_c = n_rc[m]
            g_n, n1 = q['groups'], q['n1']
            ok = lane < g_n

            def along0(fac):
                return expand(fac, g_n)

            def along1(fac):
                wide = [jnp.broadcast_to(fac[k:k + 1, :], TILE) for k in range(q['lanes'])]
                return jnp.concatenate(wide, axis=1)[None]

            rtot = rmsg[m, 0:n_r, :]
            wait_bytes(loc[0].at[0, pl.ds(0, 3 * n_r), :], row_in(m))
            for k in range(3):
                rtot = rtot + rrx[3 * m + k, 0:n_r, :]
            vr = BETA * vrc[m, 0:n_r, :] + (1.0 - BETA) * (rtot * (1.0 / q['cols_t']))
            vr_sum = jnp.sum(vr if q['flip'] else jnp.where(ok, vr, 0.0), axis=(0, 1), keepdims=True)
            mloc = vr_sum * (1.0 / q['rows_b'])
            inv_mloc = 1.0 / mloc
            rfac = lax.rsqrt(vr / mloc) if q['flip'] else lax.rsqrt(jnp.where(ok, vr / mloc, 1.0))
            part = upd[m][...].reshape(g_n, 8, n1) * (along1 if q['flip'] else along0)(rfac)
            if n_c == 8:
                ctot = merged(m)
            else:
                ctot = cmsg[m, 0:n_c, :]
                wait_bytes(loc[0].at[0, pl.ds(0, 7 * n_c), :], col_in(m))
                for k in range(7):
                    ctot = ctot + crx[7 * m + k, 0:n_c, :]
            vc = BETA * vcc[m, 0:n_c, :] + (1.0 - BETA) * (ctot * (1.0 / q['rows_t']))
            cfac = lax.rsqrt(jnp.where(ok, vc, 1.0)) if q['flip'] else lax.rsqrt(vc)
            u = part * (along0 if q['flip'] else along1)(cfac)
            t_m = jnp.sum(jnp.sum(u * u, axis=0), axis=(0, 1), keepdims=True)
            upd[m][...] = u.reshape(q['n0'], n1)
            vcc[m] = vc if q['flip'] else vr
            stats[1 + 2 * m, 0:q['lanes'], :] = vr if q['flip'] else vc
            bv = jnp.where(lane1 == NM + m, vr_sum * (1.0 / (q['rows_t'] * n_model)), bv)
            bv = jnp.where(lane1 == m, (t_m * (1.0 / q['size'])) * inv_mloc, bv)
            locrow = jnp.where(lane1 == m, mloc, locrow)
            return bv, locrow

        locrow = jnp.ones((1, LANES), jnp.float32)
        send_acc(0)
        send_raw(2)
        send_acc(1)
        finish_sum(0)
        send_raw(3)
        share_pair(0)
        send_acc(2)
        finish_sum(1)
        send_acc(3)
        share_pair(1)
        merge_pair(0)
        bv, locrow = apply_factors(0, bv, locrow)
        finish_sum(2)
        finish_sum(3)
        merge_pair(1)
        bv, locrow = apply_factors(2, bv, locrow)
        bv, locrow = apply_factors(1, bv, locrow)
        bv, locrow = apply_factors(3, bv, locrow)

        brx[0:1, :] = bv
        for kz in (3, 2, 1, 0):
            for kd in range(n_data - 1, -1, -1):
                if kz == 0 and kd == 0:
                    continue
                i = kz * n_data + kd
                remote(brx.at[pl.ds(0, 1), :], brx.at[pl.ds(i, 1), :], s_sem.at[0], totals_in,
                       data=flip_d(kd), model=flip_z(kz)).start()

        for m in range(NM):
            q = mats[m]
            wide = expand(vcc[m], q['groups'])
            for t in range(q['tiles']):
                n_t = min(LANES, q['n0'] - LANES * t)
                g_n = n_t // 8
                shape = (g_n, 8, LANES)
                pick = (lax.broadcasted_iota(jnp.int32, shape, 2)
                        == 8 * lax.broadcasted_iota(jnp.int32, shape, 0) + lax.broadcasted_iota(jnp.int32, shape, 1))
                rows = jnp.sum(jnp.where(pick, wide[16 * t:16 * t + g_n], 0.0), axis=0)
                stats[2 + 2 * m, t:t + 1, :] = jnp.sum(rows, axis=0, keepdims=True)

        wait_bytes(brx.at[pl.ds(1, n_model * n_data - 1), :], totals_in)
        tot = jnp.broadcast_to(jnp.sum(brx[...], axis=0, keepdims=True), TILE)
        mean_vr = pltpu.roll(tot, LANES - NM, 1)
        u_rms = jnp.sqrt(mean_vr * tot)
        w_rms = jnp.sqrt(pltpu.roll(tot, LANES - 2 * NM, 1))
        fac = -(LR_REL * jnp.maximum(1e-3, w_rms)) * (jnp.sqrt(mean_vr) * lax.rsqrt(locrow))
        stats[0] = fac / jnp.maximum(1.0, u_rms)
        wait_bytes(sent, s_sem.at[0])

    f32 = jnp.float32
    dma = pltpu.SemaphoreType.DMA
    vm = pltpu.VMEM
    scratch = []
    scratch += [vm((4, q['n0'], q['n1']), f32) for q in mats]
    scratch += [vm((4, q['n0'], q['n1']), f32) for q in mats]
    scratch += [vm((6, q['half'], q['n1']), f32) for q in mats]
    scratch += [vm((r,), f32) for r in rows_b]
    scratch += [vm((c,), f32) for c in cols]
    scratch += [vm((mats[0]['n0'], mats[0]['n1']), f32)]
    tile = lambda *lead: vm((*lead, 8, LANES), f32)
    scratch += [tile(NM), tile(3 * NM), tile(NM), tile(7 * NM), tile(2), vm((2, 6, 4, LANES), f32), vm((n_model * n_data, LANES), f32),
                tile(NM), tile(NM), tile(2 * NM), vm((sent_rows, LANES), f32)]
    scratch += [dma((8,)), dma((8,)), dma((2 * NM,)), dma((2,)), dma((1,)), pltpu.SemaphoreType.REGULAR((5,))]
    blocks = [jax.ShapeDtypeStruct((q['n0'], q['n1']), f32) for q in mats]
    out_shape = blocks + blocks + [jax.ShapeDtypeStruct((1 + 2 * NM, 8, LANES), f32)]
    vmem = pl.BlockSpec(memory_space=pltpu.VMEM)
    hbm = pl.BlockSpec(memory_space=pltpu.HBM)
    return pl.pallas_call(
        kernel, out_shape=out_shape, in_specs=[hbm] * 16, out_specs=[vmem] * len(out_shape),
        scratch_shapes=scratch,
        compiler_params=pltpu.CompilerParams(collective_id=0, has_side_effects=True,
                                             vmem_limit_bytes=36 * MIB))


def make_apply_kernel(rows_b, cols, n_model, n_data):
    mats = layout_of(rows_b, cols, n_model, n_data)

    def kernel(*refs):
        upd, params, stats = refs[0:4], refs[4:8], refs[8]
        new, delta, vrow_out, vcol_out = refs[9:13], refs[13:17], refs[17:21], refs[21:25]
        bufs, vrbuf, vcbuf = refs[25:29], refs[29:33], refs[33:37]
        sem = refs[37]
        for m in range(NM):
            fac = stats[0, 0:1, m:m + 1]
            n = mats[m]['n0'] // PARTS
            for i in range(PARTS):
                rows = slice(i * n, i * n + n)
                step = fac * upd[m][rows, :]
                bufs[m][0, rows, :] = step
                pltpu.make_async_copy(bufs[m].at[0, rows], delta[m].at[rows], sem.at[m]).start()
                bufs[m][1, rows, :] = params[m][rows, :] + step
                pltpu.make_async_copy(bufs[m].at[1, rows], new[m].at[rows], sem.at[m]).start()
        copies = []
        for m in range(NM):
            q = mats[m]
            out1, out0 = (vrbuf[m], vcbuf[m]) if q['flip'] else (vcbuf[m], vrbuf[m])
            for k in range(q['lanes']):
                out1[pl.ds(LANES * k, LANES)] = stats[1 + 2 * m, k:k + 1, :].reshape(LANES)
            for t in range(q['tiles']):
                n_t = min(LANES, q['n0'] - LANES * t)
                out0[pl.ds(LANES * t, n_t)] = stats[2 + 2 * m, t:t + 1, 0:n_t].reshape(n_t)
            for i, (buf, out) in enumerate(((vrbuf[m], vrow_out[m]), (vcbuf[m], vcol_out[m]))):
                copies.append(pltpu.make_async_copy(buf, out, sem.at[NM + 2 * m + i]))
                copies[-1].start()
        for m in range(NM):
            pltpu.make_async_copy(bufs[m], bufs[m], sem.at[m]).wait()
        for cp in copies:
            cp.wait()

    f32 = jnp.float32
    vmem = pl.BlockSpec(memory_space=pltpu.VMEM)
    hbm = pl.BlockSpec(memory_space=pltpu.HBM)
    blocks = [jax.ShapeDtypeStruct((q['n0'], q['n1']), f32) for q in mats]
    out_shape = (blocks + blocks + [jax.ShapeDtypeStruct((r,), f32) for r in rows_b]
                 + [jax.ShapeDtypeStruct((c,), f32) for c in cols])
    scratch = [pltpu.VMEM((2, q['n0'], q['n1']), f32) for q in mats]
    scratch += [pltpu.VMEM((n,), f32) for n in (*rows_b, *cols)] + [pltpu.SemaphoreType.DMA((3 * NM,))]
    return pl.pallas_call(
        kernel, out_shape=out_shape, in_specs=[vmem] * 9, out_specs=[hbm] * 16, scratch_shapes=scratch,
        compiler_params=pltpu.CompilerParams(vmem_limit_bytes=6 * MIB))


def solution(mesh):
    n_data = mesh.shape['data']
    n_model = mesh.shape['model']
    mat_spec = P('data', 'model')
    in_specs = (P('data', None, 'model'), mat_spec, P('data'), P('model')) * NM
    out_specs = (mat_spec, mat_spec, P('data'), P('model')) * NM

    def per_device(*arrays):
        grads, params = arrays[0::4], arrays[1::4]
        rows_b = [p.shape[0] for p in params]
        cols = [p.shape[1] for p in params]
        mats = layout_of(rows_b, cols, n_model, n_data)
        view = lambda i, a: jnp.swapaxes(a, -1, -2) if mats[i]['flip'] else a
        grads = [view(i, g) for i, g in enumerate(grads)]
        params = [view(i, p) for i, p in enumerate(params)]
        pin = lambda a: pltpu.with_memory_space_constraint(a, pltpu.HBM)
        outs = make_reduce_kernel(rows_b, cols, n_model, n_data)(
            *map(pin, grads), *map(pin, params), *map(pin, arrays[2::4]), *map(pin, arrays[3::4]))
        res = make_apply_kernel(rows_b, cols, n_model, n_data)(*outs)
        flat = []
        for m in range(NM):
            flat += [view(m, res[m]), view(m, res[4 + m]), res[8 + m], res[12 + m]]
        return tuple(flat)

    return jax.shard_map(per_device, mesh=mesh, in_specs=in_specs, out_specs=out_specs, check_vma=False)
```

```python
import jax
import jax.numpy as jnp
from jax import lax
from jax.experimental import pallas as pl
from jax.experimental.pallas import tpu as pltpu
from jax.sharding import PartitionSpec as P

OPT_STEP = 3
BETA = 1.0 - OPT_STEP ** -0.8
LR_REL = min(0.01, OPT_STEP ** -0.5)
NM = 4
OWN, NX, NY, ND = 0, 1, 2, 3
FIRST_ROWS = 88
PARTS = 4
LEAD_NS = 200
LANES = 128
TILE = (8, LANES)
MIB = 1024 * 1024
MESH_ID = pl.DeviceIdType.MESH


def layout_of(rows_b, cols, n_model, n_data):
    mats = []
    for r, c in zip(rows_b, cols):
        flip = c % LANES != 0
        n0, n1 = (c, r) if flip else (r, c)
        mats.append(dict(flip=flip, n0=n0, n1=n1, half=n0 // 2, groups=n0 // 8, tiles=-(-n0 // LANES), lanes=n1 // LANES,
                         rows_b=r, rows_t=r * n_data, cols_t=c * n_model,
                         size=float(r * n_data * c * n_model)))
    return mats


def make_reduce_kernel(rows_b, cols, n_model, n_data):
    mats = layout_of(rows_b, cols, n_model, n_data)
    halves = [q['half'] for q in mats]
    n_rc = [(q['lanes'], 8) if q['flip'] else (8, q['lanes']) for q in mats]
    sent_rows = sum(7 * q['n0'] * q['lanes'] for q in mats) + n_model * n_data - 1
    sent_rows += sum(3 * r + (24 if c == 8 else 7 * c) for r, c in n_rc)
    first = []
    for lo, hi in ((0, FIRST_ROWS), (FIRST_ROWS, halves[0])):
        first += [(0, ND, lo, hi - lo), (0, ND, halves[0] + lo, hi - lo)]
    group = {m: [(m, j, 0, mats[m]['n0']) for j in ((NX, NY, OWN) if m == 0 else (ND, NX, NY, OWN))] for m in range(NM)}

    def kernel(*refs):
        grads = refs[0:4]
        params = refs[4:8]
        vrows = refs[8:12]
        vcols = refs[12:16]
        upd = refs[16:20]
        wbuf = refs[20:24]
        stats = refs[24]
        sc = list(refs[25:])
        take = lambda n: [sc.pop(0) for _ in range(n)]
        loc, rec, fxy, vrbuf, vcbuf = (take(4) for _ in range(5))
        stg, rmsg, rrx, cmsg, crx, csib, chalf, brx, vrc, vcc, stage, sent = take(12)
        ld_sem, dd_r, l_r, col_r, s_sem, greet = take(6)
        row_in = lambda m: ld_sem.at[m]
        col_in = lambda m: col_r.at[m]
        pair_in = lambda m: dd_r.at[m]
        merge_in = lambda m: dd_r.at[2 + m]
        totals_in = dd_r.at[NM]

        z = lax.axis_index('model')
        d = lax.axis_index('data')
        core = lax.rem(d, 2)
        xx = lax.rem(d // 2, 2)
        yy = d // 4
        sib_step = 1 - 2 * core
        sib = d + sib_step
        dx = d + 2 - 4 * xx
        dy = d + 4 - 8 * yy
        dd = dx + 4 - 8 * yy
        owner = {OWN: d, NX: dx, NY: dy, ND: dd}

        def flip_d(k):
            return d + (k % 2) * sib_step + (k // 2 % 2) * (2 - 4 * xx) + (k // 4) * (4 - 8 * yy)

        def flip_z(k):
            return z + (k % 2) * (1 - 2 * lax.rem(z, 2)) + (k // 2) * (2 - 4 * (z // 2))

        def remote(src, dst, ssem, rsem, data=None, model=None):
            return pltpu.make_async_remote_copy(
                src_ref=src, dst_ref=dst, send_sem=ssem, recv_sem=rsem,
                device_id=(z if model is None else model, d if data is None else data),
                device_id_type=MESH_ID)

        def signal(sem, data=None, model=None):
            pl.semaphore_signal(
                sem, inc=1,
                device_id=(z if model is None else model, d if data is None else data),
                device_id_type=MESH_ID)

        def wait_bytes(ref, sem):
            pltpu.make_async_copy(ref, ref, sem).wait()

        barrier = pltpu.get_barrier_semaphore()
        first_core, second_core = core == 0, core == 1
        up_ok = z < n_model - 1
        down_ok = z > 0
        n_z = jnp.where(up_ok, 1, 0) + jnp.where(down_ok, 1, 0)

        def signal_z(sem, data=None, also=None):
            @pl.when(up_ok if also is None else up_ok & also)
            def _():
                signal(sem, data=data, model=z + 1)

            @pl.when(down_ok if also is None else down_ok & also)
            def _():
                signal(sem, data=data, model=z - 1)

        @pl.when(second_core)
        def _():
            signal(barrier, data=sib)

        def block(who, f):
            m, j, r0, n = f
            q = mats[m]
            if q['flip']:
                cut = pl.ds(pl.multiple_of(who * q['n1'], LANES), q['n1'])
                return grads[m].at[0, pl.ds(r0, n), cut]
            return grads[m].at[0, pl.ds(pl.multiple_of(who * q['n0'] + r0, 8), n), :]

        loads, dsend, stage_in = {}, {}, {}
        for f in first + group[0] + group[1] + group[2] + group[3]:
            m, j, r0, n = f
            slot = first.index(f) if f in first else 4 + m
            loads[f] = pltpu.make_async_copy(block(owner[j], f), loc[m].at[j, pl.ds(r0, n), :], ld_sem.at[slot])
            source = block(owner[j] + sib_step, f)
            if f in first:
                held = stg.at[pl.ds(r0, n), :]
                stage_in[f] = pltpu.make_async_copy(source, held, ld_sem.at[4 + slot])
                source = held
            dsend[f] = remote(source, rec[m].at[j, pl.ds(r0, n), :], s_sem.at[0], dd_r.at[slot], data=sib)

        def fetch(pieces):
            for f in pieces:
                dsend[f].start()
                loads[f].start()

        def fetch_done(m):
            some = pl.ds(0, 3) if m == 0 else pl.ds(0, 4)
            wait_bytes(loc[m].at[some], ld_sem.at[4 + m])
            wait_bytes(rec[m].at[some], dd_r.at[4 + m])

        def link_send(m, j, r0, n):
            h, off = (0, r0) if r0 < halves[m] else (1, r0 - halves[m])
            along_x = (j == ND and h == 0) or j == NX
            slot = (0 if along_x else 1) if j == ND else (2 if along_x else 4) + h
            return remote(loc[m].at[j, pl.ds(r0, n), :], fxy[m].at[slot, pl.ds(off, n), :],
                          s_sem.at[0], l_r.at[2 * m + (0 if j == ND else 1)], data=dx if along_x else dy)

        def relays_in(m):
            wait_bytes(fxy[m].at[pl.ds(0, 2)], l_r.at[2 * m])

        def finals_in(m):
            wait_bytes(fxy[m].at[pl.ds(2, 4)], l_r.at[2 * m + 1])

        def pair_sum(m, j, r0, n, relay=None):
            total = loc[m][j, r0:r0 + n, :] + rec[m][j, r0:r0 + n, :]
            if relay is not None:
                total = total + fxy[m][relay]
            loc[m][j, r0:r0 + n, :] = total
            link_send(m, j, r0, n).start()

        def send_raw(m):
            n = halves[m]
            fetch_done(m)
            if m > 0:
                pair_sum(m, ND, 0, n)
                pair_sum(m, ND, n, n)
            pair_sum(m, NX, 0, n)
            pair_sum(m, NY, n, n)

        def send_acc(m):
            n = halves[m]
            relays_in(m)
            pair_sum(m, NY, 0, n, 0)
            pair_sum(m, NX, n, n, 1)

        for f in first:
            stage_in[f].start()
            loads[f].start()

        @pl.when(first_core)
        def _():
            pl.semaphore_wait(barrier, 1)
            signal(barrier, data=dx + 1)
            signal(barrier, data=dy + 1)
            signal(greet.at[3], data=sib)

        signal_z(barrier, data=sib, also=first_core)

        @pl.when(second_core)
        def _():
            pl.semaphore_wait(greet.at[3], 1)

        for f in first:
            stage_in[f].wait()
            dsend[f].start()

        @pl.when(second_core)
        def _():
            pl.semaphore_wait(barrier, 2 + n_z)
            signal(greet.at[4], data=sib)

        @pl.when(first_core)
        def _():
            pl.semaphore_wait(greet.at[4], 1)

        def first_done(pieces):
            for f in pieces:
                loads[f].wait()
                dsend[f].wait_recv()

        @pl.when(second_core)
        def _():
            first_done(first[2:])
            pl.delay(LEAD_NS)

        first_done(first[:2])
        for f in first[:2]:
            pair_sum(*f)
        fetch(group[0])
        pl.when(first_core)(lambda: first_done(first[2:]))
        for f in first[2:]:
            pair_sum(*f)
        fetch(group[1])
        send_raw(0)
        fetch(group[2])
        send_raw(1)
        fetch(group[3])
        small = [pltpu.make_async_copy(vrows[m], vrbuf[m], ld_sem.at[m]) for m in range(NM)]
        small += [pltpu.make_async_copy(vcols[m], vcbuf[m], ld_sem.at[4 + m]) for m in range(2)]
        late = [pltpu.make_async_copy(params[m], wbuf[m], ld_sem.at[m]) for m in range(NM)]
        late += [pltpu.make_async_copy(vcols[m], vcbuf[m], ld_sem.at[2 + m]) for m in range(2, NM)]
        for turn in (small, late):
            for cp in turn:
                cp.start()
            for cp in turn:
                cp.wait()

        lane = lax.broadcasted_iota(jnp.int32, TILE, 1)
        sub = lax.broadcasted_iota(jnp.int32, TILE, 0)
        lane1 = lax.broadcasted_iota(jnp.int32, (1, LANES), 1)

        def group_mask(g):
            shape = (g, 8, LANES)
            return lax.broadcasted_iota(jnp.int32, shape, 2) == lax.broadcasted_iota(jnp.int32, shape, 0)

        def compact(values):
            return jnp.sum(jnp.where(group_mask(values.shape[0]), values, 0.0), axis=0)

        def expand(vec, g):
            return jnp.sum(jnp.where(group_mask(g), vec[None], 0.0), axis=2, keepdims=True)

        def rows_of(buf, n, i):
            stage[i] = jnp.zeros(TILE, jnp.float32)
            for t in range(-(-n // LANES)):
                n_t = min(LANES, n - LANES * t)
                stage[i, t:t + 1, 0:n_t] = buf[pl.ds(LANES * t, n_t)].reshape(1, n_t)

        def to_compact(i, n):
            out = jnp.zeros(TILE, jnp.float32)
            for t in range(-(-n // LANES)):
                row = jnp.broadcast_to(stage[i, t:t + 1, :], TILE)
                for g in range(min(LANES, n - LANES * t) // 8):
                    col = jnp.sum(jnp.where(lane == 8 * g + sub, row, 0.0), axis=1, keepdims=True)
                    out = jnp.where(lane == 16 * t + g, col, out)
            return out

        bv = jnp.zeros((1, LANES), jnp.float32)
        for m in range(NM):
            q = mats[m]
            w = wbuf[m][...]
            part = jnp.sum(w * w, axis=(0, 1), keepdims=True) * (1.0 / q['size'])
            bv = jnp.where(lane1 == 2 * NM + m, part, bv)
            rows_of(vrbuf[m], q['rows_b'], 2 * m)
            rows_of(vcbuf[m], cols[m], 2 * m + 1)
            if q['flip']:
                vrc[m] = stage[2 * m]
                vcc[m] = to_compact(2 * m + 1, q['n0'])
            else:
                vrc[m] = to_compact(2 * m, q['n0'])
                vcc[m] = stage[2 * m + 1]

        for i in range(3):
            signal_z(greet.at[i])
            pl.semaphore_wait(greet.at[i], n_z)

        def send_rows(m):
            n_r = n_rc[m][0]
            for k in (3, 2, 1):
                remote(rmsg.at[m, pl.ds(0, n_r)], rrx.at[3 * m + k - 1, pl.ds(0, n_r)], s_sem.at[0], row_in(m),
                       model=flip_z(k)).start()

        def send_cols(m, ks):
            n_c = n_rc[m][1]
            for k in ks:
                remote(cmsg.at[m, pl.ds(0, n_c)], crx.at[7 * m + k - 1, pl.ds(0, n_c)], s_sem.at[0], col_in(m),
                       data=flip_d(k)).start()

        def share_pair(m):
            wait_bytes(csib.at[m], pair_in(m))
            mine = jnp.where(core == 0, csib[m, 0:4, :] + cmsg[m, 0:4, :], csib[m, 4:8, :] + cmsg[m, 4:8, :])
            chalf[m, 0] = mine
            for k, peer in enumerate((dd, dx, dy)):
                remote(chalf.at[m, 0], chalf.at[m, 1 + k], s_sem.at[0], col_in(m), data=peer).start()

        def merge_pair(m):
            wait_bytes(chalf.at[m, pl.ds(1, 3)], col_in(m))
            chalf[m, 4] = chalf[m, 0] + chalf[m, 1] + chalf[m, 2] + chalf[m, 3]
            remote(chalf.at[m, 4], chalf.at[m, 5], s_sem.at[0], merge_in(m), data=sib).start()

        def merged(m):
            wait_bytes(chalf.at[m, 5], merge_in(m))
            mine, other = chalf[m, 4], chalf[m, 5]
            return jnp.concatenate([jnp.where(core == 0, mine, other), jnp.where(core == 0, other, mine)], axis=0)


        def finish_sum(m):
            q = mats[m]
            half, n1 = q['half'], q['n1']
            acc1 = jnp.zeros((8, n1), jnp.float32)
            rsums = []
            finals_in(m)
            for h in range(2):
                rows = slice(h * half, (h + 1) * half)
                total = loc[m][OWN, rows, :] + rec[m][OWN, rows, :] + fxy[m][2 + h] + fxy[m][4 + h]
                upd[m][rows, :] = total
                sq = (total * total + 1e-30).reshape(half // 8, 8, n1)
                acc1 = acc1 + jnp.sum(sq, axis=0)
                rsums.append(jnp.sum(sq, axis=2, keepdims=True))
            sum1 = jnp.sum(acc1, axis=0, keepdims=True)
            msg0, msg1 = (cmsg, rmsg) if q['flip'] else (rmsg, cmsg)
            for k in range(q['lanes']):
                msg1[m, k:k + 1, :] = sum1[:, LANES * k:LANES * k + LANES]
            if not q['flip']:
                send_cols(m, (6, 7, 2, 4, 3, 5, 1))
            msg0[m] = compact(jnp.concatenate(rsums, axis=0))
            send_rows(m)
            if q['flip']:
                remote(cmsg.at[m], csib.at[m], s_sem.at[0], pair_in(m), data=sib).start()

        def along0(m, fac):
            return expand(fac, mats[m]['groups'])

        def along1(m, fac):
            wide = [jnp.broadcast_to(fac[k:k + 1, :], TILE) for k in range(mats[m]['lanes'])]
            return jnp.concatenate(wide, axis=1)[None]

        def apply_rows(m, bv, locrow):
            q = mats[m]
            n_r = n_rc[m][0]
            ok = lane < q['groups']
            rtot = rmsg[m, 0:n_r, :]
            wait_bytes(loc[0].at[0, pl.ds(0, 3 * n_r), :], row_in(m))
            for k in range(3):
                rtot = rtot + rrx[3 * m + k, 0:n_r, :]
            vr = BETA * vrc[m, 0:n_r, :] + (1.0 - BETA) * (rtot * (1.0 / q['cols_t']))
            vr_sum = jnp.sum(vr if q['flip'] else jnp.where(ok, vr, 0.0), axis=(0, 1), keepdims=True)
            mloc = vr_sum * (1.0 / q['rows_b'])
            rfac = lax.rsqrt(vr / mloc) if q['flip'] else lax.rsqrt(jnp.where(ok, vr / mloc, 1.0))
            part = upd[m][...].reshape(q['groups'], 8, q['n1']) * (along1 if q['flip'] else along0)(m, rfac)
            upd[m][...] = part.reshape(q['n0'], q['n1'])
            vrc[m, 0:n_r, :] = vr
            bv = jnp.where(lane1 == NM + m, vr_sum * (1.0 / (q['rows_t'] * n_model)), bv)
            locrow = jnp.where(lane1 == m, mloc, locrow)
            return bv, locrow, 1.0 / mloc

        def apply_cols(m, bv, inv_mloc):
            q = mats[m]
            n_c = n_rc[m][1]
            if n_c == 8:
                ctot = merged(m)
            else:
                ctot = cmsg[m, 0:n_c, :]
                wait_bytes(loc[0].at[0, pl.ds(0, 7 * n_c), :], col_in(m))
                for k in range(7):
                    ctot = ctot + crx[7 * m + k, 0:n_c, :]
            vc = BETA * vcc[m, 0:n_c, :] + (1.0 - BETA) * (ctot * (1.0 / q['rows_t']))
            cfac = lax.rsqrt(jnp.where(lane < q['groups'], vc, 1.0)) if q['flip'] else lax.rsqrt(vc)
            u = upd[m][...].reshape(q['groups'], 8, q['n1']) * (along0 if q['flip'] else along1)(m, cfac)
            t_m = jnp.sum(jnp.sum(u * u, axis=0), axis=(0, 1), keepdims=True)
            upd[m][...] = u.reshape(q['n0'], q['n1'])
            vcc[m, 0:n_c, :] = vc
            return jnp.where(lane1 == m, (t_m * (1.0 / q['size'])) * inv_mloc, bv)

        locrow = jnp.ones((1, LANES), jnp.float32)
        send_acc(0)
        send_raw(2)
        send_acc(1)
        finish_sum(0)
        send_raw(3)
        send_acc(2)
        finish_sum(1)
        send_acc(3)
        share_pair(0)
        share_pair(1)
        bv, locrow, inv0 = apply_rows(0, bv, locrow)
        bv, locrow, inv1 = apply_rows(1, bv, locrow)
        finish_sum(2)
        finish_sum(3)
        merge_pair(0)
        merge_pair(1)
        bv, locrow, inv2 = apply_rows(2, bv, locrow)
        bv = apply_cols(0, bv, inv0)
        bv = apply_cols(1, bv, inv1)
        bv = apply_cols(2, bv, inv2)
        bv, locrow, inv3 = apply_rows(3, bv, locrow)
        bv = apply_cols(3, bv, inv3)

        brx[0:1, :] = bv
        for kz in (3, 2, 1, 0):
            for kd in range(n_data - 1, -1, -1):
                if kz == 0 and kd == 0:
                    continue
                i = kz * n_data + kd
                remote(brx.at[pl.ds(0, 1), :], brx.at[pl.ds(i, 1), :], s_sem.at[0], totals_in,
                       data=flip_d(kd), model=flip_z(kz)).start()

        for m in range(NM):
            q = mats[m]
            lined, packed = (vrc, vcc) if q['flip'] else (vcc, vrc)
            stats[1 + 2 * m, 0:q['lanes'], :] = lined[m, 0:q['lanes'], :]
            wide = expand(packed[m], q['groups'])
            for t in range(q['tiles']):
                n_t = min(LANES, q['n0'] - LANES * t)
                g_n = n_t // 8
                shape = (g_n, 8, LANES)
                pick = (lax.broadcasted_iota(jnp.int32, shape, 2)
                        == 8 * lax.broadcasted_iota(jnp.int32, shape, 0) + lax.broadcasted_iota(jnp.int32, shape, 1))
                rows = jnp.sum(jnp.where(pick, wide[16 * t:16 * t + g_n], 0.0), axis=0)
                stats[2 + 2 * m, t:t + 1, :] = jnp.sum(rows, axis=0, keepdims=True)

        wait_bytes(brx.at[pl.ds(1, n_model * n_data - 1), :], totals_in)
        tot = jnp.broadcast_to(jnp.sum(brx[...], axis=0, keepdims=True), TILE)
        mean_vr = pltpu.roll(tot, LANES - NM, 1)
        u_rms = jnp.sqrt(mean_vr * tot)
        w_rms = jnp.sqrt(pltpu.roll(tot, LANES - 2 * NM, 1))
        fac = -(LR_REL * jnp.maximum(1e-3, w_rms)) * (jnp.sqrt(mean_vr) * lax.rsqrt(locrow))
        stats[0] = fac / jnp.maximum(1.0, u_rms)
        wait_bytes(sent, s_sem.at[0])

    f32 = jnp.float32
    dma = pltpu.SemaphoreType.DMA
    vm = pltpu.VMEM
    scratch = []
    scratch += [vm((4, q['n0'], q['n1']), f32) for q in mats]
    scratch += [vm((4, q['n0'], q['n1']), f32) for q in mats]
    scratch += [vm((6, q['half'], q['n1']), f32) for q in mats]
    scratch += [vm((r,), f32) for r in rows_b]
    scratch += [vm((c,), f32) for c in cols]
    scratch += [vm((mats[0]['n0'], mats[0]['n1']), f32)]
    tile = lambda *lead: vm((*lead, 8, LANES), f32)
    scratch += [tile(NM), tile(3 * NM), tile(NM), tile(7 * NM), tile(2), vm((2, 6, 4, LANES), f32), vm((n_model * n_data, LANES), f32),
                tile(NM), tile(NM), tile(2 * NM), vm((sent_rows, LANES), f32)]
    scratch += [dma((8,)), dma((8,)), dma((2 * NM,)), dma((NM,)), dma((1,)), pltpu.SemaphoreType.REGULAR((5,))]
    blocks = [jax.ShapeDtypeStruct((q['n0'], q['n1']), f32) for q in mats]
    out_shape = blocks + blocks + [jax.ShapeDtypeStruct((1 + 2 * NM, 8, LANES), f32)]
    vmem = pl.BlockSpec(memory_space=pltpu.VMEM)
    hbm = pl.BlockSpec(memory_space=pltpu.HBM)
    return pl.pallas_call(
        kernel, out_shape=out_shape, in_specs=[hbm] * 16, out_specs=[vmem] * len(out_shape),
        scratch_shapes=scratch,
        compiler_params=pltpu.CompilerParams(collective_id=0, has_side_effects=True,
                                             vmem_limit_bytes=36 * MIB))


def make_apply_kernel(rows_b, cols, n_model, n_data):
    mats = layout_of(rows_b, cols, n_model, n_data)

    def kernel(*refs):
        upd, params, stats = refs[0:4], refs[4:8], refs[8]
        new, delta, vrow_out, vcol_out = refs[9:13], refs[13:17], refs[17:21], refs[21:25]
        bufs, vrbuf, vcbuf = refs[25:29], refs[29:33], refs[33:37]
        sem = refs[37]
        for m in range(NM):
            fac = stats[0, 0:1, m:m + 1]
            n = mats[m]['n0'] // PARTS
            for i in range(PARTS):
                rows = slice(i * n, i * n + n)
                step = fac * upd[m][rows, :]
                bufs[m][0, rows, :] = step
                pltpu.make_async_copy(bufs[m].at[0, rows], delta[m].at[rows], sem.at[m]).start()
                bufs[m][1, rows, :] = params[m][rows, :] + step
                pltpu.make_async_copy(bufs[m].at[1, rows], new[m].at[rows], sem.at[m]).start()
        copies = []
        for m in range(NM):
            q = mats[m]
            out1, out0 = (vrbuf[m], vcbuf[m]) if q['flip'] else (vcbuf[m], vrbuf[m])
            for k in range(q['lanes']):
                out1[pl.ds(LANES * k, LANES)] = stats[1 + 2 * m, k:k + 1, :].reshape(LANES)
            for t in range(q['tiles']):
                n_t = min(LANES, q['n0'] - LANES * t)
                out0[pl.ds(LANES * t, n_t)] = stats[2 + 2 * m, t:t + 1, 0:n_t].reshape(n_t)
            for i, (buf, out) in enumerate(((vrbuf[m], vrow_out[m]), (vcbuf[m], vcol_out[m]))):
                copies.append(pltpu.make_async_copy(buf, out, sem.at[NM + 2 * m + i]))
                copies[-1].start()
        for m in range(NM):
            pltpu.make_async_copy(bufs[m], bufs[m], sem.at[m]).wait()
        for cp in copies:
            cp.wait()

    f32 = jnp.float32
    vmem = pl.BlockSpec(memory_space=pltpu.VMEM)
    hbm = pl.BlockSpec(memory_space=pltpu.HBM)
    blocks = [jax.ShapeDtypeStruct((q['n0'], q['n1']), f32) for q in mats]
    out_shape = (blocks + blocks + [jax.ShapeDtypeStruct((r,), f32) for r in rows_b]
                 + [jax.ShapeDtypeStruct((c,), f32) for c in cols])
    scratch = [pltpu.VMEM((2, q['n0'], q['n1']), f32) for q in mats]
    scratch += [pltpu.VMEM((n,), f32) for n in (*rows_b, *cols)] + [pltpu.SemaphoreType.DMA((3 * NM,))]
    return pl.pallas_call(
        kernel, out_shape=out_shape, in_specs=[vmem] * 9, out_specs=[hbm] * 16, scratch_shapes=scratch,
        compiler_params=pltpu.CompilerParams(vmem_limit_bytes=6 * MIB))


def solution(mesh):
    n_data = mesh.shape['data']
    n_model = mesh.shape['model']
    mat_spec = P('data', 'model')
    in_specs = (P('data', None, 'model'), mat_spec, P('data'), P('model')) * NM
    out_specs = (mat_spec, mat_spec, P('data'), P('model')) * NM

    def per_device(*arrays):
        grads, params = arrays[0::4], arrays[1::4]
        rows_b = [p.shape[0] for p in params]
        cols = [p.shape[1] for p in params]
        mats = layout_of(rows_b, cols, n_model, n_data)
        view = lambda i, a: jnp.swapaxes(a, -1, -2) if mats[i]['flip'] else a
        grads = [view(i, g) for i, g in enumerate(grads)]
        params = [view(i, p) for i, p in enumerate(params)]
        pin = lambda a: pltpu.with_memory_space_constraint(a, pltpu.HBM)
        outs = make_reduce_kernel(rows_b, cols, n_model, n_data)(
            *map(pin, grads), *map(pin, params), *map(pin, arrays[2::4]), *map(pin, arrays[3::4]))
        res = make_apply_kernel(rows_b, cols, n_model, n_data)(*outs)
        flat = []
        for m in range(NM):
            flat += [view(m, res[m]), view(m, res[4 + m]), res[8 + m], res[12 + m]]
        return tuple(flat)

    return jax.shard_map(per_device, mesh=mesh, in_specs=in_specs, out_specs=out_specs, check_vma=False)
```

```python
import jax
import jax.numpy as jnp
from jax import lax
from jax.experimental import pallas as pl
from jax.experimental.pallas import tpu as pltpu
from jax.sharding import PartitionSpec as P

OPT_STEP = 3
BETA = 1.0 - OPT_STEP ** -0.8
LR_REL = min(0.01, OPT_STEP ** -0.5)
NM = 4
OWN, NX, NY, ND = 0, 1, 2, 3
FIRST_ROWS = 88
PARTS = 4
LEAD_NS = 200
LANES = 128
TILE = (8, LANES)
MIB = 1024 * 1024
MESH_ID = pl.DeviceIdType.MESH


def layout_of(rows_b, cols, n_model, n_data):
    mats = []
    for r, c in zip(rows_b, cols):
        flip = c % LANES != 0
        n0, n1 = (c, r) if flip else (r, c)
        mats.append(dict(flip=flip, n0=n0, n1=n1, half=n0 // 2, groups=n0 // 8, tiles=-(-n0 // LANES), lanes=n1 // LANES,
                         rows_b=r, rows_t=r * n_data, cols_t=c * n_model,
                         size=float(r * n_data * c * n_model)))
    return mats


def make_reduce_kernel(rows_b, cols, n_model, n_data):
    mats = layout_of(rows_b, cols, n_model, n_data)
    halves = [q['half'] for q in mats]
    n_rc = [(q['lanes'], 8) if q['flip'] else (8, q['lanes']) for q in mats]
    sent_rows = sum(7 * q['n0'] * q['lanes'] for q in mats) + n_model * n_data - 1
    sent_rows += sum(3 * r + (24 if c == 8 else 7 * c) for r, c in n_rc)
    first = []
    for lo, hi in ((0, FIRST_ROWS), (FIRST_ROWS, halves[0])):
        first += [(0, ND, lo, hi - lo), (0, ND, halves[0] + lo, hi - lo)]
    group = {m: [(m, j, 0, mats[m]['n0']) for j in ((NX, NY, OWN) if m == 0 else (ND, NX, NY, OWN))] for m in range(NM)}

    def kernel(*refs):
        grads = refs[0:4]
        params = refs[4:8]
        vrows = refs[8:12]
        vcols = refs[12:16]
        upd = refs[16:20]
        wbuf = refs[20:24]
        stats = refs[24]
        sc = list(refs[25:])
        take = lambda n: [sc.pop(0) for _ in range(n)]
        loc, rec, fxy, vrbuf, vcbuf = (take(4) for _ in range(5))
        stg, rmsg, rrx, cmsg, crx, csib, chalf, brx, vrc, vcc, stage, sent = take(12)
        ld_sem, dd_r, l_r, col_r, s_sem, greet = take(6)
        row_in = lambda m: ld_sem.at[m]
        col_in = lambda m: col_r.at[m]
        pair_in = lambda m: dd_r.at[m]
        merge_in = lambda m: dd_r.at[2 + m]
        totals_in = dd_r.at[NM]

        z = lax.axis_index('model')
        d = lax.axis_index('data')
        core = lax.rem(d, 2)
        xx = lax.rem(d // 2, 2)
        yy = d // 4
        sib_step = 1 - 2 * core
        sib = d + sib_step
        dx = d + 2 - 4 * xx
        dy = d + 4 - 8 * yy
        dd = dx + 4 - 8 * yy
        owner = {OWN: d, NX: dx, NY: dy, ND: dd}

        def flip_d(k):
            return d + (k % 2) * sib_step + (k // 2 % 2) * (2 - 4 * xx) + (k // 4) * (4 - 8 * yy)

        def flip_z(k):
            return z + (k % 2) * (1 - 2 * lax.rem(z, 2)) + (k // 2) * (2 - 4 * (z // 2))

        def remote(src, dst, ssem, rsem, data=None, model=None):
            return pltpu.make_async_remote_copy(
                src_ref=src, dst_ref=dst, send_sem=ssem, recv_sem=rsem,
                device_id=(z if model is None else model, d if data is None else data),
                device_id_type=MESH_ID)

        def signal(sem, data=None, model=None):
            pl.semaphore_signal(
                sem, inc=1,
                device_id=(z if model is None else model, d if data is None else data),
                device_id_type=MESH_ID)

        def wait_bytes(ref, sem):
            pltpu.make_async_copy(ref, ref, sem).wait()

        barrier = pltpu.get_barrier_semaphore()
        first_core, second_core = core == 0, core == 1
        up_ok = z < n_model - 1
        down_ok = z > 0
        n_z = jnp.where(up_ok, 1, 0) + jnp.where(down_ok, 1, 0)

        def signal_z(sem, data=None, also=None):
            @pl.when(up_ok if also is None else up_ok & also)
            def _():
                signal(sem, data=data, model=z + 1)

            @pl.when(down_ok if also is None else down_ok & also)
            def _():
                signal(sem, data=data, model=z - 1)

        @pl.when(second_core)
        def _():
            signal(barrier, data=sib)

        def block(who, f):
            m, j, r0, n = f
            q = mats[m]
            if q['flip']:
                cut = pl.ds(pl.multiple_of(who * q['n1'], LANES), q['n1'])
                return grads[m].at[0, pl.ds(r0, n), cut]
            return grads[m].at[0, pl.ds(pl.multiple_of(who * q['n0'] + r0, 8), n), :]

        loads, dsend, stage_in = {}, {}, {}
        for f in first + group[0] + group[1] + group[2] + group[3]:
            m, j, r0, n = f
            slot = first.index(f) if f in first else 4 + m
            loads[f] = pltpu.make_async_copy(block(owner[j], f), loc[m].at[j, pl.ds(r0, n), :], ld_sem.at[slot])
            source = block(owner[j] + sib_step, f)
            if f in first:
                held = stg.at[pl.ds(r0, n), :]
                stage_in[f] = pltpu.make_async_copy(source, held, ld_sem.at[4 + slot])
                source = held
            dsend[f] = remote(source, rec[m].at[j, pl.ds(r0, n), :], s_sem.at[0], dd_r.at[slot], data=sib)

        def fetch(pieces):
            for f in pieces:
                dsend[f].start()
                loads[f].start()

        def fetch_done(m):
            some = pl.ds(0, 3) if m == 0 else pl.ds(0, 4)
            wait_bytes(loc[m].at[some], ld_sem.at[4 + m])
            wait_bytes(rec[m].at[some], dd_r.at[4 + m])

        def link_send(m, j, r0, n):
            h, off = (0, r0) if r0 < halves[m] else (1, r0 - halves[m])
            along_x = (j == ND and h == 0) or j == NX
            slot = (0 if along_x else 1) if j == ND else (2 if along_x else 4) + h
            return remote(loc[m].at[j, pl.ds(r0, n), :], fxy[m].at[slot, pl.ds(off, n), :],
                          s_sem.at[0], l_r.at[2 * m + (0 if j == ND else 1)], data=dx if along_x else dy)

        def relays_in(m):
            wait_bytes(fxy[m].at[pl.ds(0, 2)], l_r.at[2 * m])

        def finals_in(m):
            wait_bytes(fxy[m].at[pl.ds(2, 4)], l_r.at[2 * m + 1])

        def pair_sum(m, j, r0, n, relay=None):
            total = loc[m][j, r0:r0 + n, :] + rec[m][j, r0:r0 + n, :]
            if relay is not None:
                total = total + fxy[m][relay]
            loc[m][j, r0:r0 + n, :] = total
            link_send(m, j, r0, n).start()

        def send_raw(m):
            n = halves[m]
            fetch_done(m)
            if m > 0:
                pair_sum(m, ND, 0, n)
                pair_sum(m, ND, n, n)
            pair_sum(m, NX, 0, n)
            pair_sum(m, NY, n, n)

        def send_acc(m):
            n = halves[m]
            relays_in(m)
            pair_sum(m, NY, 0, n, 0)
            pair_sum(m, NX, n, n, 1)

        for f in first:
            stage_in[f].start()
            loads[f].start()

        @pl.when(first_core)
        def _():
            pl.semaphore_wait(barrier, 1)
            signal(barrier, data=dx + 1)
            signal(barrier, data=dy + 1)
            signal(greet.at[3], data=sib)

        signal_z(barrier, data=sib, also=first_core)

        @pl.when(second_core)
        def _():
            pl.semaphore_wait(greet.at[3], 1)

        for f in first:
            stage_in[f].wait()
            dsend[f].start()

        @pl.when(second_core)
        def _():
            pl.semaphore_wait(barrier, 2 + n_z)
            signal(greet.at[3], data=sib)

        @pl.when(first_core)
        def _():
            pl.semaphore_wait(greet.at[3], 1)

        def first_done(pieces):
            for f in pieces:
                loads[f].wait()
                dsend[f].wait_recv()

        @pl.when(second_core)
        def _():
            first_done(first[2:])
            pl.delay(LEAD_NS)

        first_done(first[:2])
        for f in first[:2]:
            pair_sum(*f)
        fetch(group[0])
        pl.when(first_core)(lambda: first_done(first[2:]))
        for f in first[2:]:
            pair_sum(*f)
        fetch(group[1])
        send_raw(0)
        fetch(group[2])
        send_raw(1)
        fetch(group[3])
        small = [pltpu.make_async_copy(vrows[m], vrbuf[m], ld_sem.at[m]) for m in range(NM)]
        small += [pltpu.make_async_copy(vcols[m], vcbuf[m], ld_sem.at[4 + m]) for m in range(2)]
        late = [pltpu.make_async_copy(params[m], wbuf[m], ld_sem.at[m]) for m in range(NM)]
        late += [pltpu.make_async_copy(vcols[m], vcbuf[m], ld_sem.at[2 + m]) for m in range(2, NM)]
        for turn in (small, late):
            for cp in turn:
                cp.start()
            for cp in turn:
                cp.wait()

        lane = lax.broadcasted_iota(jnp.int32, TILE, 1)
        sub = lax.broadcasted_iota(jnp.int32, TILE, 0)
        lane1 = lax.broadcasted_iota(jnp.int32, (1, LANES), 1)

        def group_mask(g):
            shape = (g, 8, LANES)
            return lax.broadcasted_iota(jnp.int32, shape, 2) == lax.broadcasted_iota(jnp.int32, shape, 0)

        def compact(values):
            return jnp.sum(jnp.where(group_mask(values.shape[0]), values, 0.0), axis=0)

        def expand(vec, g):
            return jnp.sum(jnp.where(group_mask(g), vec[None], 0.0), axis=2, keepdims=True)

        def rows_of(buf, n, i):
            stage[i] = jnp.zeros(TILE, jnp.float32)
            for t in range(-(-n // LANES)):
                n_t = min(LANES, n - LANES * t)
                stage[i, t:t + 1, 0:n_t] = buf[pl.ds(LANES * t, n_t)].reshape(1, n_t)

        def to_compact(i, n):
            out = jnp.zeros(TILE, jnp.float32)
            for t in range(-(-n // LANES)):
                row = jnp.broadcast_to(stage[i, t:t + 1, :], TILE)
                for g in range(min(LANES, n - LANES * t) // 8):
                    col = jnp.sum(jnp.where(lane == 8 * g + sub, row, 0.0), axis=1, keepdims=True)
                    out = jnp.where(lane == 16 * t + g, col, out)
            return out

        bv = jnp.zeros((1, LANES), jnp.float32)
        for m in range(NM):
            q = mats[m]
            w = wbuf[m][...]
            part = jnp.sum(w * w, axis=(0, 1), keepdims=True) * (1.0 / q['size'])
            bv = jnp.where(lane1 == 2 * NM + m, part, bv)
            rows_of(vrbuf[m], q['rows_b'], 2 * m)
            rows_of(vcbuf[m], cols[m], 2 * m + 1)
            if q['flip']:
                vrc[m] = stage[2 * m]
                vcc[m] = to_compact(2 * m + 1, q['n0'])
            else:
                vrc[m] = to_compact(2 * m, q['n0'])
                vcc[m] = stage[2 * m + 1]

        for i in range(3):
            signal_z(greet.at[i])
            pl.semaphore_wait(greet.at[i], n_z)

        def send_rows(m):
            n_r = n_rc[m][0]
            for k in (3, 2, 1):
                remote(rmsg.at[m, pl.ds(0, n_r)], rrx.at[3 * m + k - 1, pl.ds(0, n_r)], s_sem.at[0], row_in(m),
                       model=flip_z(k)).start()

        def send_cols(m, ks):
            n_c = n_rc[m][1]
            for k in ks:
                remote(cmsg.at[m, pl.ds(0, n_c)], crx.at[7 * m + k - 1, pl.ds(0, n_c)], s_sem.at[0], col_in(m),
                       data=flip_d(k)).start()

        def share_pair(m):
            wait_bytes(csib.at[m], pair_in(m))
            mine = jnp.where(core == 0, csib[m, 0:4, :] + cmsg[m, 0:4, :], csib[m, 4:8, :] + cmsg[m, 4:8, :])
            chalf[m, 0] = mine
            for k, peer in enumerate((dd, dx, dy)):
                remote(chalf.at[m, 0], chalf.at[m, 1 + k], s_sem.at[0], col_in(m), data=peer).start()

        def merge_pair(m):
            wait_bytes(chalf.at[m, pl.ds(1, 3)], col_in(m))
            chalf[m, 4] = chalf[m, 0] + chalf[m, 1] + chalf[m, 2] + chalf[m, 3]
            remote(chalf.at[m, 4], chalf.at[m, 5], s_sem.at[0], merge_in(m), data=sib).start()

        def merged(m):
            wait_bytes(chalf.at[m, 5], merge_in(m))
            mine, other = chalf[m, 4], chalf[m, 5]
            return jnp.concatenate([jnp.where(core == 0, mine, other), jnp.where(core == 0, other, mine)], axis=0)


        def finish_sum(m):
            q = mats[m]
            half, n1 = q['half'], q['n1']
            acc1 = jnp.zeros((8, n1), jnp.float32)
            rsums = []
            finals_in(m)
            for h in range(2):
                rows = slice(h * half, (h + 1) * half)
                total = loc[m][OWN, rows, :] + rec[m][OWN, rows, :] + fxy[m][2 + h] + fxy[m][4 + h]
                upd[m][rows, :] = total
                sq = (total * total + 1e-30).reshape(half // 8, 8, n1)
                acc1 = acc1 + jnp.sum(sq, axis=0)
                rsums.append(jnp.sum(sq, axis=2, keepdims=True))
            sum1 = jnp.sum(acc1, axis=0, keepdims=True)
            msg0, msg1 = (cmsg, rmsg) if q['flip'] else (rmsg, cmsg)
            for k in range(q['lanes']):
                msg1[m, k:k + 1, :] = sum1[:, LANES * k:LANES * k + LANES]
            if not q['flip']:
                send_cols(m, (6, 7, 2, 4, 3, 5, 1))
            msg0[m] = compact(jnp.concatenate(rsums, axis=0))
            send_rows(m)
            if q['flip']:
                remote(cmsg.at[m], csib.at[m], s_sem.at[0], pair_in(m), data=sib).start()

        def along0(m, fac):
            return expand(fac, mats[m]['groups'])

        def along1(m, fac):
            wide = [jnp.broadcast_to(fac[k:k + 1, :], TILE) for k in range(mats[m]['lanes'])]
            return jnp.concatenate(wide, axis=1)[None]

        def apply_rows(m, bv, locrow):
            q = mats[m]
            n_r = n_rc[m][0]
            ok = lane < q['groups']
            rtot = rmsg[m, 0:n_r, :]
            wait_bytes(loc[0].at[0, pl.ds(0, 3 * n_r), :], row_in(m))
            for k in range(3):
                rtot = rtot + rrx[3 * m + k, 0:n_r, :]
            vr = BETA * vrc[m, 0:n_r, :] + (1.0 - BETA) * (rtot * (1.0 / q['cols_t']))
            vr_sum = jnp.sum(vr if q['flip'] else jnp.where(ok, vr, 0.0), axis=(0, 1), keepdims=True)
            mloc = vr_sum * (1.0 / q['rows_b'])
            rfac = lax.rsqrt(vr / mloc) if q['flip'] else lax.rsqrt(jnp.where(ok, vr / mloc, 1.0))
            part = upd[m][...].reshape(q['groups'], 8, q['n1']) * (along1 if q['flip'] else along0)(m, rfac)
            upd[m][...] = part.reshape(q['n0'], q['n1'])
            vrc[m, 0:n_r, :] = vr
            bv = jnp.where(lane1 == NM + m, vr_sum * (1.0 / (q['rows_t'] * n_model)), bv)
            locrow = jnp.where(lane1 == m, mloc, locrow)
            return bv, locrow, 1.0 / mloc

        def apply_cols(m, bv, inv_mloc):
            q = mats[m]
            n_c = n_rc[m][1]
            if n_c == 8:
                ctot = merged(m)
            else:
                ctot = cmsg[m, 0:n_c, :]
                wait_bytes(loc[0].at[0, pl.ds(0, 7 * n_c), :], col_in(m))
                for k in range(7):
                    ctot = ctot + crx[7 * m + k, 0:n_c, :]
            vc = BETA * vcc[m, 0:n_c, :] + (1.0 - BETA) * (ctot * (1.0 / q['rows_t']))
            cfac = lax.rsqrt(jnp.where(lane < q['groups'], vc, 1.0)) if q['flip'] else lax.rsqrt(vc)
            u = upd[m][...].reshape(q['groups'], 8, q['n1']) * (along0 if q['flip'] else along1)(m, cfac)
            t_m = jnp.sum(jnp.sum(u * u, axis=0), axis=(0, 1), keepdims=True)
            upd[m][...] = u.reshape(q['n0'], q['n1'])
            vcc[m, 0:n_c, :] = vc
            return jnp.where(lane1 == m, (t_m * (1.0 / q['size'])) * inv_mloc, bv)

        locrow = jnp.ones((1, LANES), jnp.float32)
        send_acc(0)
        send_raw(2)
        send_acc(1)
        finish_sum(0)
        send_raw(3)
        send_acc(2)
        finish_sum(1)
        send_acc(3)
        share_pair(0)
        share_pair(1)
        bv, locrow, inv0 = apply_rows(0, bv, locrow)
        bv, locrow, inv1 = apply_rows(1, bv, locrow)
        finish_sum(2)
        finish_sum(3)
        merge_pair(0)
        merge_pair(1)
        bv, locrow, inv2 = apply_rows(2, bv, locrow)
        bv = apply_cols(0, bv, inv0)
        bv = apply_cols(1, bv, inv1)
        bv = apply_cols(2, bv, inv2)
        bv, locrow, inv3 = apply_rows(3, bv, locrow)
        bv = apply_cols(3, bv, inv3)

        brx[0:1, :] = bv
        for kz in (3, 2, 1, 0):
            for kd in (6, 7, 2, 4, 0, 3, 5, 1):
                if kz == 0 and kd == 0:
                    continue
                i = kz * n_data + kd
                remote(brx.at[pl.ds(0, 1), :], brx.at[pl.ds(i, 1), :], s_sem.at[0], totals_in,
                       data=flip_d(kd), model=flip_z(kz)).start()

        for m in range(NM):
            q = mats[m]
            lined, packed = (vrc, vcc) if q['flip'] else (vcc, vrc)
            stats[1 + 2 * m, 0:q['lanes'], :] = lined[m, 0:q['lanes'], :]
            wide = expand(packed[m], q['groups'])
            for t in range(q['tiles']):
                n_t = min(LANES, q['n0'] - LANES * t)
                g_n = n_t // 8
                shape = (g_n, 8, LANES)
                pick = (lax.broadcasted_iota(jnp.int32, shape, 2)
                        == 8 * lax.broadcasted_iota(jnp.int32, shape, 0) + lax.broadcasted_iota(jnp.int32, shape, 1))
                rows = jnp.sum(jnp.where(pick, wide[16 * t:16 * t + g_n], 0.0), axis=0)
                stats[2 + 2 * m, t:t + 1, :] = jnp.sum(rows, axis=0, keepdims=True)

        wait_bytes(brx.at[pl.ds(1, n_model * n_data - 1), :], totals_in)
        tot = jnp.broadcast_to(jnp.sum(brx[...], axis=0, keepdims=True), TILE)
        mean_vr = pltpu.roll(tot, LANES - NM, 1)
        u_rms = jnp.sqrt(mean_vr * tot)
        w_rms = jnp.sqrt(pltpu.roll(tot, LANES - 2 * NM, 1))
        fac = -(LR_REL * jnp.maximum(1e-3, w_rms)) * (jnp.sqrt(mean_vr) * lax.rsqrt(locrow))
        stats[0] = fac / jnp.maximum(1.0, u_rms)
        wait_bytes(sent, s_sem.at[0])

    f32 = jnp.float32
    dma = pltpu.SemaphoreType.DMA
    vm = pltpu.VMEM
    scratch = []
    scratch += [vm((4, q['n0'], q['n1']), f32) for q in mats]
    scratch += [vm((4, q['n0'], q['n1']), f32) for q in mats]
    scratch += [vm((6, q['half'], q['n1']), f32) for q in mats]
    scratch += [vm((r,), f32) for r in rows_b]
    scratch += [vm((c,), f32) for c in cols]
    scratch += [vm((mats[0]['n0'], mats[0]['n1']), f32)]
    tile = lambda *lead: vm((*lead, 8, LANES), f32)
    scratch += [tile(NM), tile(3 * NM), tile(NM), tile(7 * NM), tile(2), vm((2, 6, 4, LANES), f32), vm((n_model * n_data, LANES), f32),
                tile(NM), tile(NM), tile(2 * NM), vm((sent_rows, LANES), f32)]
    scratch += [dma((8,)), dma((8,)), dma((2 * NM,)), dma((NM,)), dma((1,)), pltpu.SemaphoreType.REGULAR((4,))]
    blocks = [jax.ShapeDtypeStruct((q['n0'], q['n1']), f32) for q in mats]
    out_shape = blocks + blocks + [jax.ShapeDtypeStruct((1 + 2 * NM, 8, LANES), f32)]
    vmem = pl.BlockSpec(memory_space=pltpu.VMEM)
    hbm = pl.BlockSpec(memory_space=pltpu.HBM)
    return pl.pallas_call(
        kernel, out_shape=out_shape, in_specs=[hbm] * 16, out_specs=[vmem] * len(out_shape),
        scratch_shapes=scratch,
        compiler_params=pltpu.CompilerParams(collective_id=0, has_side_effects=True,
                                             vmem_limit_bytes=36 * MIB))


def make_apply_kernel(rows_b, cols, n_model, n_data):
    mats = layout_of(rows_b, cols, n_model, n_data)

    def kernel(*refs):
        upd, params, stats = refs[0:4], refs[4:8], refs[8]
        new, delta, vrow_out, vcol_out = refs[9:13], refs[13:17], refs[17:21], refs[21:25]
        bufs, vrbuf, vcbuf = refs[25:29], refs[29:33], refs[33:37]
        out_bytes, sem = refs[37:39]
        for m in range(NM):
            fac = stats[0, 0:1, m:m + 1]
            n = mats[m]['n0'] // PARTS
            for i in range(PARTS):
                rows = slice(i * n, i * n + n)
                step = fac * upd[m][rows, :]
                bufs[m][0, rows, :] = step
                pltpu.make_async_copy(bufs[m].at[0, rows], delta[m].at[rows], sem.at[0]).start()
                bufs[m][1, rows, :] = params[m][rows, :] + step
                pltpu.make_async_copy(bufs[m].at[1, rows], new[m].at[rows], sem.at[0]).start()
        copies = []
        for m in range(NM):
            q = mats[m]
            out1, out0 = (vrbuf[m], vcbuf[m]) if q['flip'] else (vcbuf[m], vrbuf[m])
            for k in range(q['lanes']):
                out1[pl.ds(LANES * k, LANES)] = stats[1 + 2 * m, k:k + 1, :].reshape(LANES)
            for t in range(q['tiles']):
                n_t = min(LANES, q['n0'] - LANES * t)
                out0[pl.ds(LANES * t, n_t)] = stats[2 + 2 * m, t:t + 1, 0:n_t].reshape(n_t)
            for i, (buf, out) in enumerate(((vrbuf[m], vrow_out[m]), (vcbuf[m], vcol_out[m]))):
                copies.append(pltpu.make_async_copy(buf, out, sem.at[1 + 2 * m + i]))
                copies[-1].start()
        pltpu.make_async_copy(out_bytes, out_bytes, sem.at[0]).wait()
        for cp in copies:
            cp.wait()

    f32 = jnp.float32
    vmem = pl.BlockSpec(memory_space=pltpu.VMEM)
    hbm = pl.BlockSpec(memory_space=pltpu.HBM)
    blocks = [jax.ShapeDtypeStruct((q['n0'], q['n1']), f32) for q in mats]
    out_rows = sum(2 * q['n0'] * q['lanes'] for q in mats)
    out_shape = (blocks + blocks + [jax.ShapeDtypeStruct((r,), f32) for r in rows_b]
                 + [jax.ShapeDtypeStruct((c,), f32) for c in cols])
    scratch = [pltpu.VMEM((2, q['n0'], q['n1']), f32) for q in mats]
    scratch += [pltpu.VMEM((n,), f32) for n in (*rows_b, *cols)] + [pltpu.VMEM((out_rows, LANES), f32), pltpu.SemaphoreType.DMA((1 + 2 * NM,))]
    return pl.pallas_call(
        kernel, out_shape=out_shape, in_specs=[vmem] * 9, out_specs=[hbm] * 16, scratch_shapes=scratch,
        compiler_params=pltpu.CompilerParams(vmem_limit_bytes=8 * MIB))


def solution(mesh):
    n_data = mesh.shape['data']
    n_model = mesh.shape['model']
    mat_spec = P('data', 'model')
    in_specs = (P('data', None, 'model'), mat_spec, P('data'), P('model')) * NM
    out_specs = (mat_spec, mat_spec, P('data'), P('model')) * NM

    def per_device(*arrays):
        grads, params = arrays[0::4], arrays[1::4]
        rows_b = [p.shape[0] for p in params]
        cols = [p.shape[1] for p in params]
        mats = layout_of(rows_b, cols, n_model, n_data)
        view = lambda i, a: jnp.swapaxes(a, -1, -2) if mats[i]['flip'] else a
        grads = [view(i, g) for i, g in enumerate(grads)]
        params = [view(i, p) for i, p in enumerate(params)]
        pin = lambda a: pltpu.with_memory_space_constraint(a, pltpu.HBM)
        outs = make_reduce_kernel(rows_b, cols, n_model, n_data)(
            *map(pin, grads), *map(pin, params), *map(pin, arrays[2::4]), *map(pin, arrays[3::4]))
        res = make_apply_kernel(rows_b, cols, n_model, n_data)(*outs)
        flat = []
        for m in range(NM):
            flat += [view(m, res[m]), view(m, res[4 + m]), res[8 + m], res[12 + m]]
        return tuple(flat)

    return jax.shard_map(per_device, mesh=mesh, in_specs=in_specs, out_specs=out_specs, check_vma=False)
```

```python
import jax
import jax.numpy as jnp
from jax import lax
from jax.experimental import pallas as pl
from jax.experimental.pallas import tpu as pltpu
from jax.sharding import PartitionSpec as P

OPT_STEP = 3
BETA = 1.0 - OPT_STEP ** -0.8
LR_REL = min(0.01, OPT_STEP ** -0.5)
NM = 4
OWN, NX, NY, ND = 0, 1, 2, 3
FIRST_ROWS = 88
PARTS = 4
LEAD_NS = 200
LANES = 128
TILE = (8, LANES)
MIB = 1024 * 1024
MESH_ID = pl.DeviceIdType.MESH


def layout_of(rows_b, cols, n_model, n_data):
    mats = []
    for r, c in zip(rows_b, cols):
        flip = c % LANES != 0
        n0, n1 = (c, r) if flip else (r, c)
        mats.append(dict(flip=flip, n0=n0, n1=n1, half=n0 // 2, groups=n0 // 8, tiles=-(-n0 // LANES), lanes=n1 // LANES,
                         rows_b=r, rows_t=r * n_data, cols_t=c * n_model,
                         size=float(r * n_data * c * n_model)))
    return mats


def make_reduce_kernel(rows_b, cols, n_model, n_data):
    mats = layout_of(rows_b, cols, n_model, n_data)
    halves = [q['half'] for q in mats]
    n_rc = [(q['lanes'], 8) if q['flip'] else (8, q['lanes']) for q in mats]
    sent_rows = sum(7 * q['n0'] * q['lanes'] for q in mats) + n_model * n_data - 1
    sent_rows += sum(3 * r + (24 if c == 8 else 7 * c) for r, c in n_rc)
    first = []
    for lo, hi in ((0, FIRST_ROWS), (FIRST_ROWS, halves[0])):
        first += [(0, ND, lo, hi - lo), (0, ND, halves[0] + lo, hi - lo)]
    group = {m: [(m, j, 0, mats[m]['n0']) for j in ((NX, NY, OWN) if m == 0 else (ND, NX, NY, OWN))] for m in range(NM)}

    def kernel(*refs):
        grads = refs[0:4]
        params = refs[4:8]
        vrows = refs[8:12]
        vcols = refs[12:16]
        upd = refs[16:20]
        wbuf = refs[20:24]
        stats = refs[24]
        sc = list(refs[25:])
        take = lambda n: [sc.pop(0) for _ in range(n)]
        loc, rec, fxy, vrbuf, vcbuf = (take(4) for _ in range(5))
        stg, rmsg, rrx, cmsg, crx, csib, chalf, brx, vrc, vcc, stage, sent = take(12)
        ld_sem, dd_r, l_r, col_r, s_sem, greet = take(6)
        row_in = lambda m: ld_sem.at[m]
        col_in = lambda m: (col_r.at[0], col_r.at[1], dd_r.at[NM + 1], col_r.at[2])[m]
        link_in = lambda m, final: l_r.at[2 * m + final] if m < NM - 1 else ld_sem.at[NM + final]
        pair_in = lambda m: dd_r.at[m]
        merge_in = lambda m: dd_r.at[2 + m]
        totals_in = dd_r.at[NM]

        z = lax.axis_index('model')
        d = lax.axis_index('data')
        core = lax.rem(d, 2)
        xx = lax.rem(d // 2, 2)
        yy = d // 4
        sib_step = 1 - 2 * core
        sib = d + sib_step
        dx = d + 2 - 4 * xx
        dy = d + 4 - 8 * yy
        dd = dx + 4 - 8 * yy
        owner = {OWN: d, NX: dx, NY: dy, ND: dd}

        def flip_d(k):
            return d + (k % 2) * sib_step + (k // 2 % 2) * (2 - 4 * xx) + (k // 4) * (4 - 8 * yy)

        def flip_z(k):
            return z + (k % 2) * (1 - 2 * lax.rem(z, 2)) + (k // 2) * (2 - 4 * (z // 2))

        def remote(src, dst, ssem, rsem, data=None, model=None):
            return pltpu.make_async_remote_copy(
                src_ref=src, dst_ref=dst, send_sem=ssem, recv_sem=rsem,
                device_id=(z if model is None else model, d if data is None else data),
                device_id_type=MESH_ID)

        def signal(sem, data=None, model=None):
            pl.semaphore_signal(
                sem, inc=1,
                device_id=(z if model is None else model, d if data is None else data),
                device_id_type=MESH_ID)

        def wait_bytes(ref, sem):
            pltpu.make_async_copy(ref, ref, sem).wait()

        barrier = pltpu.get_barrier_semaphore()
        first_core, second_core = core == 0, core == 1
        up_ok = z < n_model - 1
        down_ok = z > 0
        n_z = jnp.where(up_ok, 1, 0) + jnp.where(down_ok, 1, 0)

        def signal_z(sem, data=None, also=None):
            @pl.when(up_ok if also is None else up_ok & also)
            def _():
                signal(sem, data=data, model=z + 1)

            @pl.when(down_ok if also is None else down_ok & also)
            def _():
                signal(sem, data=data, model=z - 1)

        @pl.when(second_core)
        def _():
            signal(barrier, data=sib)

        def block(who, f):
            m, j, r0, n = f
            q = mats[m]
            if q['flip']:
                cut = pl.ds(pl.multiple_of(who * q['n1'], LANES), q['n1'])
                return grads[m].at[0, pl.ds(r0, n), cut]
            return grads[m].at[0, pl.ds(pl.multiple_of(who * q['n0'] + r0, 8), n), :]

        loads, dsend, stage_in = {}, {}, {}
        for f in first + group[0] + group[1] + group[2] + group[3]:
            m, j, r0, n = f
            slot = first.index(f) if f in first else 4 + m
            loads[f] = pltpu.make_async_copy(block(owner[j], f), loc[m].at[j, pl.ds(r0, n), :], ld_sem.at[slot])
            source = block(owner[j] + sib_step, f)
            if f in first:
                held = stg.at[pl.ds(r0, n), :]
                stage_in[f] = pltpu.make_async_copy(source, held, ld_sem.at[4 + slot])
                source = held
            dsend[f] = remote(source, rec[m].at[j, pl.ds(r0, n), :], s_sem.at[0], dd_r.at[slot], data=sib)

        def fetch(pieces):
            for f in pieces:
                dsend[f].start()
                loads[f].start()

        def fetch_done(m):
            some = pl.ds(0, 3) if m == 0 else pl.ds(0, 4)
            wait_bytes(loc[m].at[some], ld_sem.at[4 + m])
            wait_bytes(rec[m].at[some], dd_r.at[4 + m])

        def link_send(m, j, r0, n):
            h, off = (0, r0) if r0 < halves[m] else (1, r0 - halves[m])
            along_x = (j == ND and h == 0) or j == NX
            slot = (0 if along_x else 1) if j == ND else (2 if along_x else 4) + h
            return remote(loc[m].at[j, pl.ds(r0, n), :], fxy[m].at[slot, pl.ds(off, n), :],
                          s_sem.at[0], link_in(m, int(j != ND)), data=dx if along_x else dy)

        def relays_in(m):
            wait_bytes(fxy[m].at[pl.ds(0, 2)], link_in(m, 0))

        def finals_in(m):
            wait_bytes(fxy[m].at[pl.ds(2, 4)], link_in(m, 1))

        def pair_sum(m, j, r0, n, relay=None):
            total = loc[m][j, r0:r0 + n, :] + rec[m][j, r0:r0 + n, :]
            if relay is not None:
                total = total + fxy[m][relay]
            loc[m][j, r0:r0 + n, :] = total
            link_send(m, j, r0, n).start()

        def send_raw(m):
            n = halves[m]
            fetch_done(m)
            if m > 0:
                pair_sum(m, ND, 0, n)
                pair_sum(m, ND, n, n)
            pair_sum(m, NX, 0, n)
            pair_sum(m, NY, n, n)

        def send_acc(m):
            n = halves[m]
            relays_in(m)
            pair_sum(m, NY, 0, n, 0)
            pair_sum(m, NX, n, n, 1)

        for f in first:
            stage_in[f].start()
            loads[f].start()

        @pl.when(first_core)
        def _():
            pl.semaphore_wait(barrier, 1)
            signal(barrier, data=dx + 1)
            signal(barrier, data=dy + 1)
            signal(greet.at[3], data=sib)

        signal_z(barrier, data=sib, also=first_core)

        @pl.when(second_core)
        def _():
            pl.semaphore_wait(greet.at[3], 1)

        for f in first:
            stage_in[f].wait()
            dsend[f].start()

        @pl.when(second_core)
        def _():
            pl.semaphore_wait(barrier, 2 + n_z)
            signal(greet.at[3], data=sib)

        @pl.when(first_core)
        def _():
            pl.semaphore_wait(greet.at[3], 1)

        def first_done(pieces):
            for f in pieces:
                loads[f].wait()
                dsend[f].wait_recv()

        @pl.when(second_core)
        def _():
            first_done(first[2:])
            pl.delay(LEAD_NS)

        first_done(first[:2])
        for f in first[:2]:
            pair_sum(*f)
        fetch(group[0])
        pl.when(first_core)(lambda: first_done(first[2:]))
        for f in first[2:]:
            pair_sum(*f)
        fetch(group[1])
        send_raw(0)
        fetch(group[2])
        send_raw(1)
        fetch(group[3])
        small = [pltpu.make_async_copy(vrows[m], vrbuf[m], ld_sem.at[m]) for m in range(NM)]
        small += [pltpu.make_async_copy(vcols[m], vcbuf[m], ld_sem.at[4 + m]) for m in range(2)]
        late = [pltpu.make_async_copy(params[m], wbuf[m], ld_sem.at[m]) for m in range(NM)]
        late += [pltpu.make_async_copy(vcols[m], vcbuf[m], ld_sem.at[2 + m]) for m in range(2, NM)]
        for turn in (small, late):
            for cp in turn:
                cp.start()
            for cp in turn:
                cp.wait()

        lane = lax.broadcasted_iota(jnp.int32, TILE, 1)
        sub = lax.broadcasted_iota(jnp.int32, TILE, 0)
        lane1 = lax.broadcasted_iota(jnp.int32, (1, LANES), 1)

        def group_mask(g):
            shape = (g, 8, LANES)
            return lax.broadcasted_iota(jnp.int32, shape, 2) == lax.broadcasted_iota(jnp.int32, shape, 0)

        def compact(values):
            return jnp.sum(jnp.where(group_mask(values.shape[0]), values, 0.0), axis=0)

        def expand(vec, g):
            return jnp.sum(jnp.where(group_mask(g), vec[None], 0.0), axis=2, keepdims=True)

        def rows_of(buf, n, i):
            stage[i] = jnp.zeros(TILE, jnp.float32)
            for t in range(-(-n // LANES)):
                n_t = min(LANES, n - LANES * t)
                stage[i, t:t + 1, 0:n_t] = buf[pl.ds(LANES * t, n_t)].reshape(1, n_t)

        def to_compact(i, n):
            out = jnp.zeros(TILE, jnp.float32)
            for t in range(-(-n // LANES)):
                row = jnp.broadcast_to(stage[i, t:t + 1, :], TILE)
                for g in range(min(LANES, n - LANES * t) // 8):
                    col = jnp.sum(jnp.where(lane == 8 * g + sub, row, 0.0), axis=1, keepdims=True)
                    out = jnp.where(lane == 16 * t + g, col, out)
            return out

        bv = jnp.zeros((1, LANES), jnp.float32)
        for m in range(NM):
            q = mats[m]
            w = wbuf[m][...]
            part = jnp.sum(w * w, axis=(0, 1), keepdims=True) * (1.0 / q['size'])
            bv = jnp.where(lane1 == 2 * NM + m, part, bv)
            rows_of(vrbuf[m], q['rows_b'], 2 * m)
            rows_of(vcbuf[m], cols[m], 2 * m + 1)
            if q['flip']:
                vrc[m] = stage[2 * m]
                vcc[m] = to_compact(2 * m + 1, q['n0'])
            else:
                vrc[m] = to_compact(2 * m, q['n0'])
                vcc[m] = stage[2 * m + 1]

        for i in range(3):
            signal_z(greet.at[i])
            pl.semaphore_wait(greet.at[i], n_z)

        def send_rows(m):
            n_r = n_rc[m][0]
            for k in (3, 2, 1):
                remote(rmsg.at[m, pl.ds(0, n_r)], rrx.at[3 * m + k - 1, pl.ds(0, n_r)], s_sem.at[0], row_in(m),
                       model=flip_z(k)).start()

        def send_cols(m, ks):
            n_c = n_rc[m][1]
            for k in ks:
                remote(cmsg.at[m, pl.ds(0, n_c)], crx.at[7 * m + k - 1, pl.ds(0, n_c)], s_sem.at[0], col_in(m),
                       data=flip_d(k)).start()

        def share_pair(m):
            wait_bytes(csib.at[m], pair_in(m))
            mine = jnp.where(core == 0, csib[m, 0:4, :] + cmsg[m, 0:4, :], csib[m, 4:8, :] + cmsg[m, 4:8, :])
            chalf[m, 0] = mine
            for k, peer in enumerate((dd, dx, dy)):
                remote(chalf.at[m, 0], chalf.at[m, 1 + k], s_sem.at[0], col_in(m), data=peer).start()

        def merge_pair(m):
            wait_bytes(chalf.at[m, pl.ds(1, 3)], col_in(m))
            chalf[m, 4] = chalf[m, 0] + chalf[m, 1] + chalf[m, 2] + chalf[m, 3]
            remote(chalf.at[m, 4], chalf.at[m, 5], s_sem.at[0], merge_in(m), data=sib).start()

        def merged(m):
            wait_bytes(chalf.at[m, 5], merge_in(m))
            mine, other = chalf[m, 4], chalf[m, 5]
            return jnp.concatenate([jnp.where(core == 0, mine, other), jnp.where(core == 0, other, mine)], axis=0)


        def finish_sum(m):
            q = mats[m]
            half, n1 = q['half'], q['n1']
            acc1 = jnp.zeros((8, n1), jnp.float32)
            rsums = []
            loc[m][OWN] = loc[m][OWN] + rec[m][OWN]
            finals_in(m)
            for h in range(2):
                rows = slice(h * half, (h + 1) * half)
                total = loc[m][OWN, rows, :] + fxy[m][2 + h] + fxy[m][4 + h]
                upd[m][rows, :] = total
                sq = (total * total + 1e-30).reshape(half // 8, 8, n1)
                acc1 = acc1 + jnp.sum(sq, axis=0)
                rsums.append(jnp.sum(sq, axis=2, keepdims=True))
            sum1 = jnp.sum(acc1, axis=0, keepdims=True)
            msg0, msg1 = (cmsg, rmsg) if q['flip'] else (rmsg, cmsg)
            for k in range(q['lanes']):
                msg1[m, k:k + 1, :] = sum1[:, LANES * k:LANES * k + LANES]
            if not q['flip']:
                send_cols(m, (6, 7, 2, 4, 3, 5, 1))
            msg0[m] = compact(jnp.concatenate(rsums, axis=0))
            send_rows(m)
            if q['flip']:
                remote(cmsg.at[m], csib.at[m], s_sem.at[0], pair_in(m), data=sib).start()

        def along0(m, fac):
            return expand(fac, mats[m]['groups'])

        def along1(m, fac):
            wide = [jnp.broadcast_to(fac[k:k + 1, :], TILE) for k in range(mats[m]['lanes'])]
            return jnp.concatenate(wide, axis=1)[None]

        def apply_rows(m, bv, locrow):
            q = mats[m]
            n_r = n_rc[m][0]
            ok = lane < q['groups']
            rtot = rmsg[m, 0:n_r, :]
            wait_bytes(loc[0].at[0, pl.ds(0, 3 * n_r), :], row_in(m))
            for k in range(3):
                rtot = rtot + rrx[3 * m + k, 0:n_r, :]
            vr = BETA * vrc[m, 0:n_r, :] + (1.0 - BETA) * (rtot * (1.0 / q['cols_t']))
            vr_sum = jnp.sum(vr if q['flip'] else jnp.where(ok, vr, 0.0), axis=(0, 1), keepdims=True)
            mloc = vr_sum * (1.0 / q['rows_b'])
            rfac = lax.rsqrt(vr / mloc) if q['flip'] else lax.rsqrt(jnp.where(ok, vr / mloc, 1.0))
            part = upd[m][...].reshape(q['groups'], 8, q['n1']) * (along1 if q['flip'] else along0)(m, rfac)
            upd[m][...] = part.reshape(q['n0'], q['n1'])
            vrc[m, 0:n_r, :] = vr
            bv = jnp.where(lane1 == NM + m, vr_sum * (1.0 / (q['rows_t'] * n_model)), bv)
            locrow = jnp.where(lane1 == m, mloc, locrow)
            return bv, locrow, 1.0 / mloc

        def apply_cols(m, bv, inv_mloc):
            q = mats[m]
            n_c = n_rc[m][1]
            if n_c == 8:
                ctot = merged(m)
            else:
                ctot = cmsg[m, 0:n_c, :]
                wait_bytes(loc[0].at[0, pl.ds(0, 7 * n_c), :], col_in(m))
                for k in range(7):
                    ctot = ctot + crx[7 * m + k, 0:n_c, :]
            vc = BETA * vcc[m, 0:n_c, :] + (1.0 - BETA) * (ctot * (1.0 / q['rows_t']))
            cfac = lax.rsqrt(jnp.where(lane < q['groups'], vc, 1.0)) if q['flip'] else lax.rsqrt(vc)
            u = upd[m][...].reshape(q['groups'], 8, q['n1']) * (along0 if q['flip'] else along1)(m, cfac)
            t_m = jnp.sum(jnp.sum(u * u, axis=0), axis=(0, 1), keepdims=True)
            upd[m][...] = u.reshape(q['n0'], q['n1'])
            vcc[m, 0:n_c, :] = vc
            return jnp.where(lane1 == m, (t_m * (1.0 / q['size'])) * inv_mloc, bv)

        locrow = jnp.ones((1, LANES), jnp.float32)
        send_acc(0)
        send_raw(2)
        send_acc(1)
        finish_sum(0)
        send_raw(3)
        send_acc(2)
        finish_sum(1)
        send_acc(3)
        share_pair(0)
        share_pair(1)
        bv, locrow, inv0 = apply_rows(0, bv, locrow)
        bv, locrow, inv1 = apply_rows(1, bv, locrow)
        finish_sum(2)
        finish_sum(3)
        merge_pair(0)
        merge_pair(1)
        bv, locrow, inv2 = apply_rows(2, bv, locrow)
        bv = apply_cols(0, bv, inv0)
        bv = apply_cols(1, bv, inv1)
        bv = apply_cols(2, bv, inv2)
        bv, locrow, inv3 = apply_rows(3, bv, locrow)
        bv = apply_cols(3, bv, inv3)

        brx[0:1, :] = bv
        for kz in (3, 2, 1, 0):
            for kd in (6, 7, 2, 4, 0, 3, 5, 1):
                if kz == 0 and kd == 0:
                    continue
                i = kz * n_data + kd
                remote(brx.at[pl.ds(0, 1), :], brx.at[pl.ds(i, 1), :], s_sem.at[0], totals_in,
                       data=flip_d(kd), model=flip_z(kz)).start()

        for m in range(NM):
            q = mats[m]
            lined, packed = (vrc, vcc) if q['flip'] else (vcc, vrc)
            stats[1 + 2 * m, 0:q['lanes'], :] = lined[m, 0:q['lanes'], :]
            wide = expand(packed[m], q['groups'])
            for t in range(q['tiles']):
                n_t = min(LANES, q['n0'] - LANES * t)
                g_n = n_t // 8
                shape = (g_n, 8, LANES)
                pick = (lax.broadcasted_iota(jnp.int32, shape, 2)
                        == 8 * lax.broadcasted_iota(jnp.int32, shape, 0) + lax.broadcasted_iota(jnp.int32, shape, 1))
                rows = jnp.sum(jnp.where(pick, wide[16 * t:16 * t + g_n], 0.0), axis=0)
                stats[2 + 2 * m, t:t + 1, :] = jnp.sum(rows, axis=0, keepdims=True)

        wait_bytes(brx.at[pl.ds(1, n_model * n_data - 1), :], totals_in)
        tot = jnp.broadcast_to(jnp.sum(brx[...], axis=0, keepdims=True), TILE)
        mean_vr = pltpu.roll(tot, LANES - NM, 1)
        u_rms = jnp.sqrt(mean_vr * tot)
        w_rms = jnp.sqrt(pltpu.roll(tot, LANES - 2 * NM, 1))
        fac = -(LR_REL * jnp.maximum(1e-3, w_rms)) * (jnp.sqrt(mean_vr) * lax.rsqrt(locrow))
        stats[0] = fac / jnp.maximum(1.0, u_rms)
        wait_bytes(sent, s_sem.at[0])

    f32 = jnp.float32
    dma = pltpu.SemaphoreType.DMA
    vm = pltpu.VMEM
    scratch = []
    scratch += [vm((4, q['n0'], q['n1']), f32) for q in mats]
    scratch += [vm((4, q['n0'], q['n1']), f32) for q in mats]
    scratch += [vm((6, q['half'], q['n1']), f32) for q in mats]
    scratch += [vm((r,), f32) for r in rows_b]
    scratch += [vm((c,), f32) for c in cols]
    scratch += [vm((mats[0]['n0'], mats[0]['n1']), f32)]
    tile = lambda *lead: vm((*lead, 8, LANES), f32)
    scratch += [tile(NM), tile(3 * NM), tile(NM), tile(7 * NM), tile(2), vm((2, 6, 4, LANES), f32), vm((n_model * n_data, LANES), f32),
                tile(NM), tile(NM), tile(2 * NM), vm((sent_rows, LANES), f32)]
    scratch += [dma((8,)), dma((8,)), dma((2 * NM - 2,)), dma((NM - 1,)), dma((1,)), pltpu.SemaphoreType.REGULAR((4,))]
    blocks = [jax.ShapeDtypeStruct((q['n0'], q['n1']), f32) for q in mats]
    out_shape = blocks + blocks + [jax.ShapeDtypeStruct((1 + 2 * NM, 8, LANES), f32)]
    vmem = pl.BlockSpec(memory_space=pltpu.VMEM)
    hbm = pl.BlockSpec(memory_space=pltpu.HBM)
    return pl.pallas_call(
        kernel, out_shape=out_shape, in_specs=[hbm] * 16, out_specs=[vmem] * len(out_shape),
        scratch_shapes=scratch,
        compiler_params=pltpu.CompilerParams(collective_id=0, has_side_effects=True,
                                             vmem_limit_bytes=36 * MIB))


def make_apply_kernel(rows_b, cols, n_model, n_data):
    mats = layout_of(rows_b, cols, n_model, n_data)

    def kernel(*refs):
        upd, params, stats = refs[0:4], refs[4:8], refs[8]
        new, delta, vrow_out, vcol_out = refs[9:13], refs[13:17], refs[17:21], refs[21:25]
        bufs, vrbuf, vcbuf = refs[25:29], refs[29:33], refs[33:37]
        out_bytes, sem = refs[37:39]
        for m in range(NM):
            fac = stats[0, 0:1, m:m + 1]
            n = mats[m]['n0'] // PARTS
            for i in range(PARTS):
                rows = slice(i * n, i * n + n)
                step = fac * upd[m][rows, :]
                bufs[m][0, rows, :] = step
                pltpu.make_async_copy(bufs[m].at[0, rows], delta[m].at[rows], sem.at[0]).start()
                bufs[m][1, rows, :] = params[m][rows, :] + step
                pltpu.make_async_copy(bufs[m].at[1, rows], new[m].at[rows], sem.at[0]).start()
        copies = []
        for m in range(NM):
            q = mats[m]
            out1, out0 = (vrbuf[m], vcbuf[m]) if q['flip'] else (vcbuf[m], vrbuf[m])
            for k in range(q['lanes']):
                out1[pl.ds(LANES * k, LANES)] = stats[1 + 2 * m, k:k + 1, :].reshape(LANES)
            for t in range(q['tiles']):
                n_t = min(LANES, q['n0'] - LANES * t)
                out0[pl.ds(LANES * t, n_t)] = stats[2 + 2 * m, t:t + 1, 0:n_t].reshape(n_t)
            for i, (buf, out) in enumerate(((vrbuf[m], vrow_out[m]), (vcbuf[m], vcol_out[m]))):
                copies.append(pltpu.make_async_copy(buf, out, sem.at[1 + 2 * m + i]))
                copies[-1].start()
        pltpu.make_async_copy(out_bytes, out_bytes, sem.at[0]).wait()
        for cp in copies:
            cp.wait()

    f32 = jnp.float32
    vmem = pl.BlockSpec(memory_space=pltpu.VMEM)
    hbm = pl.BlockSpec(memory_space=pltpu.HBM)
    blocks = [jax.ShapeDtypeStruct((q['n0'], q['n1']), f32) for q in mats]
    out_rows = sum(2 * q['n0'] * q['lanes'] for q in mats)
    out_shape = (blocks + blocks + [jax.ShapeDtypeStruct((r,), f32) for r in rows_b]
                 + [jax.ShapeDtypeStruct((c,), f32) for c in cols])
    scratch = [pltpu.VMEM((2, q['n0'], q['n1']), f32) for q in mats]
    scratch += [pltpu.VMEM((n,), f32) for n in (*rows_b, *cols)] + [pltpu.VMEM((out_rows, LANES), f32), pltpu.SemaphoreType.DMA((1 + 2 * NM,))]
    return pl.pallas_call(
        kernel, out_shape=out_shape, in_specs=[vmem] * 9, out_specs=[hbm] * 16, scratch_shapes=scratch,
        compiler_params=pltpu.CompilerParams(vmem_limit_bytes=8 * MIB))


def solution(mesh):
    n_data = mesh.shape['data']
    n_model = mesh.shape['model']
    mat_spec = P('data', 'model')
    in_specs = (P('data', None, 'model'), mat_spec, P('data'), P('model')) * NM
    out_specs = (mat_spec, mat_spec, P('data'), P('model')) * NM

    def per_device(*arrays):
        grads, params = arrays[0::4], arrays[1::4]
        rows_b = [p.shape[0] for p in params]
        cols = [p.shape[1] for p in params]
        mats = layout_of(rows_b, cols, n_model, n_data)
        view = lambda i, a: jnp.swapaxes(a, -1, -2) if mats[i]['flip'] else a
        grads = [view(i, g) for i, g in enumerate(grads)]
        params = [view(i, p) for i, p in enumerate(params)]
        pin = lambda a: pltpu.with_memory_space_constraint(a, pltpu.HBM)
        outs = make_reduce_kernel(rows_b, cols, n_model, n_data)(
            *map(pin, grads), *map(pin, params), *map(pin, arrays[2::4]), *map(pin, arrays[3::4]))
        res = make_apply_kernel(rows_b, cols, n_model, n_data)(*outs)
        flat = []
        for m in range(NM):
            flat += [view(m, res[m]), view(m, res[4 + m]), res[8 + m], res[12 + m]]
        return tuple(flat)

    return jax.shard_map(per_device, mesh=mesh, in_specs=in_specs, out_specs=out_specs, check_vma=False)
```

```python
import jax
import jax.numpy as jnp
from jax import lax
from jax.experimental import pallas as pl
from jax.experimental.pallas import tpu as pltpu
from jax.sharding import PartitionSpec as P

OPT_STEP = 3
BETA = 1.0 - OPT_STEP ** -0.8
LR_REL = min(0.01, OPT_STEP ** -0.5)
NM = 4
OWN, NX, NY, ND = 0, 1, 2, 3
FIRST_ROWS = 88
PARTS = (8, 4, 4, 4)
LEAD_NS = 200
LANES = 128
TILE = (8, LANES)
MIB = 1024 * 1024
MESH_ID = pl.DeviceIdType.MESH


def layout_of(rows_b, cols, n_model, n_data):
    mats = []
    for r, c in zip(rows_b, cols):
        flip = c % LANES != 0
        n0, n1 = (c, r) if flip else (r, c)
        mats.append(dict(flip=flip, n0=n0, n1=n1, half=n0 // 2, groups=n0 // 8, tiles=-(-n0 // LANES), lanes=n1 // LANES,
                         rows_b=r, rows_t=r * n_data, cols_t=c * n_model,
                         size=float(r * n_data * c * n_model)))
    return mats


def make_reduce_kernel(rows_b, cols, n_model, n_data):
    mats = layout_of(rows_b, cols, n_model, n_data)
    halves = [q['half'] for q in mats]
    n_rc = [(q['lanes'], 8) if q['flip'] else (8, q['lanes']) for q in mats]
    sent_rows = sum(7 * q['n0'] * q['lanes'] for q in mats) + n_model * n_data - 1
    sent_rows += sum(3 * r + (24 if c == 8 else 7 * c) for r, c in n_rc)
    first = []
    for lo, hi in ((0, FIRST_ROWS), (FIRST_ROWS, halves[0])):
        first += [(0, ND, lo, hi - lo), (0, ND, halves[0] + lo, hi - lo)]
    group = {m: [(m, j, 0, mats[m]['n0']) for j in ((NX, NY, OWN) if m == 0 else (ND, NX, NY, OWN))] for m in range(NM)}

    def kernel(*refs):
        grads = refs[0:4]
        params = refs[4:8]
        vrows = refs[8:12]
        vcols = refs[12:16]
        upd = refs[16:20]
        wbuf = refs[20:24]
        stats = refs[24]
        sc = list(refs[25:])
        take = lambda n: [sc.pop(0) for _ in range(n)]
        loc, rec, fxy, vrbuf, vcbuf = (take(4) for _ in range(5))
        stg, rmsg, rrx, cmsg, crx, csib, chalf, brx, vrc, vcc, stage, sent = take(12)
        ld_sem, dd_r, l_r, col_r, s_sem, greet = take(6)
        row_in = lambda m: ld_sem.at[m]
        col_in = lambda m: (col_r.at[0], col_r.at[1], dd_r.at[NM + 1], col_r.at[2])[m]
        link_in = lambda m, final: l_r.at[2 * m + final] if m < NM - 1 else ld_sem.at[NM + final]
        pair_in = lambda m: dd_r.at[m]
        merge_in = lambda m: dd_r.at[2 + m]
        totals_in = dd_r.at[NM]

        z = lax.axis_index('model')
        d = lax.axis_index('data')
        core = lax.rem(d, 2)
        xx = lax.rem(d // 2, 2)
        yy = d // 4
        sib_step = 1 - 2 * core
        sib = d + sib_step
        dx = d + 2 - 4 * xx
        dy = d + 4 - 8 * yy
        dd = dx + 4 - 8 * yy
        owner = {OWN: d, NX: dx, NY: dy, ND: dd}

        def flip_d(k):
            return d + (k % 2) * sib_step + (k // 2 % 2) * (2 - 4 * xx) + (k // 4) * (4 - 8 * yy)

        def flip_z(k):
            return z + (k % 2) * (1 - 2 * lax.rem(z, 2)) + (k // 2) * (2 - 4 * (z // 2))

        def remote(src, dst, ssem, rsem, data=None, model=None):
            return pltpu.make_async_remote_copy(
                src_ref=src, dst_ref=dst, send_sem=ssem, recv_sem=rsem,
                device_id=(z if model is None else model, d if data is None else data),
                device_id_type=MESH_ID)

        def signal(sem, data=None, model=None):
            pl.semaphore_signal(
                sem, inc=1,
                device_id=(z if model is None else model, d if data is None else data),
                device_id_type=MESH_ID)

        def wait_bytes(ref, sem):
            pltpu.make_async_copy(ref, ref, sem).wait()

        barrier = pltpu.get_barrier_semaphore()
        first_core, second_core = core == 0, core == 1
        up_ok = z < n_model - 1
        down_ok = z > 0
        n_z = jnp.where(up_ok, 1, 0) + jnp.where(down_ok, 1, 0)

        def signal_z(sem, data=None, also=None):
            @pl.when(up_ok if also is None else up_ok & also)
            def _():
                signal(sem, data=data, model=z + 1)

            @pl.when(down_ok if also is None else down_ok & also)
            def _():
                signal(sem, data=data, model=z - 1)

        @pl.when(second_core)
        def _():
            signal(barrier, data=sib)

        def block(who, f):
            m, j, r0, n = f
            q = mats[m]
            if q['flip']:
                cut = pl.ds(pl.multiple_of(who * q['n1'], LANES), q['n1'])
                return grads[m].at[0, pl.ds(r0, n), cut]
            return grads[m].at[0, pl.ds(pl.multiple_of(who * q['n0'] + r0, 8), n), :]

        loads, dsend, stage_in = {}, {}, {}
        for f in first + group[0] + group[1] + group[2] + group[3]:
            m, j, r0, n = f
            slot = first.index(f) if f in first else 4 + m
            loads[f] = pltpu.make_async_copy(block(owner[j], f), loc[m].at[j, pl.ds(r0, n), :], ld_sem.at[slot])
            source = block(owner[j] + sib_step, f)
            if f in first:
                held = stg.at[pl.ds(r0, n), :]
                stage_in[f] = pltpu.make_async_copy(source, held, ld_sem.at[4 + slot])
                source = held
            dsend[f] = remote(source, rec[m].at[j, pl.ds(r0, n), :], s_sem.at[0], dd_r.at[slot], data=sib)

        def fetch(pieces):
            for f in pieces:
                dsend[f].start()
                loads[f].start()

        def fetch_done(m):
            some = pl.ds(0, 3) if m == 0 else pl.ds(0, 4)
            wait_bytes(loc[m].at[some], ld_sem.at[4 + m])
            wait_bytes(rec[m].at[some], dd_r.at[4 + m])

        def link_send(m, j, r0, n):
            h, off = (0, r0) if r0 < halves[m] else (1, r0 - halves[m])
            along_x = (j == ND and h == 0) or j == NX
            slot = (0 if along_x else 1) if j == ND else (2 if along_x else 4) + h
            return remote(loc[m].at[j, pl.ds(r0, n), :], fxy[m].at[slot, pl.ds(off, n), :],
                          s_sem.at[0], link_in(m, int(j != ND)), data=dx if along_x else dy)

        def relays_in(m):
            wait_bytes(fxy[m].at[pl.ds(0, 2)], link_in(m, 0))

        def finals_in(m):
            wait_bytes(fxy[m].at[pl.ds(2, 4)], link_in(m, 1))

        def pair_sum(m, j, r0, n, relay=None):
            total = loc[m][j, r0:r0 + n, :] + rec[m][j, r0:r0 + n, :]
            if relay is not None:
                total = total + fxy[m][relay]
            loc[m][j, r0:r0 + n, :] = total
            link_send(m, j, r0, n).start()

        def send_raw(m):
            n = halves[m]
            fetch_done(m)
            if m > 0:
                pair_sum(m, ND, 0, n)
                pair_sum(m, ND, n, n)
            pair_sum(m, NX, 0, n)
            pair_sum(m, NY, n, n)

        def send_acc(m):
            n = halves[m]
            relays_in(m)
            pair_sum(m, NY, 0, n, 0)
            pair_sum(m, NX, n, n, 1)

        for f in first:
            stage_in[f].start()
            loads[f].start()

        @pl.when(first_core)
        def _():
            pl.semaphore_wait(barrier, 1)
            signal(barrier, data=dx + 1)
            signal(barrier, data=dy + 1)
            signal(greet.at[3], data=sib)

        signal_z(barrier, data=sib, also=first_core)

        @pl.when(second_core)
        def _():
            pl.semaphore_wait(greet.at[3], 1)

        for f in first:
            stage_in[f].wait()
            dsend[f].start()

        @pl.when(second_core)
        def _():
            pl.semaphore_wait(barrier, 2 + n_z)
            signal(greet.at[3], data=sib)

        @pl.when(first_core)
        def _():
            pl.semaphore_wait(greet.at[3], 1)

        def first_done(pieces):
            for f in pieces:
                loads[f].wait()
                dsend[f].wait_recv()

        @pl.when(second_core)
        def _():
            first_done(first[2:])

            @pl.when(xx + yy < 2)
            def _():
                pl.delay(LEAD_NS)

        first_done(first[:2])
        for f in first[:2]:
            pair_sum(*f)
        fetch(group[0])
        pl.when(first_core)(lambda: first_done(first[2:]))
        for f in first[2:]:
            pair_sum(*f)
        fetch(group[1])
        send_raw(0)
        fetch(group[2])
        send_raw(1)
        fetch(group[3])
        small = [pltpu.make_async_copy(vrows[m], vrbuf[m], ld_sem.at[m]) for m in range(NM)]
        small += [pltpu.make_async_copy(vcols[m], vcbuf[m], ld_sem.at[4 + m]) for m in range(2)]
        late = [pltpu.make_async_copy(params[m], wbuf[m], ld_sem.at[m]) for m in range(NM)]
        late += [pltpu.make_async_copy(vcols[m], vcbuf[m], ld_sem.at[2 + m]) for m in range(2, NM)]
        for turn in (small, late):
            for cp in turn:
                cp.start()
            for cp in turn:
                cp.wait()

        lane = lax.broadcasted_iota(jnp.int32, TILE, 1)
        sub = lax.broadcasted_iota(jnp.int32, TILE, 0)
        lane1 = lax.broadcasted_iota(jnp.int32, (1, LANES), 1)

        def group_mask(g):
            shape = (g, 8, LANES)
            return lax.broadcasted_iota(jnp.int32, shape, 2) == lax.broadcasted_iota(jnp.int32, shape, 0)

        def compact(values):
            return jnp.sum(jnp.where(group_mask(values.shape[0]), values, 0.0), axis=0)

        def expand(vec, g):
            return jnp.sum(jnp.where(group_mask(g), vec[None], 0.0), axis=2, keepdims=True)

        def rows_of(buf, n, i):
            stage[i] = jnp.zeros(TILE, jnp.float32)
            for t in range(-(-n // LANES)):
                n_t = min(LANES, n - LANES * t)
                stage[i, t:t + 1, 0:n_t] = buf[pl.ds(LANES * t, n_t)].reshape(1, n_t)

        def to_compact(i, n):
            out = jnp.zeros(TILE, jnp.float32)
            for t in range(-(-n // LANES)):
                row = jnp.broadcast_to(stage[i, t:t + 1, :], TILE)
                for g in range(min(LANES, n - LANES * t) // 8):
                    col = jnp.sum(jnp.where(lane == 8 * g + sub, row, 0.0), axis=1, keepdims=True)
                    out = jnp.where(lane == 16 * t + g, col, out)
            return out

        bv = jnp.zeros((1, LANES), jnp.float32)
        for m in range(NM):
            q = mats[m]
            w = wbuf[m][...]
            part = jnp.sum(w * w, axis=(0, 1), keepdims=True) * (1.0 / q['size'])
            bv = jnp.where(lane1 == 2 * NM + m, part, bv)
            rows_of(vrbuf[m], q['rows_b'], 2 * m)
            rows_of(vcbuf[m], cols[m], 2 * m + 1)
            if q['flip']:
                vrc[m] = stage[2 * m]
                vcc[m] = to_compact(2 * m + 1, q['n0'])
            else:
                vrc[m] = to_compact(2 * m, q['n0'])
                vcc[m] = stage[2 * m + 1]

        for i in range(3):
            signal_z(greet.at[i])
            pl.semaphore_wait(greet.at[i], n_z)

        def send_rows(m):
            n_r = n_rc[m][0]
            for k in (3, 2, 1):
                remote(rmsg.at[m, pl.ds(0, n_r)], rrx.at[3 * m + k - 1, pl.ds(0, n_r)], s_sem.at[0], row_in(m),
                       model=flip_z(k)).start()

        def send_cols(m, ks):
            n_c = n_rc[m][1]
            for k in ks:
                remote(cmsg.at[m, pl.ds(0, n_c)], crx.at[7 * m + k - 1, pl.ds(0, n_c)], s_sem.at[0], col_in(m),
                       data=flip_d(k)).start()

        def share_pair(m):
            wait_bytes(csib.at[m], pair_in(m))
            mine = jnp.where(core == 0, csib[m, 0:4, :] + cmsg[m, 0:4, :], csib[m, 4:8, :] + cmsg[m, 4:8, :])
            chalf[m, 0] = mine
            for k, peer in enumerate((dd, dx, dy)):
                remote(chalf.at[m, 0], chalf.at[m, 1 + k], s_sem.at[0], col_in(m), data=peer).start()

        def merge_pair(m):
            wait_bytes(chalf.at[m, pl.ds(1, 3)], col_in(m))
            chalf[m, 4] = chalf[m, 0] + chalf[m, 1] + chalf[m, 2] + chalf[m, 3]
            remote(chalf.at[m, 4], chalf.at[m, 5], s_sem.at[0], merge_in(m), data=sib).start()

        def merged(m):
            wait_bytes(chalf.at[m, 5], merge_in(m))
            mine, other = chalf[m, 4], chalf[m, 5]
            return jnp.concatenate([jnp.where(core == 0, mine, other), jnp.where(core == 0, other, mine)], axis=0)


        def finish_sum(m):
            q = mats[m]
            half, n1 = q['half'], q['n1']
            acc1 = jnp.zeros((8, n1), jnp.float32)
            rsums = []
            loc[m][OWN] = loc[m][OWN] + rec[m][OWN]
            finals_in(m)
            for h in range(2):
                rows = slice(h * half, (h + 1) * half)
                total = loc[m][OWN, rows, :] + fxy[m][2 + h] + fxy[m][4 + h]
                upd[m][rows, :] = total
                sq = (total * total + 1e-30).reshape(half // 8, 8, n1)
                acc1 = acc1 + jnp.sum(sq, axis=0)
                rsums.append(jnp.sum(sq, axis=2, keepdims=True))
            sum1 = jnp.sum(acc1, axis=0, keepdims=True)
            msg0, msg1 = (cmsg, rmsg) if q['flip'] else (rmsg, cmsg)
            for k in range(q['lanes']):
                msg1[m, k:k + 1, :] = sum1[:, LANES * k:LANES * k + LANES]
            if not q['flip']:
                send_cols(m, (6, 7, 2, 4, 3, 5, 1))
            msg0[m] = compact(jnp.concatenate(rsums, axis=0))
            send_rows(m)
            if q['flip']:
                remote(cmsg.at[m], csib.at[m], s_sem.at[0], pair_in(m), data=sib).start()

        def along0(m, fac):
            return expand(fac, mats[m]['groups'])

        def along1(m, fac):
            wide = [jnp.broadcast_to(fac[k:k + 1, :], TILE) for k in range(mats[m]['lanes'])]
            return jnp.concatenate(wide, axis=1)[None]

        def apply_rows(m, bv, locrow):
            q = mats[m]
            n_r = n_rc[m][0]
            ok = lane < q['groups']
            rtot = rmsg[m, 0:n_r, :]
            wait_bytes(loc[0].at[0, pl.ds(0, 3 * n_r), :], row_in(m))
            for k in range(3):
                rtot = rtot + rrx[3 * m + k, 0:n_r, :]
            vr = BETA * vrc[m, 0:n_r, :] + (1.0 - BETA) * (rtot * (1.0 / q['cols_t']))
            vr_sum = jnp.sum(vr if q['flip'] else jnp.where(ok, vr, 0.0), axis=(0, 1), keepdims=True)
            mloc = vr_sum * (1.0 / q['rows_b'])
            rfac = lax.rsqrt(vr / mloc) if q['flip'] else lax.rsqrt(jnp.where(ok, vr / mloc, 1.0))
            part = upd[m][...].reshape(q['groups'], 8, q['n1']) * (along1 if q['flip'] else along0)(m, rfac)
            upd[m][...] = part.reshape(q['n0'], q['n1'])
            vrc[m, 0:n_r, :] = vr
            bv = jnp.where(lane1 == NM + m, vr_sum * (1.0 / (q['rows_t'] * n_model)), bv)
            locrow = jnp.where(lane1 == m, mloc, locrow)
            return bv, locrow, 1.0 / mloc

        def apply_cols(m, bv, inv_mloc):
            q = mats[m]
            n_c = n_rc[m][1]
            if n_c == 8:
                ctot = merged(m)
            else:
                ctot = cmsg[m, 0:n_c, :]
                wait_bytes(loc[0].at[0, pl.ds(0, 7 * n_c), :], col_in(m))
                for k in range(7):
                    ctot = ctot + crx[7 * m + k, 0:n_c, :]
            vc = BETA * vcc[m, 0:n_c, :] + (1.0 - BETA) * (ctot * (1.0 / q['rows_t']))
            cfac = lax.rsqrt(jnp.where(lane < q['groups'], vc, 1.0)) if q['flip'] else lax.rsqrt(vc)
            u = upd[m][...].reshape(q['groups'], 8, q['n1']) * (along0 if q['flip'] else along1)(m, cfac)
            t_m = jnp.sum(jnp.sum(u * u, axis=0), axis=(0, 1), keepdims=True)
            upd[m][...] = u.reshape(q['n0'], q['n1'])
            vcc[m, 0:n_c, :] = vc
            return jnp.where(lane1 == m, (t_m * (1.0 / q['size'])) * inv_mloc, bv)

        locrow = jnp.ones((1, LANES), jnp.float32)
        send_acc(0)
        send_raw(2)
        send_acc(1)
        finish_sum(0)
        send_raw(3)
        send_acc(2)
        finish_sum(1)
        send_acc(3)
        share_pair(0)
        share_pair(1)
        bv, locrow, inv0 = apply_rows(0, bv, locrow)
        bv, locrow, inv1 = apply_rows(1, bv, locrow)
        finish_sum(2)
        finish_sum(3)
        merge_pair(0)
        merge_pair(1)
        bv, locrow, inv2 = apply_rows(2, bv, locrow)
        bv = apply_cols(0, bv, inv0)
        bv = apply_cols(1, bv, inv1)
        bv = apply_cols(2, bv, inv2)
        bv, locrow, inv3 = apply_rows(3, bv, locrow)
        bv = apply_cols(3, bv, inv3)

        brx[0:1, :] = bv
        for kz in (3, 2, 1, 0):
            for kd in (6, 7, 2, 4, 0, 3, 5, 1):
                if kz == 0 and kd == 0:
                    continue
                i = kz * n_data + kd
                remote(brx.at[pl.ds(0, 1), :], brx.at[pl.ds(i, 1), :], s_sem.at[0], totals_in,
                       data=flip_d(kd), model=flip_z(kz)).start()

        for m in range(NM):
            q = mats[m]
            lined, packed = (vrc, vcc) if q['flip'] else (vcc, vrc)
            stats[1 + 2 * m, 0:q['lanes'], :] = lined[m, 0:q['lanes'], :]
            wide = expand(packed[m], q['groups'])
            for t in range(q['tiles']):
                n_t = min(LANES, q['n0'] - LANES * t)
                g_n = n_t // 8
                shape = (g_n, 8, LANES)
                pick = (lax.broadcasted_iota(jnp.int32, shape, 2)
                        == 8 * lax.broadcasted_iota(jnp.int32, shape, 0) + lax.broadcasted_iota(jnp.int32, shape, 1))
                rows = jnp.sum(jnp.where(pick, wide[16 * t:16 * t + g_n], 0.0), axis=0)
                stats[2 + 2 * m, t:t + 1, :] = jnp.sum(rows, axis=0, keepdims=True)

        wait_bytes(brx.at[pl.ds(1, n_model * n_data - 1), :], totals_in)
        tot = jnp.broadcast_to(jnp.sum(brx[...], axis=0, keepdims=True), TILE)
        mean_vr = pltpu.roll(tot, LANES - NM, 1)
        u_rms = jnp.sqrt(mean_vr * tot)
        w_rms = jnp.sqrt(pltpu.roll(tot, LANES - 2 * NM, 1))
        fac = -(LR_REL * jnp.maximum(1e-3, w_rms)) * (jnp.sqrt(mean_vr) * lax.rsqrt(locrow))
        stats[0] = fac / jnp.maximum(1.0, u_rms)
        wait_bytes(sent, s_sem.at[0])

    f32 = jnp.float32
    dma = pltpu.SemaphoreType.DMA
    vm = pltpu.VMEM
    scratch = []
    scratch += [vm((4, q['n0'], q['n1']), f32) for q in mats]
    scratch += [vm((4, q['n0'], q['n1']), f32) for q in mats]
    scratch += [vm((6, q['half'], q['n1']), f32) for q in mats]
    scratch += [vm((r,), f32) for r in rows_b]
    scratch += [vm((c,), f32) for c in cols]
    scratch += [vm((mats[0]['n0'], mats[0]['n1']), f32)]
    tile = lambda *lead: vm((*lead, 8, LANES), f32)
    scratch += [tile(NM), tile(3 * NM), tile(NM), tile(7 * NM), tile(2), vm((2, 6, 4, LANES), f32), vm((n_model * n_data, LANES), f32),
                tile(NM), tile(NM), tile(2 * NM), vm((sent_rows, LANES), f32)]
    scratch += [dma((8,)), dma((8,)), dma((2 * NM - 2,)), dma((NM - 1,)), dma((1,)), pltpu.SemaphoreType.REGULAR((4,))]
    blocks = [jax.ShapeDtypeStruct((q['n0'], q['n1']), f32) for q in mats]
    out_shape = blocks + blocks + [jax.ShapeDtypeStruct((1 + 2 * NM, 8, LANES), f32)]
    vmem = pl.BlockSpec(memory_space=pltpu.VMEM)
    hbm = pl.BlockSpec(memory_space=pltpu.HBM)
    return pl.pallas_call(
        kernel, out_shape=out_shape, in_specs=[hbm] * 16, out_specs=[vmem] * len(out_shape),
        scratch_shapes=scratch,
        compiler_params=pltpu.CompilerParams(collective_id=0, has_side_effects=True,
                                             vmem_limit_bytes=36 * MIB))


def make_apply_kernel(rows_b, cols, n_model, n_data):
    mats = layout_of(rows_b, cols, n_model, n_data)

    def kernel(*refs):
        upd, params, stats = refs[0:4], refs[4:8], refs[8]
        new, delta, vrow_out, vcol_out = refs[9:13], refs[13:17], refs[17:21], refs[21:25]
        bufs, vrbuf, vcbuf = refs[25:29], refs[29:33], refs[33:37]
        out_bytes, sem = refs[37:39]
        for m in range(NM):
            fac = stats[0, 0:1, m:m + 1]
            n = mats[m]['n0'] // PARTS[m]
            for i in range(PARTS[m]):
                rows = slice(i * n, i * n + n)
                step = fac * upd[m][rows, :]
                bufs[m][0, rows, :] = step
                pltpu.make_async_copy(bufs[m].at[0, rows], delta[m].at[rows], sem.at[0]).start()
                bufs[m][1, rows, :] = params[m][rows, :] + step
                pltpu.make_async_copy(bufs[m].at[1, rows], new[m].at[rows], sem.at[0]).start()
        copies = []
        for m in range(NM):
            q = mats[m]
            out1, out0 = (vrbuf[m], vcbuf[m]) if q['flip'] else (vcbuf[m], vrbuf[m])
            for k in range(q['lanes']):
                out1[pl.ds(LANES * k, LANES)] = stats[1 + 2 * m, k:k + 1, :].reshape(LANES)
            for t in range(q['tiles']):
                n_t = min(LANES, q['n0'] - LANES * t)
                out0[pl.ds(LANES * t, n_t)] = stats[2 + 2 * m, t:t + 1, 0:n_t].reshape(n_t)
            for i, (buf, out) in enumerate(((vrbuf[m], vrow_out[m]), (vcbuf[m], vcol_out[m]))):
                copies.append(pltpu.make_async_copy(buf, out, sem.at[1 + 2 * m + i]))
                copies[-1].start()
        pltpu.make_async_copy(out_bytes, out_bytes, sem.at[0]).wait()
        for cp in copies:
            cp.wait()

    f32 = jnp.float32
    vmem = pl.BlockSpec(memory_space=pltpu.VMEM)
    hbm = pl.BlockSpec(memory_space=pltpu.HBM)
    blocks = [jax.ShapeDtypeStruct((q['n0'], q['n1']), f32) for q in mats]
    out_rows = sum(2 * q['n0'] * q['lanes'] for q in mats)
    out_shape = (blocks + blocks + [jax.ShapeDtypeStruct((r,), f32) for r in rows_b]
                 + [jax.ShapeDtypeStruct((c,), f32) for c in cols])
    scratch = [pltpu.VMEM((2, q['n0'], q['n1']), f32) for q in mats]
    scratch += [pltpu.VMEM((n,), f32) for n in (*rows_b, *cols)] + [pltpu.VMEM((out_rows, LANES), f32), pltpu.SemaphoreType.DMA((1 + 2 * NM,))]
    return pl.pallas_call(
        kernel, out_shape=out_shape, in_specs=[vmem] * 9, out_specs=[hbm] * 16, scratch_shapes=scratch,
        compiler_params=pltpu.CompilerParams(vmem_limit_bytes=8 * MIB))


def solution(mesh):
    n_data = mesh.shape['data']
    n_model = mesh.shape['model']
    mat_spec = P('data', 'model')
    in_specs = (P('data', None, 'model'), mat_spec, P('data'), P('model')) * NM
    out_specs = (mat_spec, mat_spec, P('data'), P('model')) * NM

    def per_device(*arrays):
        grads, params = arrays[0::4], arrays[1::4]
        rows_b = [p.shape[0] for p in params]
        cols = [p.shape[1] for p in params]
        mats = layout_of(rows_b, cols, n_model, n_data)
        view = lambda i, a: jnp.swapaxes(a, -1, -2) if mats[i]['flip'] else a
        grads = [view(i, g) for i, g in enumerate(grads)]
        params = [view(i, p) for i, p in enumerate(params)]
        pin = lambda a: pltpu.with_memory_space_constraint(a, pltpu.HBM)
        outs = make_reduce_kernel(rows_b, cols, n_model, n_data)(
            *map(pin, grads), *map(pin, params), *map(pin, arrays[2::4]), *map(pin, arrays[3::4]))
        res = make_apply_kernel(rows_b, cols, n_model, n_data)(*outs)
        flat = []
        for m in range(NM):
            flat += [view(m, res[m]), view(m, res[4 + m]), res[8 + m], res[12 + m]]
        return tuple(flat)

    return jax.shard_map(per_device, mesh=mesh, in_specs=in_specs, out_specs=out_specs, check_vma=False)
```
